8 devices in a mesh: dp: 1 (over z), tp: 2 (over y), cp: 4 (over x, core).
Axes of the slice: x: 2, y: 2, z: 1, core: 2. Of those that a mesh axis runs over, the one named last changes fastest.
Arguments:
- hidden: bfloat16 [1024, 6144], P(('dp', 'cp'))
- seg_ids: int32 [1024], P(('dp', 'cp'))
- w_q: bfloat16 [6144, 6144], P(None, 'tp')
- b_q: bfloat16 [6144], P('tp')
- w_kv: bfloat16 [6144, 256], replicated
- b_kv: bfloat16 [256], replicated
- w_o: bfloat16 [6144, 6144], P('tp')
- b_o: bfloat16 [6144], replicated
- ln_gain: bfloat16 [6144], replicated
- ln_bias: bfloat16 [6144], replicated
Outputs:
- output 1: bfloat16 [1024, 6144], P(('dp', 'cp'))
- output 2: bfloat16 [1024, 128], P(('dp', 'cp'))
- output 3: bfloat16 [1024, 128], P(('dp', 'cp'))
All inputs are finite; a program needn't handle non-finite values.
Results may differ from the reference program's by a relative error of at most 0.0118747.
Values are sent between devices in bfloat16 or wider.
A program may use at most 1 GiB of HBM per device.

```python
import jax
import jax.numpy as jnp
from jax import lax

D_MODEL = 6144
N_HEADS = 48
HEAD_DIM = 128
TOKENS = 1024
HEAD_GROUPS = 2

LN_EPS = 1e-5
ATTN_SCALE = HEAD_DIM ** -0.5
QUERY_ROWS = min(TOKENS, 64)


def draw_segments(seg_key):
    len_low = TOKENS // 27 + 1
    len_high = (TOKENS * 5) // 8
    max_prompts = TOKENS // len_low + 1
    lengths = jax.random.randint(seg_key, (max_prompts,), len_low, len_high + 1, dtype=jnp.int32)
    prompt_ends = jnp.cumsum(lengths)
    positions = jnp.arange(TOKENS, dtype=jnp.int32)
    return jnp.sum((positions[:, None] >= prompt_ends[None, :]).astype(jnp.int32), axis=1)


def setup_inputs(seed: int = 0, part: int = 0) -> dict:
    part_key = jax.random.fold_in(jax.random.key(seed), part)
    key_hidden, key_seg = jax.random.split(part_key)
    shared = jax.random.split(jax.random.key(seed + 1), 8)
    q_width = N_HEADS * HEAD_DIM
    hidden = (0.5 * jax.random.normal(key_hidden, (TOKENS, D_MODEL), jnp.float32)).astype(jnp.bfloat16)
    seg_ids = draw_segments(key_seg)
    w_q = (1.6 * D_MODEL ** -0.5 * jax.random.normal(shared[0], (D_MODEL, q_width), jnp.float32)).astype(jnp.bfloat16)
    b_q = (0.3 * jax.random.normal(shared[1], (q_width,), jnp.float32)).astype(jnp.bfloat16)
    w_kv = (1.6 * D_MODEL ** -0.5 * jax.random.normal(shared[2], (D_MODEL, 2 * HEAD_DIM), jnp.float32)).astype(jnp.bfloat16)
    b_kv = (0.2 * jax.random.normal(shared[3], (2 * HEAD_DIM,), jnp.float32)).astype(jnp.bfloat16)
    w_o = (q_width ** -0.5 * jax.random.normal(shared[4], (q_width, D_MODEL), jnp.float32)).astype(jnp.bfloat16)
    b_o = (0.3 * jax.random.normal(shared[5], (D_MODEL,), jnp.float32)).astype(jnp.bfloat16)
    ln_gain = (1.0 + 0.3 * jax.random.normal(shared[6], (D_MODEL,), jnp.float32)).astype(jnp.bfloat16)
    ln_bias = (0.3 * jax.random.normal(shared[7], (D_MODEL,), jnp.float32)).astype(jnp.bfloat16)
    return dict(hidden=hidden, seg_ids=seg_ids, w_q=w_q, b_q=b_q, w_kv=w_kv, b_kv=b_kv, w_o=w_o, b_o=b_o, ln_gain=ln_gain, ln_bias=ln_bias)


def reference(hidden, seg_ids, w_q, b_q, w_kv, b_kv, w_o, b_o, ln_gain, ln_bias):
    x_float = hidden.astype(jnp.float32)
    centered = x_float - jnp.mean(x_float, axis=-1, keepdims=True)
    variance = jnp.mean(centered * centered, axis=-1, keepdims=True)
    normed = (centered * lax.rsqrt(variance + LN_EPS) * ln_gain.astype(jnp.float32) + ln_bias.astype(jnp.float32)).astype(jnp.bfloat16)
    q_all = (jnp.dot(normed, w_q, preferred_element_type=jnp.float32) + b_q.astype(jnp.float32)).astype(jnp.bfloat16)
    kv_all = (jnp.dot(normed, w_kv, preferred_element_type=jnp.float32) + b_kv.astype(jnp.float32)).astype(jnp.bfloat16)
    k_cache = kv_all[:, :HEAD_DIM]
    v_cache = kv_all[:, HEAD_DIM:]
    k_float = k_cache.astype(jnp.float32)
    v_float = v_cache.astype(jnp.float32)
    positions = jnp.arange(TOKENS, dtype=jnp.int32)
    n_blocks = TOKENS // QUERY_ROWS
    q_blocks = q_all.reshape(n_blocks, QUERY_ROWS, N_HEADS, HEAD_DIM)
    seg_blocks = seg_ids.reshape(n_blocks, QUERY_ROWS)
    pos_blocks = positions.reshape(n_blocks, QUERY_ROWS)

    def attend(block_in):
        q_blk, seg_q, pos_q = block_in
        scores = jnp.einsum('bhd,kd->bhk', q_blk.astype(jnp.float32), k_float) * ATTN_SCALE
        visible = (seg_ids[None, :] == seg_q[:, None]) & (positions[None, :] <= pos_q[:, None])
        scores = jnp.where(visible[:, None, :], scores, -jnp.inf)
        p_weights = jax.nn.softmax(scores, axis=-1)
        return jnp.einsum('bhk,kd->bhd', p_weights, v_float).astype(jnp.bfloat16)

    attn_out = lax.map(attend, (q_blocks, seg_blocks, pos_blocks))
    group_width = N_HEADS * HEAD_DIM // HEAD_GROUPS
    attn_groups = attn_out.reshape(TOKENS, HEAD_GROUPS, group_width).transpose(1, 0, 2)
    wo_groups = w_o.reshape(HEAD_GROUPS, group_width, D_MODEL)

    def add_group(run_total, group_pair):
        attn_g, wo_g = group_pair
        partial = jnp.dot(attn_g, wo_g, preferred_element_type=jnp.float32).astype(jnp.bfloat16)
        return run_total + partial.astype(jnp.float32), None

    proj_sum, scan_tail = lax.scan(add_group, jnp.zeros((TOKENS, D_MODEL), jnp.float32), (attn_groups, wo_groups))
    y_out = (x_float + proj_sum + b_o.astype(jnp.float32)).astype(jnp.bfloat16)
    return (y_out, k_cache, v_cache)
```

```python
import functools

import jax
import jax.numpy as jnp
from jax import lax
from jax.experimental import pallas as pl
from jax.experimental.pallas import tpu as pltpu
from jax.sharding import PartitionSpec as P

HEAD_DIM = 128
LN_EPS = 1e-5
EXP2_SCALE = HEAD_DIM ** -0.5 * 1.4426950408889634
MESH = pl.DeviceIdType.MESH

ROWS = 128
TILE_K = 3072
TILE_N = 512
SLOTS = 11
LN_ROWS = 32


def block_kernel(n_cp, hid_hbm, seg_ref, wq_hbm, bq_ref, wkv_hbm, bkv_ref, wo_hbm, bo_ref, gain_ref, bias_ref,
                 y_ref, k_ref, v_ref,
                 normed, wkv, wbuf, kv_all, seg_all, mask, qbuf, obuf, send, recv,
                 hid_sem, wkv_sem, w_sem, kv_send, kv_recv, seg_send, seg_recv, tp_send, tp_recv):
    my = lax.axis_index('cp')
    partner = 1 - lax.axis_index('tp')
    tok, d_model = y_ref.shape
    q_width = qbuf.shape[1]
    n_chunk = tok // ROWS
    q_tiles = q_width // TILE_N
    k_halves = d_model // TILE_K
    o_tiles = d_model // TILE_N
    q_items = q_tiles * k_halves
    items = q_items + o_tiles
    total = n_chunk * items

    barrier = pltpu.get_barrier_semaphore()
    for step in range(1, n_cp):
        pl.semaphore_signal(barrier, inc=1, device_id={'cp': lax.rem(my + step, n_cp)}, device_id_type=MESH)
    pl.semaphore_signal(barrier, inc=1, device_id={'tp': partner}, device_id_type=MESH)

    def hid_copy(i):
        rows = pl.ds(i * LN_ROWS, LN_ROWS)
        return pltpu.make_async_copy(hid_hbm.at[rows, :], y_ref.at[rows, :], hid_sem.at[i])

    def w_issue(g):
        slot = lax.rem(g, SLOTS)
        item = lax.rem(g, items)

        @pl.when(item < q_items)
        def _():
            col = pl.multiple_of(lax.div(item, k_halves) * TILE_N, TILE_N)
            row = pl.multiple_of(lax.rem(item, k_halves) * TILE_K, TILE_K)
            pltpu.make_async_copy(wq_hbm.at[pl.ds(row, TILE_K), pl.ds(col, TILE_N)], wbuf.at[slot], w_sem.at[slot]).start()

        @pl.when(item >= q_items)
        def _():
            col = pl.multiple_of((item - q_items) * TILE_N, TILE_N)
            pltpu.make_async_copy(wo_hbm.at[:, pl.ds(col, TILE_N)], wbuf.at[slot], w_sem.at[slot]).start()

    def w_wait(g):
        slot = lax.rem(g, SLOTS)
        pltpu.make_async_copy(wo_hbm.at[:, pl.ds(0, TILE_N)], wbuf.at[slot], w_sem.at[slot]).wait()
        return slot

    def w_next(g):
        @pl.when(g + SLOTS < total)
        def _():
            w_issue(g + SLOTS)

    n_ln = tok // LN_ROWS
    for i in range(n_ln):
        hid_copy(i).start()
    wkv_copy = pltpu.make_async_copy(wkv_hbm, wkv, wkv_sem)
    wkv_copy.start()
    for g in range(SLOTS - n_ln):
        w_issue(jnp.int32(g))

    def ln_block(i, carry):
        hid_copy(i).wait()
        w_issue(i + SLOTS - n_ln)
        rows = pl.ds(pl.multiple_of(i * LN_ROWS, LN_ROWS), LN_ROWS)
        n_col = d_model // 128

        def load(j):
            return y_ref[rows, j * 128:(j + 1) * 128].astype(jnp.float32)

        accs = [load(j) for j in range(4)]
        for j in range(4, n_col):
            accs[j % 4] = accs[j % 4] + load(j)
        mean = jnp.sum((accs[0] + accs[1]) + (accs[2] + accs[3]), axis=-1, keepdims=True) * (1.0 / d_model)
        mean = jnp.broadcast_to(mean, (LN_ROWS, 128))
        accs = [None] * 4
        for j in range(n_col):
            cen = load(j) - mean
            accs[j % 4] = cen * cen if accs[j % 4] is None else accs[j % 4] + cen * cen
        var = jnp.sum((accs[0] + accs[1]) + (accs[2] + accs[3]), axis=-1, keepdims=True) * (1.0 / d_model)
        rstd = jnp.broadcast_to(lax.rsqrt(var + LN_EPS), (LN_ROWS, 128))
        for j in range(n_col):
            cols = slice(j * 128, (j + 1) * 128)
            out = (load(j) - mean) * rstd * gain_ref[:, cols].astype(jnp.float32) + bias_ref[:, cols].astype(jnp.float32)
            normed[rows, cols] = out.astype(jnp.bfloat16)
        return carry

    lax.fori_loop(0, n_ln, ln_block, 0)

    wkv_copy.wait()
    kv_own = jnp.dot(normed[...], wkv[...], preferred_element_type=jnp.float32) + bkv_ref[...].astype(jnp.float32)
    kv_own = kv_own.astype(jnp.bfloat16)
    kv_all[pl.ds(my, 1)] = kv_own[None]
    seg_all[pl.ds(my, 1)] = seg_ref[...][None]
    k_ref[...] = kv_own[:, :HEAD_DIM]
    v_ref[...] = kv_own[:, HEAD_DIM:]

    pl.semaphore_wait(barrier, n_cp)

    def kv_copies(src, dst):
        return (pltpu.make_async_remote_copy(src_ref=kv_all.at[src], dst_ref=kv_all.at[src], send_sem=kv_send.at[dst],
                                             recv_sem=kv_recv.at[src], device_id={'cp': dst}, device_id_type=MESH),
                pltpu.make_async_remote_copy(src_ref=seg_ref, dst_ref=seg_all.at[src], send_sem=seg_send.at[dst],
                                             recv_sem=seg_recv.at[src], device_id={'cp': dst}, device_id_type=MESH))

    for dst in range(1, n_cp):
        @pl.when(my < dst)
        def _():
            for copy in kv_copies(my, dst):
                copy.start()

    def tile_copy(t):
        return pltpu.make_async_remote_copy(src_ref=send.at[t], dst_ref=recv.at[t], send_sem=tp_send.at[t],
                                            recv_sem=tp_recv.at[t], device_id={'tp': partner}, device_id_type=MESH)

    def chunk(c, carry):
        base = c * items
        rows = pl.ds(pl.multiple_of(c * ROWS, ROWS), ROWS)

        def q_tile(j, carry):
            acc = None
            for half in range(k_halves):
                g = base + j * k_halves + half
                slot = w_wait(g)
                part = jnp.dot(normed[rows, half * TILE_K:(half + 1) * TILE_K], wbuf[slot], preferred_element_type=jnp.float32)
                acc = part if acc is None else acc + part
                w_next(g)
            cols = pl.ds(pl.multiple_of(j * TILE_N, TILE_N), TILE_N)
            qbuf[:, cols] = (acc + bq_ref[:, cols].astype(jnp.float32)).astype(jnp.bfloat16)
            return carry

        lax.fori_loop(0, q_tiles, q_tile, 0)

        @pl.when(c == 0)
        def _():
            for src in range(n_cp - 1):
                @pl.when(src < my)
                def _():
                    for copy in kv_copies(src, src):
                        copy.wait_recv()

        seg_q = jnp.broadcast_to(seg_ref[pl.ds(c, 1), :].astype(jnp.float32), (ROWS, ROWS)).T
        q_pos = my * tok + c * ROWS + lax.broadcasted_iota(jnp.int32, (ROWS, 128), 0)
        lane = lax.broadcasted_iota(jnp.int32, (ROWS, 128), 1)
        for b in range(n_cp * tok // 128):
            src, part = b * 128 // tok, b % (tok // 128)

            @pl.when(src <= my)
            def _():
                seg_k = seg_all[src, part:part + 1, :].astype(jnp.float32)
                seen = (seg_q == seg_k) & (lane + b * 128 <= q_pos)
                mask[:, b * 128:(b + 1) * 128] = jnp.where(seen, 0.0, -jnp.inf)

        def head_pair(p, carry):
            q_two = qbuf[:, pl.ds(pl.multiple_of(p * 256, 256), 256)]
            q_rows = jnp.concatenate([q_two[:, :HEAD_DIM], q_two[:, HEAD_DIM:]], axis=0)
            for nb in range(1, n_cp + 1):
                @pl.when(my == nb - 1)
                def _():
                    keys = nb * tok
                    k_blk = kv_all[0:nb, :, :HEAD_DIM].reshape(keys, HEAD_DIM)
                    v_blk = kv_all[0:nb, :, HEAD_DIM:].reshape(keys, HEAD_DIM)
                    s = lax.dot_general(q_rows, k_blk, (((1,), (1,)), ((), ())), preferred_element_type=jnp.float32)
                    s = s.reshape(2, ROWS, keys) + mask[:, :keys][None]
                    p_wts = jnp.exp2((s - jnp.max(s, axis=-1, keepdims=True)) * EXP2_SCALE)
                    l_sum = jnp.sum(p_wts, axis=-1, keepdims=True).reshape(2 * ROWS, 1)
                    o = jnp.dot(p_wts.reshape(2 * ROWS, keys).astype(jnp.bfloat16), v_blk, preferred_element_type=jnp.float32)
                    o = (o / l_sum).astype(jnp.bfloat16)
                    obuf[:, pl.ds(pl.multiple_of(p * 256, 256), 256)] = jnp.concatenate([o[:ROWS], o[ROWS:]], axis=1)
            return carry

        lax.fori_loop(0, q_width // 256, head_pair, 0)

        def o_tile(n, carry):
            g = base + q_items + n
            slot = w_wait(g)
            t = c * o_tiles + n
            send[t] = jnp.dot(obuf[...], wbuf[slot], preferred_element_type=jnp.float32).astype(jnp.bfloat16)
            tile_copy(t).start()
            w_next(g)
            return carry

        lax.fori_loop(0, o_tiles, o_tile, 0)
        return carry

    lax.fori_loop(0, n_chunk, chunk, 0)

    for dst in range(1, n_cp):
        @pl.when(my < dst)
        def _():
            for copy in kv_copies(my, dst):
                copy.wait_send()

    def finish(t, carry):
        copy = tile_copy(t)
        copy.wait_recv()
        copy.wait_send()
        rows = pl.ds(pl.multiple_of(lax.div(t, o_tiles) * ROWS, ROWS), ROWS)
        cols = pl.ds(pl.multiple_of(lax.rem(t, o_tiles) * TILE_N, TILE_N), TILE_N)
        both = send[t].astype(jnp.float32) + recv[t].astype(jnp.float32)
        y_ref[rows, cols] = (y_ref[rows, cols].astype(jnp.float32) + both + bo_ref[:, cols].astype(jnp.float32)).astype(jnp.bfloat16)
        return carry

    lax.fori_loop(0, n_chunk * o_tiles, finish, 0)


def solution(mesh):
    n_cp = mesh.shape['cp']

    def local_block(hidden, seg_ids, w_q, b_q, w_kv, b_kv, w_o, b_o, ln_gain, ln_bias):
        tok, d_model = hidden.shape
        q_width = w_q.shape[1]
        n_tiles = (tok // ROWS) * (d_model // TILE_N)
        vmem = pl.BlockSpec(memory_space=pltpu.VMEM)
        hbm = pl.BlockSpec(memory_space=pl.ANY)
        bf16, f32 = jnp.bfloat16, jnp.float32
        dma = pltpu.SemaphoreType.DMA
        flops = 2 * tok * d_model * (2 * q_width + 256)
        y, k, v = pl.pallas_call(
            functools.partial(block_kernel, n_cp),
            out_shape=(jax.ShapeDtypeStruct((tok, d_model), bf16),
                       jax.ShapeDtypeStruct((tok, HEAD_DIM), bf16),
                       jax.ShapeDtypeStruct((tok, HEAD_DIM), bf16)),
            in_specs=[hbm, vmem, hbm, vmem, hbm, vmem, hbm, vmem, vmem, vmem],
            out_specs=(vmem, vmem, vmem),
            scratch_shapes=[
                pltpu.VMEM((tok, d_model), bf16),
                pltpu.VMEM((d_model, 2 * HEAD_DIM), bf16),
                pltpu.VMEM((SLOTS, TILE_K, TILE_N), bf16),
                pltpu.VMEM((n_cp, tok, 2 * HEAD_DIM), bf16),
                pltpu.VMEM((n_cp, tok // 128, 128), jnp.int32),
                pltpu.VMEM((ROWS, n_cp * tok), f32),
                pltpu.VMEM((ROWS, q_width), bf16),
                pltpu.VMEM((ROWS, q_width), bf16),
                pltpu.VMEM((n_tiles, ROWS, TILE_N), bf16),
                pltpu.VMEM((n_tiles, ROWS, TILE_N), bf16),
                dma((tok // LN_ROWS,)), dma, dma((SLOTS,)),
                dma((n_cp,)), dma((n_cp,)), dma((n_cp,)), dma((n_cp,)),
                dma((n_tiles,)), dma((n_tiles,)),
            ],
            compiler_params=pltpu.CompilerParams(collective_id=0, has_side_effects=True, vmem_limit_bytes=62 * 1024 * 1024),
            cost_estimate=pl.CostEstimate(flops=flops, bytes_accessed=2 * 4 * d_model * q_width, transcendentals=0),
        )(hidden, seg_ids.reshape(tok // 128, 128), w_q, b_q.reshape(1, -1), w_kv, b_kv.reshape(1, -1), w_o,
          b_o.reshape(1, -1), ln_gain.reshape(1, -1), ln_bias.reshape(1, -1))
        return y, k, v

    row_spec = P(('dp', 'cp'), None)
    tok_spec = P(('dp', 'cp'))
    return jax.shard_map(local_block, mesh=mesh,
                         in_specs=(row_spec, tok_spec, P(None, 'tp'), P('tp'), P(None, None), P(None), P('tp', None), P(None), P(None), P(None)),
                         out_specs=(row_spec, row_spec, row_spec), check_vma=False)
```

```python
import functools

import jax
import jax.numpy as jnp
from jax import lax
from jax.experimental import pallas as pl
from jax.experimental.pallas import tpu as pltpu
from jax.sharding import PartitionSpec as P

HEAD_DIM = 128
LN_EPS = 1e-5
EXP2_SCALE = HEAD_DIM ** -0.5 * 1.4426950408889634
MESH = pl.DeviceIdType.MESH

ROWS = 128
TILE_K = 3072
TILE_N = 512
SLOTS = 10
LAG = 3
LN_ROWS = 32


def block_kernel(n_cp, hid_hbm, seg_hbm, wq_hbm, bq_hbm, wkv_hbm, bkv_hbm, wo_hbm, bo_hbm, gain_hbm, bias_hbm,
                 y_ref, k_ref, v_ref,
                 normed, wkv, wbuf, kv_all, seg_all, mask, qbuf, obuf, send, recv,
                 bq_raw, bkv_raw, bo_raw, gain_raw, bias_raw, bq, bkv, bo, gain, bias,
                 hid_sem, wkv_sem, small_sem, w_sem, kv_send, kv_recv, seg_send, seg_recv, tp_send, tp_recv):
    my = lax.axis_index('cp')
    partner = 1 - lax.axis_index('tp')
    tok, d_model = y_ref.shape
    q_width = qbuf.shape[1]
    n_chunk = tok // ROWS
    q_tiles = q_width // TILE_N
    k_halves = d_model // TILE_K
    o_tiles = d_model // TILE_N
    q_items = q_tiles * k_halves
    items = q_items + o_tiles
    total = n_chunk * items
    f32, bf16 = jnp.float32, jnp.bfloat16

    def hid_copy(i):
        rows = pl.ds(i * LN_ROWS, LN_ROWS)
        return pltpu.make_async_copy(hid_hbm.at[rows, :], y_ref.at[rows, :], hid_sem.at[i])

    def w_issue(g):
        slot = lax.rem(g, SLOTS)
        item = lax.rem(g, items)

        @pl.when(item < q_items)
        def _():
            col = pl.multiple_of(lax.div(item, k_halves) * TILE_N, TILE_N)
            row = pl.multiple_of(lax.rem(item, k_halves) * TILE_K, TILE_K)
            pltpu.make_async_copy(wq_hbm.at[pl.ds(row, TILE_K), pl.ds(col, TILE_N)], wbuf.at[slot], w_sem.at[slot]).start()

        @pl.when(item >= q_items)
        def _():
            col = pl.multiple_of((item - q_items) * TILE_N, TILE_N)
            pltpu.make_async_copy(wo_hbm.at[:, pl.ds(col, TILE_N)], wbuf.at[slot], w_sem.at[slot]).start()

    def w_wait(g):
        slot = lax.rem(g, SLOTS)
        pltpu.make_async_copy(wo_hbm.at[:, pl.ds(0, TILE_N)], wbuf.at[slot], w_sem.at[slot]).wait()
        return slot

    def w_next(g):
        @pl.when(g + SLOTS < total)
        def _():
            w_issue(g + SLOTS)

    n_ln = tok // LN_ROWS
    hid_copy(0).start()
    small = [pltpu.make_async_copy(src, dst, small_sem.at[i]) for i, (src, dst) in enumerate((
        (gain_hbm, gain_raw), (bias_hbm, bias_raw), (bkv_hbm, bkv_raw), (bq_hbm, bq_raw), (bo_hbm, bo_raw), (seg_hbm, seg_all.at[my])))]
    for copy in small:
        copy.start()
    for i in range(1, n_ln):
        hid_copy(i).start()
    wkv_copy = pltpu.make_async_copy(wkv_hbm, wkv, wkv_sem)
    wkv_copy.start()
    for g in range(SLOTS - n_ln):
        w_issue(jnp.int32(g))

    barrier = pltpu.get_barrier_semaphore()
    for step in range(1, n_cp):
        pl.semaphore_signal(barrier, inc=1, device_id={'cp': lax.rem(my + step, n_cp)}, device_id_type=MESH)
    pl.semaphore_signal(barrier, inc=1, device_id={'tp': partner}, device_id_type=MESH)

    for copy in small:
        copy.wait()
    gain[...] = gain_raw[...].astype(f32)
    bias[...] = bias_raw[...].astype(f32)
    bkv[...] = bkv_raw[...].astype(f32)
    bq[...] = bq_raw[...].astype(f32)
    bo[...] = bo_raw[...].astype(f32)

    def ln_block(i, carry):
        hid_copy(i).wait()
        w_issue(i + SLOTS - n_ln)
        rows = pl.ds(pl.multiple_of(i * LN_ROWS, LN_ROWS), LN_ROWS)
        n_col = d_model // 128

        def load(j):
            return y_ref[rows, j * 128:(j + 1) * 128].astype(f32)

        accs = [load(j) for j in range(4)]
        for j in range(4, n_col):
            accs[j % 4] = accs[j % 4] + load(j)
        mean = jnp.sum((accs[0] + accs[1]) + (accs[2] + accs[3]), axis=-1, keepdims=True) * (1.0 / d_model)
        mean = jnp.broadcast_to(mean, (LN_ROWS, 128))
        accs = [None] * 4
        for j in range(n_col):
            cen = load(j) - mean
            accs[j % 4] = cen * cen if accs[j % 4] is None else accs[j % 4] + cen * cen
        var = jnp.sum((accs[0] + accs[1]) + (accs[2] + accs[3]), axis=-1, keepdims=True) * (1.0 / d_model)
        rstd = jnp.broadcast_to(lax.rsqrt(var + LN_EPS), (LN_ROWS, 128))
        for j in range(n_col):
            out = (load(j) - mean) * rstd * gain[j:j + 1, :] + bias[j:j + 1, :]
            normed[rows, j * 128:(j + 1) * 128] = out.astype(bf16)
        return carry

    def kv_copy(src, h, dst):
        rows = pl.ds(pl.multiple_of(h * ROWS, ROWS), ROWS)
        return pltpu.make_async_remote_copy(src_ref=kv_all.at[src, rows, :], dst_ref=kv_all.at[src, rows, :],
                                            send_sem=kv_send.at[dst, h], recv_sem=kv_recv.at[src, h],
                                            device_id={'cp': dst}, device_id_type=MESH)

    def seg_copy(src, dst):
        return pltpu.make_async_remote_copy(src_ref=seg_all.at[src], dst_ref=seg_all.at[src], send_sem=seg_send.at[dst],
                                            recv_sem=seg_recv.at[src], device_id={'cp': dst}, device_id_type=MESH)

    ln_half = n_ln // n_chunk

    def kv_half(h, carry):
        lax.fori_loop(h * ln_half, (h + 1) * ln_half, ln_block, 0)
        rows = pl.ds(pl.multiple_of(h * ROWS, ROWS), ROWS)

        @pl.when(h == 0)
        def _():
            wkv_copy.wait()

        part = jnp.dot(normed[rows, :], wkv[...], preferred_element_type=f32)
        k_own = (part[:, :HEAD_DIM] + bkv[0:1, :]).astype(bf16)
        v_own = (part[:, HEAD_DIM:] + bkv[1:2, :]).astype(bf16)
        kv_all[pl.ds(my, 1), rows, :HEAD_DIM] = k_own[None]
        kv_all[pl.ds(my, 1), rows, HEAD_DIM:] = v_own[None]
        k_ref[rows, :] = k_own
        v_ref[rows, :] = v_own

        @pl.when(h == 0)
        def _():
            pl.semaphore_wait(barrier, n_cp)
            for dst in range(1, n_cp):
                @pl.when(my < dst)
                def _():
                    seg_copy(my, dst).start()

        for dst in range(1, n_cp):
            @pl.when(my < dst)
            def _():
                kv_copy(my, h, dst).start()
        return carry

    lax.fori_loop(0, n_chunk, kv_half, 0)

    def tile_copy(t):
        return pltpu.make_async_remote_copy(src_ref=send.at[t], dst_ref=recv.at[t], send_sem=tp_send.at[t],
                                            recv_sem=tp_recv.at[t], device_id={'tp': partner}, device_id_type=MESH)

    def chunk(c, carry):
        base = c * items
        rows = pl.ds(pl.multiple_of(c * ROWS, ROWS), ROWS)

        def q_tile(j):
            acc = None
            for half in range(k_halves):
                g = base + j * k_halves + half
                slot = w_wait(g)
                part = jnp.dot(normed[rows, half * TILE_K:(half + 1) * TILE_K], wbuf[slot], preferred_element_type=f32)
                acc = part if acc is None else acc + part
                w_next(g)
            for i in range(TILE_N // 128):
                cols = pl.ds(pl.multiple_of(j * TILE_N + i * 128, 128), 128)
                row = j * (TILE_N // 128) + i
                qbuf[:, cols] = (acc[:, i * 128:(i + 1) * 128] + bq[pl.ds(row, 1), :]).astype(bf16)

        def make_mask():
            @pl.when(c == 0)
            def _():
                for src in range(n_cp - 1):
                    @pl.when(src < my)
                    def _():
                        seg_copy(src, src).wait_recv()
                        for h in range(n_chunk):
                            kv_copy(src, h, src).wait_recv()

            seg_q = jnp.broadcast_to(seg_all[my, pl.ds(c, 1), :].astype(f32), (ROWS, ROWS)).T
            q_pos = my * tok + c * ROWS + lax.broadcasted_iota(jnp.int32, (ROWS, 128), 0)
            lane = lax.broadcasted_iota(jnp.int32, (ROWS, 128), 1)
            for b in range(n_cp * tok // 128):
                src, part = b * 128 // tok, b % (tok // 128)

                @pl.when(src <= my)
                def _():
                    seg_k = seg_all[src, part:part + 1, :].astype(f32)
                    seen = (seg_q == seg_k) & (lane + b * 128 <= q_pos)
                    mask[:, b * 128:(b + 1) * 128] = jnp.where(seen, 0.0, -jnp.inf)

        def head_pair(p, carry):
            q_two = qbuf[:, pl.ds(pl.multiple_of(p * 256, 256), 256)]
            q_rows = jnp.concatenate([q_two[:, :HEAD_DIM], q_two[:, HEAD_DIM:]], axis=0)
            for nb in range(1, n_cp * n_chunk + 1):
                @pl.when(my * n_chunk + c == nb - 1)
                def _():
                    keys = nb * ROWS
                    full = -(-keys // tok)
                    k_blk = kv_all[0:full, :, :HEAD_DIM].reshape(full * tok, HEAD_DIM)[:keys]
                    v_blk = kv_all[0:full, :, HEAD_DIM:].reshape(full * tok, HEAD_DIM)[:keys]
                    s = lax.dot_general(q_rows, k_blk, (((1,), (1,)), ((), ())), preferred_element_type=f32)
                    s = s.reshape(2, ROWS, keys) + mask[:, :keys][None]
                    p_wts = jnp.exp2((s - jnp.max(s, axis=-1, keepdims=True)) * EXP2_SCALE)
                    l_sum = jnp.sum(p_wts, axis=-1, keepdims=True).reshape(2 * ROWS, 1)
                    o = jnp.dot(p_wts.reshape(2 * ROWS, keys).astype(bf16), v_blk, preferred_element_type=f32)
                    o = (o / l_sum).astype(bf16)
                    obuf[:, pl.ds(pl.multiple_of(p * 256, 256), 256)] = jnp.concatenate([o[:ROWS], o[ROWS:]], axis=1)
            return carry

        pairs = TILE_N // 256

        def stage(u, carry):
            @pl.when(u < q_tiles)
            def _():
                q_tile(u)

            @pl.when(u == LAG)
            def _():
                make_mask()

            @pl.when(u >= LAG)
            def _():
                lax.fori_loop((u - LAG) * pairs, (u - LAG + 1) * pairs, head_pair, 0)
            return carry

        lax.fori_loop(0, q_tiles + LAG, stage, 0)

        def o_tile(n, carry):
            g = base + q_items + n
            slot = w_wait(g)
            t = c * o_tiles + n
            send[t] = jnp.dot(obuf[...], wbuf[slot], preferred_element_type=f32).astype(bf16)
            tile_copy(t).start()
            w_next(g)
            return carry

        lax.fori_loop(0, o_tiles, o_tile, 0)
        return carry

    lax.fori_loop(0, n_chunk, chunk, 0)

    for dst in range(1, n_cp):
        @pl.when(my < dst)
        def _():
            seg_copy(my, dst).wait_send()
            for h in range(n_chunk):
                kv_copy(my, h, dst).wait_send()

    def finish(t, carry):
        copy = tile_copy(t)
        copy.wait_recv()
        copy.wait_send()
        n = lax.rem(t, o_tiles)
        rows = pl.ds(pl.multiple_of(lax.div(t, o_tiles) * ROWS, ROWS), ROWS)
        for i in range(TILE_N // 128):
            cols = pl.ds(pl.multiple_of(n * TILE_N + i * 128, 128), 128)
            part = slice(i * 128, (i + 1) * 128)
            both = send[t, :, part].astype(f32) + recv[t, :, part].astype(f32)
            y_ref[rows, cols] = (y_ref[rows, cols].astype(f32) + both + bo[pl.ds(n * (TILE_N // 128) + i, 1), :]).astype(bf16)
        return carry

    lax.fori_loop(0, n_chunk * o_tiles, finish, 0)


def solution(mesh):
    n_cp = mesh.shape['cp']

    def local_block(hidden, seg_ids, w_q, b_q, w_kv, b_kv, w_o, b_o, ln_gain, ln_bias):
        tok, d_model = hidden.shape
        q_width = w_q.shape[1]
        n_chunk = tok // ROWS
        n_tiles = n_chunk * (d_model // TILE_N)
        vmem = pl.BlockSpec(memory_space=pltpu.VMEM)
        hbm = pl.BlockSpec(memory_space=pltpu.HBM)
        bf16, f32 = jnp.bfloat16, jnp.float32
        dma = pltpu.SemaphoreType.DMA
        flops = 2 * tok * d_model * (2 * q_width + 256)
        args = (hidden, seg_ids.reshape(-1, 128), w_q, b_q.reshape(-1, 128), w_kv, b_kv.reshape(-1, 128), w_o,
                b_o.reshape(-1, 128), ln_gain.reshape(-1, 128), ln_bias.reshape(-1, 128))
        args = tuple(pltpu.with_memory_space_constraint(a, pltpu.HBM) for a in args)
        rows = [q_width // 128, 2, d_model // 128, d_model // 128, d_model // 128]
        return pl.pallas_call(
            functools.partial(block_kernel, n_cp),
            out_shape=(pltpu.VMEM((tok, d_model), bf16), pltpu.VMEM((tok, HEAD_DIM), bf16), pltpu.VMEM((tok, HEAD_DIM), bf16)),
            in_specs=[hbm] * len(args),
            out_specs=(vmem, vmem, vmem),
            scratch_shapes=[
                pltpu.VMEM((tok, d_model), bf16),
                pltpu.VMEM((d_model, 2 * HEAD_DIM), bf16),
                pltpu.VMEM((SLOTS, TILE_K, TILE_N), bf16),
                pltpu.VMEM((n_cp, tok, 2 * HEAD_DIM), bf16),
                pltpu.VMEM((n_cp, tok // 128, 128), jnp.int32),
                pltpu.VMEM((ROWS, n_cp * tok), f32),
                pltpu.VMEM((ROWS, q_width), bf16),
                pltpu.VMEM((ROWS, q_width), bf16),
                pltpu.VMEM((n_tiles, ROWS, TILE_N), bf16),
                pltpu.VMEM((n_tiles, ROWS, TILE_N), bf16),
                *[pltpu.VMEM((r, 128), bf16) for r in rows],
                *[pltpu.VMEM((r, 128), f32) for r in rows],
                dma((tok // LN_ROWS,)), dma, dma((6,)), dma((SLOTS,)),
                dma((n_cp, n_chunk)), dma((n_cp, n_chunk)), dma((n_cp,)), dma((n_cp,)),
                dma((n_tiles,)), dma((n_tiles,)),
            ],
            compiler_params=pltpu.CompilerParams(collective_id=0, has_side_effects=True, vmem_limit_bytes=56 * 1024 * 1024),
            cost_estimate=pl.CostEstimate(flops=flops, bytes_accessed=2 * 4 * d_model * q_width, transcendentals=0),
        )(*args)

    row_spec = P(('dp', 'cp'), None)
    tok_spec = P(('dp', 'cp'))
    return jax.shard_map(local_block, mesh=mesh,
                         in_specs=(row_spec, tok_spec, P(None, 'tp'), P('tp'), P(None, None), P(None), P('tp', None), P(None), P(None), P(None)),
                         out_specs=(row_spec, row_spec, row_spec), check_vma=False)
```

```python
import functools

import jax
import jax.numpy as jnp
from jax import lax
from jax.experimental import pallas as pl
from jax.experimental.pallas import tpu as pltpu
from jax.sharding import PartitionSpec as P

HEAD_DIM = 128
LN_EPS = 1e-5
EXP2_SCALE = HEAD_DIM ** -0.5 * 1.4426950408889634
MESH = pl.DeviceIdType.MESH

CHUNKS = (96, 160)
HALF = 128
TILE_K = 3072
TILE_N = 512
SLOTS = 10
EARLY = 2
EARLY_TILES = 4
LAG = 3
LN_ROWS = 32


def block_kernel(n_cp, hid_hbm, seg_hbm, wq_hbm, bq_hbm, wkv_hbm, bkv_hbm, wo_hbm, bo_hbm, gain_hbm, bias_hbm,
                 y_ref, k_ref, v_ref,
                 normed, wkv, wbuf, kv_all, seg_all, seg_q, mask, qbuf, obuf, send0, send1, recv0, recv1,
                 bq_raw, bkv_raw, bo_raw, gain_raw, bias_raw, bq, bkv, bo, gain, bias,
                 hid_sem, wkv_sem, small_sem, w_sem, kv_send, kv_recv, seg_send, seg_recv, tp_send, tp_recv):
    my = lax.axis_index('cp')
    partner = 1 - lax.axis_index('tp')
    tok, d_model = y_ref.shape
    q_width = qbuf.shape[1]
    n_chunk = len(CHUNKS)
    n_half = tok // HALF
    send, recv = (send0, send1), (recv0, recv1)
    q_tiles = q_width // TILE_N
    k_halves = d_model // TILE_K
    o_tiles = d_model // TILE_N
    q_items = q_tiles * k_halves
    items = q_items + o_tiles
    total = n_chunk * items
    f32, bf16 = jnp.float32, jnp.bfloat16

    def hid_copy(i):
        rows = pl.ds(i * LN_ROWS, LN_ROWS)
        return pltpu.make_async_copy(hid_hbm.at[rows, :], y_ref.at[rows, :], hid_sem.at[i])

    def w_issue(g):
        slot = lax.rem(g, SLOTS)
        item = lax.rem(g, items)

        @pl.when(item < q_items)
        def _():
            col = pl.multiple_of(lax.div(item, k_halves) * TILE_N, TILE_N)
            row = pl.multiple_of(lax.rem(item, k_halves) * TILE_K, TILE_K)
            pltpu.make_async_copy(wq_hbm.at[pl.ds(row, TILE_K), pl.ds(col, TILE_N)], wbuf.at[slot], w_sem.at[slot]).start()

        @pl.when(item >= q_items)
        def _():
            col = pl.multiple_of((item - q_items) * TILE_N, TILE_N)
            pltpu.make_async_copy(wo_hbm.at[:, pl.ds(col, TILE_N)], wbuf.at[slot], w_sem.at[slot]).start()

    def w_wait(g):
        slot = lax.rem(g, SLOTS)
        pltpu.make_async_copy(wo_hbm.at[:, pl.ds(0, TILE_N)], wbuf.at[slot], w_sem.at[slot]).wait()
        return slot

    def w_next(g):
        @pl.when(g + SLOTS < total)
        def _():
            w_issue(g + SLOTS)

    n_ln = tok // LN_ROWS
    ln_half = n_ln // n_half
    hid_copy(0).start()
    small = [pltpu.make_async_copy(src, dst, small_sem.at[i]) for i, (src, dst) in enumerate((
        (gain_hbm, gain_raw), (bias_hbm, bias_raw), (bkv_hbm, bkv_raw), (bq_hbm, bq_raw), (bo_hbm, bo_raw), (seg_hbm, seg_all.at[my])))]
    for copy in small:
        copy.start()
    for i in range(1, n_ln):
        hid_copy(i).start()
    wkv_copy = pltpu.make_async_copy(wkv_hbm, wkv, wkv_sem)
    wkv_copy.start()
    for g in range(SLOTS - n_ln):
        w_issue(jnp.int32(g))

    barrier = pltpu.get_barrier_semaphore()
    for step in range(1, n_cp):
        pl.semaphore_signal(barrier, inc=1, device_id={'cp': lax.rem(my + step, n_cp)}, device_id_type=MESH)
    pl.semaphore_signal(barrier, inc=1, device_id={'tp': partner}, device_id_type=MESH)

    with jax.named_scope("small"):
        for copy in small:
            copy.wait()
    gain[...] = gain_raw[...].astype(f32)
    bias[...] = bias_raw[...].astype(f32)
    bkv[...] = bkv_raw[...].astype(f32)
    bq[...] = bq_raw[...].astype(f32)
    bo[...] = bo_raw[...].astype(f32)

    def ln_block(i, carry):
        with jax.named_scope("hidwait"):
            hid_copy(i).wait()

        @pl.when(i < ln_half)
        def _():
            for more in range(n_half):
                w_issue((i - ln_half) * n_half + more + SLOTS)

        rows = pl.ds(pl.multiple_of(i * LN_ROWS, LN_ROWS), LN_ROWS)
        n_col = d_model // 128

        def load(j):
            return y_ref[rows, j * 128:(j + 1) * 128].astype(f32)

        accs = [load(j) for j in range(4)]
        for j in range(4, n_col):
            accs[j % 4] = accs[j % 4] + load(j)
        mean = jnp.sum((accs[0] + accs[1]) + (accs[2] + accs[3]), axis=-1, keepdims=True) * (1.0 / d_model)
        mean = jnp.broadcast_to(mean, (LN_ROWS, 128))
        accs = [None] * 4
        for j in range(n_col):
            cen = load(j) - mean
            accs[j % 4] = cen * cen if accs[j % 4] is None else accs[j % 4] + cen * cen
        var = jnp.sum((accs[0] + accs[1]) + (accs[2] + accs[3]), axis=-1, keepdims=True) * (1.0 / d_model)
        rstd = jnp.broadcast_to(lax.rsqrt(var + LN_EPS), (LN_ROWS, 128))
        for j in range(n_col):
            out = (load(j) - mean) * rstd * gain[j:j + 1, :] + bias[j:j + 1, :]
            normed[rows, j * 128:(j + 1) * 128] = out.astype(bf16)
        return carry

    def kv_copy(src, h, dst):
        rows = pl.ds(h * HALF, HALF)
        return pltpu.make_async_remote_copy(src_ref=kv_all.at[src, rows, :], dst_ref=kv_all.at[src, rows, :],
                                            send_sem=kv_send.at[dst, h], recv_sem=kv_recv.at[src, h],
                                            device_id={'cp': dst}, device_id_type=MESH)

    def seg_copy(src, dst):
        return pltpu.make_async_remote_copy(src_ref=seg_all.at[src], dst_ref=seg_all.at[src], send_sem=seg_send.at[dst],
                                            recv_sem=seg_recv.at[src], device_id={'cp': dst}, device_id_type=MESH)

    def kv_half(h):
        with jax.named_scope("ln"):
            lax.fori_loop(h * ln_half, (h + 1) * ln_half, ln_block, 0)
        rows = pl.ds(h * HALF, HALF)
        if h == 0:
            wkv_copy.wait()
        with jax.named_scope("kvdot"):
            part = jnp.dot(normed[rows, :], wkv[...], preferred_element_type=f32)
            k_own = (part[:, :HEAD_DIM] + bkv[0:1, :]).astype(bf16)
            v_own = (part[:, HEAD_DIM:] + bkv[1:2, :]).astype(bf16)
            kv_all[pl.ds(my, 1), rows, :HEAD_DIM] = k_own[None]
            kv_all[pl.ds(my, 1), rows, HEAD_DIM:] = v_own[None]
            k_ref[rows, :] = k_own
            v_ref[rows, :] = v_own
        if h == 0:
            with jax.named_scope("barrier"):
                pl.semaphore_wait(barrier, n_cp)
            for dst in range(1, n_cp):
                @pl.when(my < dst)
                def _():
                    seg_copy(my, dst).start()

        for dst in range(1, n_cp):
            @pl.when(my < dst)
            def _():
                kv_copy(my, h, dst).start()

    kv_half(0)

    @pl.when(my < EARLY)
    def _():
        for h in range(1, n_half):
            kv_half(h)

    for part in range(tok // 128):
        seg_q[part * 128:(part + 1) * 128, :] = jnp.broadcast_to(seg_all[my, part:part + 1, :].astype(f32), (128, 128)).T

    def tile_copy(c, n):
        return pltpu.make_async_remote_copy(src_ref=send[c].at[n], dst_ref=recv[c].at[n], send_sem=tp_send.at[c, n],
                                            recv_sem=tp_recv.at[c, n], device_id={'tp': partner}, device_id_type=MESH)

    def chunk(c):
        base = c * items
        n_row = CHUNKS[c]
        first = sum(CHUNKS[:c])
        rows = slice(first, first + n_row)

        def q_tile(j):
            acc = None
            for half in range(k_halves):
                g = base + j * k_halves + half
                slot = w_wait(g)
                part = jnp.dot(normed[rows, half * TILE_K:(half + 1) * TILE_K], wbuf[slot], preferred_element_type=f32)
                acc = part if acc is None else acc + part
                w_next(g)
            for i in range(TILE_N // 128):
                cols = pl.ds(pl.multiple_of(j * TILE_N + i * 128, 128), 128)
                row = j * (TILE_N // 128) + i
                qbuf[:n_row, cols] = (acc[:, i * 128:(i + 1) * 128] + bq[pl.ds(row, 1), :]).astype(bf16)

        def make_mask():
            if c == 0:
                for src in range(n_cp - 1):
                    @pl.when(src < my)
                    def _():
                        seg_copy(src, src).wait_recv()
                        for h in range(n_half):
                            kv_copy(src, h, src).wait_recv()

            q_pos = my * tok + first + lax.broadcasted_iota(jnp.int32, (n_row, 128), 0)
            lane = lax.broadcasted_iota(jnp.int32, (n_row, 128), 1)
            for b in range(n_cp * tok // 128):
                src, part = b * 128 // tok, b % (tok // 128)

                @pl.when(src <= my)
                def _():
                    seg_k = seg_all[src, part:part + 1, :].astype(f32)
                    seen = (seg_q[rows, :] == seg_k) & (lane + b * 128 <= q_pos)
                    mask[:n_row, b * 128:(b + 1) * 128] = jnp.where(seen, 0.0, -jnp.inf)

        own_keys = -(-(first + n_row) // 128) * 128

        def heads(j):
            cols = pl.ds(pl.multiple_of(j * TILE_N, TILE_N), TILE_N)
            for nb in range(n_cp):
                @pl.when(my == nb)
                def _():
                    keys = nb * tok + own_keys
                    k_blk = kv_all[0:nb + 1, :, :HEAD_DIM].reshape((nb + 1) * tok, HEAD_DIM)[:keys]
                    v_blk = kv_all[0:nb + 1, :, HEAD_DIM:].reshape((nb + 1) * tok, HEAD_DIM)[:keys]
                    q_cols = qbuf[:n_row, cols]
                    outs = []
                    for pair in range(TILE_N // 256):
                        q_rows = jnp.concatenate([q_cols[:, (2 * pair + i) * HEAD_DIM:(2 * pair + i + 1) * HEAD_DIM] for i in range(2)], axis=0)
                        s = lax.dot_general(q_rows, k_blk, (((1,), (1,)), ((), ())), preferred_element_type=f32)
                        s = s.reshape(2, n_row, keys) + mask[:n_row, :keys][None]
                        p_wts = jnp.exp2((s - jnp.max(s, axis=-1, keepdims=True)) * EXP2_SCALE)
                        l_sum = jnp.sum(p_wts, axis=-1, keepdims=True).reshape(2 * n_row, 1)
                        o = jnp.dot(p_wts.reshape(2 * n_row, keys).astype(bf16), v_blk, preferred_element_type=f32)
                        o = (o / l_sum).astype(bf16)
                        outs += [o[:n_row], o[n_row:]]
                    obuf[:n_row, cols] = jnp.concatenate(outs, axis=1)

        def stage(u, carry):
            @pl.when(u < q_tiles)
            def _():
                with jax.named_scope("qtile"):
                    q_tile(u)

            @pl.when(u == LAG)
            def _():
                with jax.named_scope("mask"):
                    make_mask()

            @pl.when(u >= LAG)
            def _():
                with jax.named_scope("attn"):
                    heads(u - LAG)
            return carry

        lax.fori_loop(0, q_tiles + LAG, stage, 0)

        def o_tile(n, carry):
            with jax.named_scope("otile"):
                g = base + q_items + n
                slot = w_wait(g)
                send[c][n] = jnp.dot(obuf[:n_row, :], wbuf[slot], preferred_element_type=f32).astype(bf16)
                tile_copy(c, n).start()
                w_next(g)
            return carry

        if c == 0:
            lax.fori_loop(0, EARLY_TILES, o_tile, 0)

            @pl.when(my >= EARLY)
            def _():
                for h in range(1, n_half):
                    kv_half(h)

            lax.fori_loop(EARLY_TILES, o_tiles, o_tile, 0)
        else:
            lax.fori_loop(0, o_tiles, o_tile, 0)

    for c in range(n_chunk):
        chunk(c)

    for dst in range(1, n_cp):
        @pl.when(my < dst)
        def _():
            seg_copy(my, dst).wait_send()
            for h in range(n_half):
                kv_copy(my, h, dst).wait_send()

    for c in range(n_chunk):
        first = sum(CHUNKS[:c])
        rows = slice(first, first + CHUNKS[c])

        def finish(n, carry):
            copy = tile_copy(c, n)
            copy.wait_recv()
            copy.wait_send()
            for i in range(TILE_N // 128):
                cols = pl.ds(pl.multiple_of(n * TILE_N + i * 128, 128), 128)
                part = slice(i * 128, (i + 1) * 128)
                both = send[c][n, :, part].astype(f32) + recv[c][n, :, part].astype(f32)
                y_ref[rows, cols] = (y_ref[rows, cols].astype(f32) + both + bo[pl.ds(n * (TILE_N // 128) + i, 1), :]).astype(bf16)
            return carry

        with jax.named_scope("finish"):
            lax.fori_loop(0, o_tiles, finish, 0)


def close_kernel(y_ref, k_ref, v_ref, y_hbm, k_hbm, v_hbm, sem):
    rows = y_ref.shape[0] // 8
    copies = [pltpu.make_async_copy(k_ref, k_hbm, sem.at[8]), pltpu.make_async_copy(v_ref, v_hbm, sem.at[9])]
    copies += [pltpu.make_async_copy(y_ref.at[pl.ds(i * rows, rows), :], y_hbm.at[pl.ds(i * rows, rows), :], sem.at[i]) for i in range(8)]
    for copy in copies:
        copy.start()
    for copy in copies:
        copy.wait()


def solution(mesh):
    n_cp = mesh.shape['cp']

    def local_block(hidden, seg_ids, w_q, b_q, w_kv, b_kv, w_o, b_o, ln_gain, ln_bias):
        tok, d_model = hidden.shape
        q_width = w_q.shape[1]
        o_tiles = d_model // TILE_N
        vmem = pl.BlockSpec(memory_space=pltpu.VMEM)
        hbm = pl.BlockSpec(memory_space=pltpu.HBM)
        bf16, f32 = jnp.bfloat16, jnp.float32
        dma = pltpu.SemaphoreType.DMA
        flops = 2 * tok * d_model * (2 * q_width + 256)
        args = (hidden, seg_ids.reshape(-1, 128), w_q, b_q.reshape(-1, 128), w_kv, b_kv.reshape(-1, 128), w_o,
                b_o.reshape(-1, 128), ln_gain.reshape(-1, 128), ln_bias.reshape(-1, 128))
        args = tuple(pltpu.with_memory_space_constraint(a, pltpu.HBM) for a in args)
        rows = [q_width // 128, 2, d_model // 128, d_model // 128, d_model // 128]
        y, k, v = pl.pallas_call(
            functools.partial(block_kernel, n_cp),
            out_shape=(pltpu.VMEM((tok, d_model), bf16), pltpu.VMEM((tok, HEAD_DIM), bf16), pltpu.VMEM((tok, HEAD_DIM), bf16)),
            in_specs=[hbm] * len(args),
            out_specs=(vmem, vmem, vmem),
            scratch_shapes=[
                pltpu.VMEM((tok, d_model), bf16),
                pltpu.VMEM((d_model, 2 * HEAD_DIM), bf16),
                pltpu.VMEM((SLOTS, TILE_K, TILE_N), bf16),
                pltpu.VMEM((n_cp, tok, 2 * HEAD_DIM), bf16),
                pltpu.VMEM((n_cp, tok // 128, 128), jnp.int32),
                pltpu.VMEM((tok, 128), f32),
                pltpu.VMEM((max(CHUNKS), n_cp * tok), f32),
                pltpu.VMEM((max(CHUNKS), q_width), bf16),
                pltpu.VMEM((max(CHUNKS), q_width), bf16),
                *[pltpu.VMEM((o_tiles, r, TILE_N), bf16) for r in CHUNKS * 2],
                *[pltpu.VMEM((r, 128), bf16) for r in rows],
                *[pltpu.VMEM((r, 128), f32) for r in rows],
                dma((tok // LN_ROWS,)), dma, dma((6,)), dma((SLOTS,)),
                dma((n_cp, tok // HALF)), dma((n_cp, tok // HALF)), dma((n_cp,)), dma((n_cp,)),
                dma((len(CHUNKS), o_tiles)), dma((len(CHUNKS), o_tiles)),
            ],
            compiler_params=pltpu.CompilerParams(collective_id=0, has_side_effects=True, vmem_limit_bytes=56 * 1024 * 1024),
            cost_estimate=pl.CostEstimate(flops=flops, bytes_accessed=2 * 4 * d_model * q_width, transcendentals=0),
        )(*args)
        return pl.pallas_call(
            close_kernel,
            out_shape=tuple(jax.ShapeDtypeStruct(a.shape, bf16) for a in (y, k, v)),
            in_specs=[vmem] * 3,
            out_specs=(hbm,) * 3,
            scratch_shapes=[dma((10,))],
            cost_estimate=pl.CostEstimate(flops=1, bytes_accessed=4 * tok * d_model, transcendentals=0),
        )(*(pltpu.with_memory_space_constraint(a, pltpu.VMEM) for a in (y, k, v)))

    row_spec = P(('dp', 'cp'), None)
    tok_spec = P(('dp', 'cp'))
    return jax.shard_map(local_block, mesh=mesh,
                         in_specs=(row_spec, tok_spec, P(None, 'tp'), P('tp'), P(None, None), P(None), P('tp', None), P(None), P(None), P(None)),
                         out_specs=(row_spec, row_spec, row_spec), check_vma=False)
```

```python
import functools

import jax
import jax.numpy as jnp
from jax import lax
from jax.experimental import pallas as pl
from jax.experimental.pallas import tpu as pltpu
from jax.sharding import PartitionSpec as P

HEAD_DIM = 128
LN_EPS = 1e-5
EXP2_SCALE = HEAD_DIM ** -0.5 * 1.4426950408889634
MESH = pl.DeviceIdType.MESH

CHUNKS = (128, 128)
HALF = 128
TILE_K = 3072
TILE_N = 512
AHEAD = 3
SLOTS = 9
EARLY = 2
EARLY_TILES = 3
LAG = 3
LN_ROWS = 32


def block_kernel(n_cp, hid_hbm, seg_hbm, wq_hbm, bq_hbm, wkv_hbm, bkv_hbm, wo_hbm, bo_hbm, gain_hbm, bias_hbm,
                 y_ref, k_ref, v_ref,
                 normed, wkv, wbuf, kv_all, seg_all, seg_q, mask, qbuf, obuf, send0, send1, recv0, recv1,
                 bq_raw, bkv_raw, bo_raw, gain_raw, bias_raw, bq, bkv, bo, gain, bias,
                 hid_sem, wkv_sem, small_sem, w_sem, kv_send, kv_recv, seg_send, seg_recv, tp_send, tp_recv):
    my = lax.axis_index('cp')
    partner = 1 - lax.axis_index('tp')
    tok, d_model = y_ref.shape
    q_width = qbuf.shape[1]
    n_chunk = len(CHUNKS)
    n_half = tok // HALF
    send, recv = (send0, send1), (recv0, recv1)
    q_tiles = q_width // TILE_N
    k_halves = d_model // TILE_K
    o_tiles = d_model // TILE_N
    q_items = q_tiles * k_halves
    items = q_items + o_tiles
    total = n_chunk * items
    f32, bf16 = jnp.float32, jnp.bfloat16

    def hid_copy(i):
        rows = pl.ds(i * LN_ROWS, LN_ROWS)
        return pltpu.make_async_copy(hid_hbm.at[rows, :], y_ref.at[rows, :], hid_sem.at[i])

    def w_issue(g):
        slot = lax.rem(g, SLOTS)
        item = lax.rem(g, items)

        @pl.when(item < q_items)
        def _():
            col = pl.multiple_of(lax.div(item, k_halves) * TILE_N, TILE_N)
            row = pl.multiple_of(lax.rem(item, k_halves) * TILE_K, TILE_K)
            pltpu.make_async_copy(wq_hbm.at[pl.ds(row, TILE_K), pl.ds(col, TILE_N)], wbuf.at[slot], w_sem.at[slot]).start()

        @pl.when(item >= q_items)
        def _():
            col = pl.multiple_of((item - q_items) * TILE_N, TILE_N)
            pltpu.make_async_copy(wo_hbm.at[:, pl.ds(col, TILE_N)], wbuf.at[slot], w_sem.at[slot]).start()

    def w_wait(g):
        slot = lax.rem(g, SLOTS)
        pltpu.make_async_copy(wo_hbm.at[:, pl.ds(0, TILE_N)], wbuf.at[slot], w_sem.at[slot]).wait()
        return slot

    def w_next(g):
        @pl.when(g + SLOTS < total)
        def _():
            w_issue(g + SLOTS)

    n_ln = tok // LN_ROWS
    ln_half = n_ln // n_half
    small = [pltpu.make_async_copy(src, dst, small_sem.at[i]) for i, (src, dst) in enumerate((
        (gain_hbm, gain_raw), (bias_hbm, bias_raw), (bkv_hbm, bkv_raw), (bq_hbm, bq_raw), (bo_hbm, bo_raw), (seg_hbm, seg_all.at[my])))]
    wkv_copy = pltpu.make_async_copy(wkv_hbm, wkv, wkv_sem)
    hid_copy(0).start()
    for copy in small:
        copy.start()
    for i in range(1, n_ln):
        hid_copy(i).start()

    barrier = pltpu.get_barrier_semaphore()
    for step in range(1, n_cp):
        pl.semaphore_signal(barrier, inc=1, device_id={'cp': lax.rem(my + step, n_cp)}, device_id_type=MESH)
    pl.semaphore_signal(barrier, inc=1, device_id={'tp': partner}, device_id_type=MESH)

    with jax.named_scope("small"):
        for copy in small:
            copy.wait()
    gain[...] = gain_raw[...].astype(f32)
    bias[...] = bias_raw[...].astype(f32)
    bkv[...] = bkv_raw[...].astype(f32)
    bq[...] = bq_raw[...].astype(f32)
    bo[...] = bo_raw[...].astype(f32)

    def ln_block(i, carry):
        with jax.named_scope("hidwait"):
            hid_copy(i).wait()

        @pl.when(i == 0)
        def _():
            wkv_copy.start()

        @pl.when((i > 0) & (i < ln_half))
        def _():
            for more in range(AHEAD):
                w_issue((i - 1) * AHEAD + more)

        rows = pl.ds(pl.multiple_of(i * LN_ROWS, LN_ROWS), LN_ROWS)
        n_col = d_model // 128

        def load(j):
            return y_ref[rows, j * 128:(j + 1) * 128].astype(f32)

        accs = [load(j) for j in range(4)]
        for j in range(4, n_col):
            accs[j % 4] = accs[j % 4] + load(j)
        mean = jnp.sum((accs[0] + accs[1]) + (accs[2] + accs[3]), axis=-1, keepdims=True) * (1.0 / d_model)
        mean = jnp.broadcast_to(mean, (LN_ROWS, 128))
        accs = [None] * 4
        for j in range(n_col):
            cen = load(j) - mean
            accs[j % 4] = cen * cen if accs[j % 4] is None else accs[j % 4] + cen * cen
        var = jnp.sum((accs[0] + accs[1]) + (accs[2] + accs[3]), axis=-1, keepdims=True) * (1.0 / d_model)
        rstd = jnp.broadcast_to(lax.rsqrt(var + LN_EPS), (LN_ROWS, 128))
        for j in range(n_col):
            out = (load(j) - mean) * rstd * gain[j:j + 1, :] + bias[j:j + 1, :]
            normed[rows, j * 128:(j + 1) * 128] = out.astype(bf16)
        return carry

    def kv_copy(src, h, dst):
        rows = pl.ds(h * HALF, HALF)
        return pltpu.make_async_remote_copy(src_ref=kv_all.at[src, rows, :], dst_ref=kv_all.at[src, rows, :],
                                            send_sem=kv_send.at[dst, h], recv_sem=kv_recv.at[src, h],
                                            device_id={'cp': dst}, device_id_type=MESH)

    def seg_copy(src, dst):
        return pltpu.make_async_remote_copy(src_ref=seg_all.at[src], dst_ref=seg_all.at[src], send_sem=seg_send.at[dst],
                                            recv_sem=seg_recv.at[src], device_id={'cp': dst}, device_id_type=MESH)

    def kv_half(h):
        with jax.named_scope("ln"):
            lax.fori_loop(h * ln_half, (h + 1) * ln_half, ln_block, 0)
        rows = pl.ds(h * HALF, HALF)
        if h == 0:
            wkv_copy.wait()
        with jax.named_scope("kvdot"):
            part = jnp.dot(normed[rows, :], wkv[...], preferred_element_type=f32)
            k_own = (part[:, :HEAD_DIM] + bkv[0:1, :]).astype(bf16)
            v_own = (part[:, HEAD_DIM:] + bkv[1:2, :]).astype(bf16)
            kv_all[pl.ds(my, 1), rows, :HEAD_DIM] = k_own[None]
            kv_all[pl.ds(my, 1), rows, HEAD_DIM:] = v_own[None]
            k_ref[rows, :] = k_own
            v_ref[rows, :] = v_own
        if h == 0:
            with jax.named_scope("barrier"):
                pl.semaphore_wait(barrier, n_cp)
            for dst in range(1, n_cp):
                @pl.when(my < dst)
                def _():
                    seg_copy(my, dst).start()

        for dst in range(1, n_cp):
            @pl.when(my < dst)
            def _():
                kv_copy(my, h, dst).start()

    kv_half(0)

    @pl.when(my < EARLY)
    def _():
        for h in range(1, n_half):
            kv_half(h)

    for part in range(tok // 128):
        seg_q[part * 128:(part + 1) * 128, :] = jnp.broadcast_to(seg_all[my, part:part + 1, :].astype(f32), (128, 128)).T

    def tile_copy(c, n):
        return pltpu.make_async_remote_copy(src_ref=send[c].at[n], dst_ref=recv[c].at[n], send_sem=tp_send.at[c, n],
                                            recv_sem=tp_recv.at[c, n], device_id={'tp': partner}, device_id_type=MESH)

    def chunk(c):
        base = c * items
        n_row = CHUNKS[c]
        first = sum(CHUNKS[:c])
        rows = slice(first, first + n_row)

        def q_tile(j):
            acc = None
            for half in range(k_halves):
                g = base + j * k_halves + half
                slot = w_wait(g)
                part = jnp.dot(normed[rows, half * TILE_K:(half + 1) * TILE_K], wbuf[slot], preferred_element_type=f32)
                acc = part if acc is None else acc + part
                w_next(g)
            for i in range(TILE_N // 128):
                cols = pl.ds(pl.multiple_of(j * TILE_N + i * 128, 128), 128)
                row = j * (TILE_N // 128) + i
                qbuf[:n_row, cols] = (acc[:, i * 128:(i + 1) * 128] + bq[pl.ds(row, 1), :]).astype(bf16)

        def make_mask():
            if c == 0:
                for src in range(n_cp - 1):
                    @pl.when(src < my)
                    def _():
                        seg_copy(src, src).wait_recv()
                        for h in range(n_half):
                            kv_copy(src, h, src).wait_recv()

            q_pos = my * tok + first + lax.broadcasted_iota(jnp.int32, (n_row, 128), 0)
            lane = lax.broadcasted_iota(jnp.int32, (n_row, 128), 1)
            for b in range(n_cp * tok // 128):
                src, part = b * 128 // tok, b % (tok // 128)

                @pl.when(src <= my)
                def _():
                    seg_k = seg_all[src, part:part + 1, :].astype(f32)
                    seen = (seg_q[rows, :] == seg_k) & (lane + b * 128 <= q_pos)
                    mask[:n_row, b * 128:(b + 1) * 128] = jnp.where(seen, 0.0, -jnp.inf)

        own_keys = -(-(first + n_row) // 128) * 128

        def heads(j):
            cols = pl.ds(pl.multiple_of(j * TILE_N, TILE_N), TILE_N)
            for nb in range(n_cp):
                @pl.when(my == nb)
                def _():
                    keys = nb * tok + own_keys
                    k_blk = kv_all[0:nb + 1, :, :HEAD_DIM].reshape((nb + 1) * tok, HEAD_DIM)[:keys]
                    v_blk = kv_all[0:nb + 1, :, HEAD_DIM:].reshape((nb + 1) * tok, HEAD_DIM)[:keys]
                    q_cols = qbuf[:n_row, cols]
                    outs = []
                    for pair in range(TILE_N // 256):
                        q_rows = jnp.concatenate([q_cols[:, (2 * pair + i) * HEAD_DIM:(2 * pair + i + 1) * HEAD_DIM] for i in range(2)], axis=0)
                        s = lax.dot_general(q_rows, k_blk, (((1,), (1,)), ((), ())), preferred_element_type=f32)
                        s = s.reshape(2, n_row, keys) + mask[:n_row, :keys][None]
                        p_wts = jnp.exp2((s - jnp.max(s, axis=-1, keepdims=True)) * EXP2_SCALE)
                        l_sum = jnp.sum(p_wts, axis=-1, keepdims=True).reshape(2 * n_row, 1)
                        o = jnp.dot(p_wts.reshape(2 * n_row, keys).astype(bf16), v_blk, preferred_element_type=f32)
                        o = (o / l_sum).astype(bf16)
                        outs += [o[:n_row], o[n_row:]]
                    obuf[:n_row, cols] = jnp.concatenate(outs, axis=1)

        lag = jnp.where(my == n_cp - 1, q_tiles, LAG) if c == 0 else LAG

        def stage(u, carry):
            @pl.when(u < q_tiles)
            def _():
                with jax.named_scope("qtile"):
                    q_tile(u)

            @pl.when(u == lag)
            def _():
                with jax.named_scope("mask"):
                    make_mask()

            @pl.when(u >= lag)
            def _():
                with jax.named_scope("attn"):
                    heads(u - lag)
            return carry

        lax.fori_loop(0, q_tiles + lag, stage, 0)

        def o_tile(n, carry):
            with jax.named_scope("otile"):
                g = base + q_items + n
                slot = w_wait(g)
                send[c][n] = jnp.dot(obuf[:n_row, :], wbuf[slot], preferred_element_type=f32).astype(bf16)
                tile_copy(c, n).start()
                w_next(g)
            return carry

        if c == 0:
            lax.fori_loop(0, EARLY_TILES, o_tile, 0)

            @pl.when(my >= EARLY)
            def _():
                for h in range(1, n_half):
                    kv_half(h)

            lax.fori_loop(EARLY_TILES, o_tiles, o_tile, 0)
        else:
            lax.fori_loop(0, o_tiles, o_tile, 0)

    for c in range(n_chunk):
        chunk(c)

    for dst in range(1, n_cp):
        @pl.when(my < dst)
        def _():
            seg_copy(my, dst).wait_send()
            for h in range(n_half):
                kv_copy(my, h, dst).wait_send()

    for c in range(n_chunk):
        first = sum(CHUNKS[:c])
        rows = slice(first, first + CHUNKS[c])

        def finish(n, carry):
            copy = tile_copy(c, n)
            copy.wait_recv()
            copy.wait_send()
            for i in range(TILE_N // 128):
                cols = pl.ds(pl.multiple_of(n * TILE_N + i * 128, 128), 128)
                part = slice(i * 128, (i + 1) * 128)
                both = send[c][n, :, part].astype(f32) + recv[c][n, :, part].astype(f32)
                y_ref[rows, cols] = (y_ref[rows, cols].astype(f32) + both + bo[pl.ds(n * (TILE_N // 128) + i, 1), :]).astype(bf16)
            return carry

        with jax.named_scope("finish"):
            lax.fori_loop(0, o_tiles, finish, 0)


def close_kernel(y_ref, k_ref, v_ref, y_hbm, k_hbm, v_hbm, sem):
    rows = y_ref.shape[0] // 8
    copies = [pltpu.make_async_copy(k_ref, k_hbm, sem.at[8]), pltpu.make_async_copy(v_ref, v_hbm, sem.at[9])]
    copies += [pltpu.make_async_copy(y_ref.at[pl.ds(i * rows, rows), :], y_hbm.at[pl.ds(i * rows, rows), :], sem.at[i]) for i in range(8)]
    for copy in copies:
        copy.start()
    for copy in copies:
        copy.wait()


def solution(mesh):
    n_cp = mesh.shape['cp']

    def local_block(hidden, seg_ids, w_q, b_q, w_kv, b_kv, w_o, b_o, ln_gain, ln_bias):
        tok, d_model = hidden.shape
        q_width = w_q.shape[1]
        o_tiles = d_model // TILE_N
        vmem = pl.BlockSpec(memory_space=pltpu.VMEM)
        hbm = pl.BlockSpec(memory_space=pltpu.HBM)
        bf16, f32 = jnp.bfloat16, jnp.float32
        dma = pltpu.SemaphoreType.DMA
        flops = 2 * tok * d_model * (2 * q_width + 256)
        args = (hidden, seg_ids.reshape(-1, 128), w_q, b_q.reshape(-1, 128), w_kv, b_kv.reshape(-1, 128), w_o,
                b_o.reshape(-1, 128), ln_gain.reshape(-1, 128), ln_bias.reshape(-1, 128))
        args = tuple(pltpu.with_memory_space_constraint(a, pltpu.HBM) for a in args)
        rows = [q_width // 128, 2, d_model // 128, d_model // 128, d_model // 128]
        y, k, v = pl.pallas_call(
            functools.partial(block_kernel, n_cp),
            out_shape=(pltpu.VMEM((tok, d_model), bf16), pltpu.VMEM((tok, HEAD_DIM), bf16), pltpu.VMEM((tok, HEAD_DIM), bf16)),
            in_specs=[hbm] * len(args),
            out_specs=(vmem, vmem, vmem),
            scratch_shapes=[
                pltpu.VMEM((tok, d_model), bf16),
                pltpu.VMEM((d_model, 2 * HEAD_DIM), bf16),
                pltpu.VMEM((SLOTS, TILE_K, TILE_N), bf16),
                pltpu.VMEM((n_cp, tok, 2 * HEAD_DIM), bf16),
                pltpu.VMEM((n_cp, tok // 128, 128), jnp.int32),
                pltpu.VMEM((tok, 128), f32),
                pltpu.VMEM((max(CHUNKS), n_cp * tok), f32),
                pltpu.VMEM((max(CHUNKS), q_width), bf16),
                pltpu.VMEM((max(CHUNKS), q_width), bf16),
                *[pltpu.VMEM((o_tiles, r, TILE_N), bf16) for r in CHUNKS * 2],
                *[pltpu.VMEM((r, 128), bf16) for r in rows],
                *[pltpu.VMEM((r, 128), f32) for r in rows],
                dma((tok // LN_ROWS,)), dma, dma((6,)), dma((SLOTS,)),
                dma((n_cp, tok // HALF)), dma((n_cp, tok // HALF)), dma((n_cp,)), dma((n_cp,)),
                dma((len(CHUNKS), o_tiles)), dma((len(CHUNKS), o_tiles)),
            ],
            compiler_params=pltpu.CompilerParams(collective_id=0, has_side_effects=True, vmem_limit_bytes=56 * 1024 * 1024),
            cost_estimate=pl.CostEstimate(flops=flops, bytes_accessed=2 * 4 * d_model * q_width, transcendentals=0),
        )(*args)
        return pl.pallas_call(
            close_kernel,
            out_shape=tuple(jax.ShapeDtypeStruct(a.shape, bf16) for a in (y, k, v)),
            in_specs=[vmem] * 3,
            out_specs=(hbm,) * 3,
            scratch_shapes=[dma((10,))],
            cost_estimate=pl.CostEstimate(flops=1, bytes_accessed=4 * tok * d_model, transcendentals=0),
        )(*(pltpu.with_memory_space_constraint(a, pltpu.VMEM) for a in (y, k, v)))

    row_spec = P(('dp', 'cp'), None)
    tok_spec = P(('dp', 'cp'))
    return jax.shard_map(local_block, mesh=mesh,
                         in_specs=(row_spec, tok_spec, P(None, 'tp'), P('tp'), P(None, None), P(None), P('tp', None), P(None), P(None), P(None)),
                         out_specs=(row_spec, row_spec, row_spec), check_vma=False)
```

```python
import functools

import jax
import jax.numpy as jnp
from jax import lax
from jax.experimental import pallas as pl
from jax.experimental.pallas import tpu as pltpu
from jax.sharding import PartitionSpec as P

HEAD_DIM = 128
LN_EPS = 1e-5
EXP2_SCALE = HEAD_DIM ** -0.5 * 1.4426950408889634
MESH = pl.DeviceIdType.MESH

CHUNKS = (128, 128)
HALF = 128
TILE_K = 3072
TILE_N = 512
AHEAD = 3
SLOTS = 9
EARLY = 2
EARLY_TILES = 3
LAG = 3
LN_ROWS = 32


def block_kernel(n_cp, hid_hbm, seg_hbm, wq_hbm, bq_hbm, wkv_hbm, bkv_hbm, wo_hbm, bo_hbm, gain_hbm, bias_hbm,
                 y_ref, k_ref, v_ref,
                 normed, wkv, wbuf, kv_all, seg_all, below, mask, qbuf, obuf, send0, send1, recv0, recv1,
                 bq_raw, bkv_raw, bo_raw, gain_raw, bias_raw, bq, bkv, bo, gain, bias,
                 hid_sem, wkv_sem, small_sem, w_sem, kv_send, kv_recv, seg_send, seg_recv, tp_send, tp_recv):
    my = lax.axis_index('cp')
    partner = 1 - lax.axis_index('tp')
    tok, d_model = y_ref.shape
    q_width = qbuf.shape[1]
    n_chunk = len(CHUNKS)
    n_half = tok // HALF
    send, recv = (send0, send1), (recv0, recv1)
    q_tiles = q_width // TILE_N
    k_halves = d_model // TILE_K
    o_tiles = d_model // TILE_N
    q_items = q_tiles * k_halves
    items = q_items + o_tiles
    total = n_chunk * items
    f32, bf16 = jnp.float32, jnp.bfloat16

    def hid_copy(i):
        rows = pl.ds(i * LN_ROWS, LN_ROWS)
        return pltpu.make_async_copy(hid_hbm.at[rows, :], y_ref.at[rows, :], hid_sem.at[i])

    def w_issue(g):
        slot = lax.rem(g, SLOTS)
        item = lax.rem(g, items)

        @pl.when(item < q_items)
        def _():
            col = pl.multiple_of(lax.div(item, k_halves) * TILE_N, TILE_N)
            row = pl.multiple_of(lax.rem(item, k_halves) * TILE_K, TILE_K)
            pltpu.make_async_copy(wq_hbm.at[pl.ds(row, TILE_K), pl.ds(col, TILE_N)], wbuf.at[slot], w_sem.at[slot]).start()

        @pl.when(item >= q_items)
        def _():
            col = pl.multiple_of((item - q_items) * TILE_N, TILE_N)
            pltpu.make_async_copy(wo_hbm.at[:, pl.ds(col, TILE_N)], wbuf.at[slot], w_sem.at[slot]).start()

    def w_wait(g):
        slot = lax.rem(g, SLOTS)
        pltpu.make_async_copy(wo_hbm.at[:, pl.ds(0, TILE_N)], wbuf.at[slot], w_sem.at[slot]).wait()
        return slot

    def w_next(g):
        @pl.when(g + SLOTS < total)
        def _():
            w_issue(g + SLOTS)

    n_ln = tok // LN_ROWS
    ln_half = n_ln // n_half
    small = [pltpu.make_async_copy(src, dst, small_sem.at[i]) for i, (src, dst) in enumerate((
        (gain_hbm, gain_raw), (bias_hbm, bias_raw), (bkv_hbm, bkv_raw), (bq_hbm, bq_raw), (bo_hbm, bo_raw), (seg_hbm, seg_all.at[my])))]
    wkv_copy = pltpu.make_async_copy(wkv_hbm, wkv, wkv_sem)
    hid_copy(0).start()
    for copy in small:
        copy.start()
    for i in range(1, n_ln):
        hid_copy(i).start()

    barrier = pltpu.get_barrier_semaphore()
    for step in range(1, n_cp):
        pl.semaphore_signal(barrier, inc=1, device_id={'cp': lax.rem(my + step, n_cp)}, device_id_type=MESH)
    pl.semaphore_signal(barrier, inc=1, device_id={'tp': partner}, device_id_type=MESH)

    with jax.named_scope("small"):
        for copy in small:
            copy.wait()
    gain[...] = gain_raw[...].astype(f32)
    bias[...] = bias_raw[...].astype(f32)
    bkv[...] = bkv_raw[...].astype(f32)
    bq[...] = bq_raw[...].astype(f32)
    bo[...] = bo_raw[...].astype(f32)

    def ln_block(i, carry):
        with jax.named_scope("hidwait"):
            hid_copy(i).wait()

        @pl.when(i == 0)
        def _():
            wkv_copy.start()

        @pl.when((i > 0) & (i < ln_half))
        def _():
            for more in range(AHEAD):
                w_issue((i - 1) * AHEAD + more)

        rows = pl.ds(pl.multiple_of(i * LN_ROWS, LN_ROWS), LN_ROWS)
        n_col = d_model // 128

        def load(j):
            return y_ref[rows, j * 128:(j + 1) * 128].astype(f32)

        accs = [load(j) for j in range(4)]
        for j in range(4, n_col):
            accs[j % 4] = accs[j % 4] + load(j)
        mean = jnp.sum((accs[0] + accs[1]) + (accs[2] + accs[3]), axis=-1, keepdims=True) * (1.0 / d_model)
        mean = jnp.broadcast_to(mean, (LN_ROWS, 128))
        accs = [None] * 4
        for j in range(n_col):
            cen = load(j) - mean
            accs[j % 4] = cen * cen if accs[j % 4] is None else accs[j % 4] + cen * cen
        var = jnp.sum((accs[0] + accs[1]) + (accs[2] + accs[3]), axis=-1, keepdims=True) * (1.0 / d_model)
        rstd = jnp.broadcast_to(lax.rsqrt(var + LN_EPS), (LN_ROWS, 128))
        for j in range(n_col):
            out = (load(j) - mean) * rstd * gain[j:j + 1, :] + bias[j:j + 1, :]
            normed[rows, j * 128:(j + 1) * 128] = out.astype(bf16)
        return carry

    def kv_copy(src, h, dst):
        return pltpu.make_async_remote_copy(src_ref=kv_all.at[src, h], dst_ref=kv_all.at[src, h],
                                            send_sem=kv_send.at[dst, h], recv_sem=kv_recv.at[src, h],
                                            device_id={'cp': dst}, device_id_type=MESH)

    def seg_copy(src, dst):
        return pltpu.make_async_remote_copy(src_ref=seg_all.at[src], dst_ref=seg_all.at[src], send_sem=seg_send.at[dst],
                                            recv_sem=seg_recv.at[src], device_id={'cp': dst}, device_id_type=MESH)

    def kv_half(h):
        with jax.named_scope("ln"):
            lax.fori_loop(h * ln_half, (h + 1) * ln_half, ln_block, 0)
        rows = pl.ds(h * HALF, HALF)
        if h == 0:
            wkv_copy.wait()
        with jax.named_scope("kvdot"):
            part = jnp.dot(normed[rows, :], wkv[...], preferred_element_type=f32)
            k_own = (part[:, :HEAD_DIM] + bkv[0:1, :]).astype(bf16)
            v_own = (part[:, HEAD_DIM:] + bkv[1:2, :]).astype(bf16)
            kv_all[my, h, 0] = k_own
            kv_all[my, h, 1] = v_own.astype(f32).T.astype(bf16)
            k_ref[rows, :] = k_own
            v_ref[rows, :] = v_own
        if h == 0:
            with jax.named_scope("barrier"):
                pl.semaphore_wait(barrier, n_cp)
            for dst in range(1, n_cp):
                @pl.when(my < dst)
                def _():
                    seg_copy(my, dst).start()

        for dst in range(1, n_cp):
            @pl.when(my < dst)
            def _():
                kv_copy(my, h, dst).start()

    kv_half(0)

    @pl.when(my < EARLY)
    def _():
        for h in range(1, n_half):
            kv_half(h)

    def tile_copy(c, n):
        return pltpu.make_async_remote_copy(src_ref=send[c].at[n], dst_ref=recv[c].at[n], send_sem=tp_send.at[c, n],
                                            recv_sem=tp_recv.at[c, n], device_id={'tp': partner}, device_id_type=MESH)

    def chunk(c):
        base = c * items
        n_row = CHUNKS[c]
        first = sum(CHUNKS[:c])
        rows = slice(first, first + n_row)

        def q_tile(j):
            acc = None
            for half in range(k_halves):
                g = base + j * k_halves + half
                slot = w_wait(g)
                for n in range(2):
                    k0 = half * TILE_K + n * (TILE_K // 2)
                    part = jnp.dot(normed[rows, k0:k0 + TILE_K // 2], wbuf[slot, n * (TILE_K // 2):(n + 1) * (TILE_K // 2), :], preferred_element_type=f32)
                    acc = part if acc is None else acc + part
                w_next(g)
            for i in range(TILE_N // 128):
                cols = pl.ds(pl.multiple_of(j * TILE_N + i * 128, 128), 128)
                row = j * (TILE_N // 128) + i
                qbuf[:n_row, cols] = (acc[:, i * 128:(i + 1) * 128] + bq[pl.ds(row, 1), :]).astype(bf16)

        own_keys = first + n_row

        def make_mask():
            if c == 0:
                for src in range(n_cp - 1):
                    @pl.when(src < my)
                    def _():
                        seg_copy(src, src).wait_recv()
                        for h in range(n_half):
                            kv_copy(src, h, src).wait_recv()

            seg_q = jnp.broadcast_to(seg_all[my, c:c + 1, :].astype(f32), (128, 128)).T
            below[...] = jnp.zeros((128, 128), f32)
            for b in range(n_cp * tok // 128):
                src, part = b * 128 // tok, b % (tok // 128)

                @pl.when(b * 128 < my * tok + own_keys)
                def _():
                    below[...] += jnp.where(seg_all[src, part:part + 1, :].astype(f32) < seg_q, 1.0, 0.0)

            prompt = jnp.broadcast_to(jnp.sum(below[...], axis=1, keepdims=True), (128, 128)).T
            key = lax.broadcasted_iota(jnp.int32, (128, 128), 0)
            q_pos = my * tok + first + lax.broadcasted_iota(jnp.int32, (128, 128), 1)
            for b in range(n_cp * tok // 128):
                src, part = b * 128 // tok, b % (tok // 128)

                @pl.when(b * 128 < my * tok + own_keys)
                def _():
                    k_pos = key + b * 128
                    seen = (k_pos.astype(f32) >= prompt) & (k_pos <= q_pos)
                    mask[b * 128:(b + 1) * 128, :] = jnp.where(seen, 0.0, -jnp.inf)

        def heads(j):
            cols = pl.ds(pl.multiple_of(j * TILE_N, TILE_N), TILE_N)
            n_head = TILE_N // HEAD_DIM
            for nb in range(n_cp):
                @pl.when(my == nb)
                def _():
                    keys = nb * tok + own_keys
                    parts = [kv_all.at[b * 128 // tok, b % (tok // 128)] for b in range(keys // 128)]
                    k_blk = jnp.concatenate([part[0] for part in parts], axis=0)
                    v_t = jnp.concatenate([part[1] for part in parts], axis=1)
                    q_cols = qbuf[:, cols]
                    q_rows = jnp.concatenate([q_cols[:, i * HEAD_DIM:(i + 1) * HEAD_DIM] for i in range(n_head)], axis=0)
                    s = lax.dot_general(k_blk, q_rows, (((1,), (1,)), ((), ())), preferred_element_type=f32)
                    s = s + jnp.concatenate([mask[:keys, :]] * n_head, axis=1)
                    p_wts = jnp.exp2((s - jnp.max(s, axis=0, keepdims=True)) * EXP2_SCALE)
                    l_sum = jnp.sum(p_wts, axis=0, keepdims=True)
                    o = jnp.dot(v_t, p_wts.astype(bf16), preferred_element_type=f32) / l_sum
                    obuf[:, cols] = jnp.concatenate([o[:, i * HEAD_DIM:(i + 1) * HEAD_DIM].T for i in range(n_head)], axis=1).astype(bf16)

        lag = jnp.where(my == n_cp - 1, q_tiles, LAG) if c == 0 else LAG

        def stage(u, carry):
            @pl.when(u < q_tiles)
            def _():
                with jax.named_scope("qtile"):
                    q_tile(u)

            @pl.when(u == lag)
            def _():
                with jax.named_scope("mask"):
                    make_mask()

            @pl.when(u >= lag)
            def _():
                with jax.named_scope("attn"):
                    heads(u - lag)
            return carry

        lax.fori_loop(0, q_tiles + lag, stage, 0)

        def o_tile(n, carry):
            with jax.named_scope("otile"):
                g = base + q_items + n
                slot = w_wait(g)
                send[c][n] = jnp.dot(obuf[:n_row, :], wbuf[slot], preferred_element_type=f32).astype(bf16)
                tile_copy(c, n).start()
                w_next(g)
            return carry

        if c == 0:
            lax.fori_loop(0, EARLY_TILES, o_tile, 0)

            @pl.when(my >= EARLY)
            def _():
                for h in range(1, n_half):
                    kv_half(h)

            lax.fori_loop(EARLY_TILES, o_tiles, o_tile, 0)
        else:
            lax.fori_loop(0, o_tiles, o_tile, 0)

    for c in range(n_chunk):
        chunk(c)

    for dst in range(1, n_cp):
        @pl.when(my < dst)
        def _():
            seg_copy(my, dst).wait_send()
            for h in range(n_half):
                kv_copy(my, h, dst).wait_send()

    for c in range(n_chunk):
        first = sum(CHUNKS[:c])
        rows = slice(first, first + CHUNKS[c])

        def finish(n, carry):
            copy = tile_copy(c, n)
            copy.wait_recv()
            copy.wait_send()
            for i in range(TILE_N // 128):
                cols = pl.ds(pl.multiple_of(n * TILE_N + i * 128, 128), 128)
                part = slice(i * 128, (i + 1) * 128)
                both = send[c][n, :, part].astype(f32) + recv[c][n, :, part].astype(f32)
                y_ref[rows, cols] = (y_ref[rows, cols].astype(f32) + both + bo[pl.ds(n * (TILE_N // 128) + i, 1), :]).astype(bf16)
            return carry

        with jax.named_scope("finish"):
            lax.fori_loop(0, o_tiles, finish, 0)


def close_kernel(y_ref, k_ref, v_ref, y_hbm, k_hbm, v_hbm, sem):
    rows = y_ref.shape[0] // 8
    copies = [pltpu.make_async_copy(k_ref, k_hbm, sem.at[8]), pltpu.make_async_copy(v_ref, v_hbm, sem.at[9])]
    copies += [pltpu.make_async_copy(y_ref.at[pl.ds(i * rows, rows), :], y_hbm.at[pl.ds(i * rows, rows), :], sem.at[i]) for i in range(8)]
    for copy in copies:
        copy.start()
    for copy in copies:
        copy.wait()


def solution(mesh):
    n_cp = mesh.shape['cp']

    def local_block(hidden, seg_ids, w_q, b_q, w_kv, b_kv, w_o, b_o, ln_gain, ln_bias):
        tok, d_model = hidden.shape
        q_width = w_q.shape[1]
        o_tiles = d_model // TILE_N
        vmem = pl.BlockSpec(memory_space=pltpu.VMEM)
        hbm = pl.BlockSpec(memory_space=pltpu.HBM)
        bf16, f32 = jnp.bfloat16, jnp.float32
        dma = pltpu.SemaphoreType.DMA
        flops = 2 * tok * d_model * (2 * q_width + 256)
        args = (hidden, seg_ids.reshape(-1, 128), w_q, b_q.reshape(-1, 128), w_kv, b_kv.reshape(-1, 128), w_o,
                b_o.reshape(-1, 128), ln_gain.reshape(-1, 128), ln_bias.reshape(-1, 128))
        args = tuple(pltpu.with_memory_space_constraint(a, pltpu.HBM) for a in args)
        rows = [q_width // 128, 2, d_model // 128, d_model // 128, d_model // 128]
        y, k, v = pl.pallas_call(
            functools.partial(block_kernel, n_cp),
            out_shape=(pltpu.VMEM((tok, d_model), bf16), pltpu.VMEM((tok, HEAD_DIM), bf16), pltpu.VMEM((tok, HEAD_DIM), bf16)),
            in_specs=[hbm] * len(args),
            out_specs=(vmem, vmem, vmem),
            scratch_shapes=[
                pltpu.VMEM((tok, d_model), bf16),
                pltpu.VMEM((d_model, 2 * HEAD_DIM), bf16),
                pltpu.VMEM((SLOTS, TILE_K, TILE_N), bf16),
                pltpu.VMEM((n_cp, tok // HALF, 2, HALF, HEAD_DIM), bf16),
                pltpu.VMEM((n_cp, tok // 128, 128), jnp.int32),
                pltpu.VMEM((128, 128), f32),
                pltpu.VMEM((n_cp * tok, 128), f32),
                pltpu.VMEM((max(CHUNKS), q_width), bf16),
                pltpu.VMEM((max(CHUNKS), q_width), bf16),
                *[pltpu.VMEM((o_tiles, r, TILE_N), bf16) for r in CHUNKS * 2],
                *[pltpu.VMEM((r, 128), bf16) for r in rows],
                *[pltpu.VMEM((r, 128), f32) for r in rows],
                dma((tok // LN_ROWS,)), dma, dma((6,)), dma((SLOTS,)),
                dma((n_cp, tok // HALF)), dma((n_cp, tok // HALF)), dma((n_cp,)), dma((n_cp,)),
                dma((len(CHUNKS), o_tiles)), dma((len(CHUNKS), o_tiles)),
            ],
            compiler_params=pltpu.CompilerParams(collective_id=0, has_side_effects=True, vmem_limit_bytes=56 * 1024 * 1024),
            cost_estimate=pl.CostEstimate(flops=flops, bytes_accessed=2 * 4 * d_model * q_width, transcendentals=0),
        )(*args)
        return pl.pallas_call(
            close_kernel,
            out_shape=tuple(jax.ShapeDtypeStruct(a.shape, bf16) for a in (y, k, v)),
            in_specs=[vmem] * 3,
            out_specs=(hbm,) * 3,
            scratch_shapes=[dma((10,))],
            cost_estimate=pl.CostEstimate(flops=1, bytes_accessed=4 * tok * d_model, transcendentals=0),
        )(*(pltpu.with_memory_space_constraint(a, pltpu.VMEM) for a in (y, k, v)))

    row_spec = P(('dp', 'cp'), None)
    tok_spec = P(('dp', 'cp'))
    return jax.shard_map(local_block, mesh=mesh,
                         in_specs=(row_spec, tok_spec, P(None, 'tp'), P('tp'), P(None, None), P(None), P('tp', None), P(None), P(None), P(None)),
                         out_specs=(row_spec, row_spec, row_spec), check_vma=False)
```

```python
import functools

import jax
import jax.numpy as jnp
from jax import lax
from jax.experimental import pallas as pl
from jax.experimental.pallas import tpu as pltpu
from jax.sharding import PartitionSpec as P

HEAD_DIM = 128
LN_EPS = 1e-5
EXP2_SCALE = HEAD_DIM ** -0.5 * 1.4426950408889634
MESH = pl.DeviceIdType.MESH

CHUNKS = (128, 128)
HALF = 128
TILE_K = 3072
TILE_N = 512
AHEAD = 3
SLOTS = 9
LN_ROWS = 32


def block_kernel(n_cp, hid_hbm, seg_hbm, wq_hbm, bq_hbm, wkv_hbm, bkv_hbm, wo_hbm, bo_hbm, gain_hbm, bias_hbm,
                 y_ref, k_ref, v_ref,
                 normed, wkv, wbuf, kv_all, seg_all, below, mask, qbuf, obuf, send0, send1, recv0, recv1,
                 bq_raw, bkv_raw, bo_raw, gain_raw, bias_raw, bq, bkv, bo, gain, bias,
                 hid_sem, wkv_sem, small_sem, w_sem, kv_send, kv_recv, seg_send, seg_recv, tp_send, tp_recv):
    my = lax.axis_index('cp')
    partner = 1 - lax.axis_index('tp')
    tok, d_model = y_ref.shape
    q_width = qbuf.shape[1]
    n_chunk = len(CHUNKS)
    n_half = tok // HALF
    send, recv = (send0, send1), (recv0, recv1)
    q_tiles = q_width // TILE_N
    k_halves = d_model // TILE_K
    o_tiles = d_model // TILE_N
    q_items = q_tiles * k_halves
    items = q_items + o_tiles
    total = n_chunk * items
    f32, bf16 = jnp.float32, jnp.bfloat16

    def hid_copy(i):
        rows = pl.ds(i * LN_ROWS, LN_ROWS)
        return pltpu.make_async_copy(hid_hbm.at[rows, :], y_ref.at[rows, :], hid_sem.at[i])

    def w_issue(g):
        slot = lax.rem(g, SLOTS)
        item = lax.rem(g, items)

        @pl.when(item < q_items)
        def _():
            col = pl.multiple_of(lax.div(item, k_halves) * TILE_N, TILE_N)
            row = pl.multiple_of(lax.rem(item, k_halves) * TILE_K, TILE_K)
            pltpu.make_async_copy(wq_hbm.at[pl.ds(row, TILE_K), pl.ds(col, TILE_N)], wbuf.at[slot], w_sem.at[slot]).start()

        @pl.when(item >= q_items)
        def _():
            col = pl.multiple_of((item - q_items) * TILE_N, TILE_N)
            pltpu.make_async_copy(wo_hbm.at[:, pl.ds(col, TILE_N)], wbuf.at[slot], w_sem.at[slot]).start()

    def w_wait(g):
        slot = lax.rem(g, SLOTS)
        pltpu.make_async_copy(wo_hbm.at[:, pl.ds(0, TILE_N)], wbuf.at[slot], w_sem.at[slot]).wait()
        return slot

    def w_next(g):
        @pl.when(g + SLOTS < total)
        def _():
            w_issue(g + SLOTS)

    n_ln = tok // LN_ROWS
    ln_half = n_ln // n_half
    small = [pltpu.make_async_copy(src, dst, small_sem.at[i]) for i, (src, dst) in enumerate((
        (gain_hbm, gain_raw), (bias_hbm, bias_raw), (bkv_hbm, bkv_raw), (bq_hbm, bq_raw), (bo_hbm, bo_raw), (seg_hbm, seg_all.at[my])))]
    wkv_copy = pltpu.make_async_copy(wkv_hbm, wkv, wkv_sem)
    hid_copy(0).start()
    for copy in small:
        copy.start()
    for i in range(1, n_ln):
        hid_copy(i).start()

    barrier = pltpu.get_barrier_semaphore()
    for step in range(1, n_cp):
        pl.semaphore_signal(barrier, inc=1, device_id={'cp': lax.rem(my + step, n_cp)}, device_id_type=MESH)
    pl.semaphore_signal(barrier, inc=1, device_id={'tp': partner}, device_id_type=MESH)

    with jax.named_scope("hid"):
        hid_copy(0).wait()
        wkv_copy.start()
        for i in range(1, n_ln):
            hid_copy(i).wait()
            if i >= n_ln - AHEAD:
                w_issue(jnp.int32(i - n_ln + AHEAD))

    with jax.named_scope("small"):
        for copy in small:
            copy.wait()
    gain[...] = gain_raw[...].astype(f32)
    bias[...] = bias_raw[...].astype(f32)
    bkv[...] = bkv_raw[...].astype(f32)
    bq[...] = bq_raw[...].astype(f32)
    bo[...] = bo_raw[...].astype(f32)

    def ln_block(i, carry):
        @pl.when(i < (SLOTS - AHEAD) // 2)
        def _():
            for more in range(2):
                w_issue(i * 2 + more + AHEAD)

        rows = pl.ds(pl.multiple_of(i * LN_ROWS, LN_ROWS), LN_ROWS)
        n_col = d_model // 128

        def load(j):
            return y_ref[rows, j * 128:(j + 1) * 128].astype(f32)

        accs = [load(j) for j in range(4)]
        for j in range(4, n_col):
            accs[j % 4] = accs[j % 4] + load(j)
        mean = jnp.sum((accs[0] + accs[1]) + (accs[2] + accs[3]), axis=-1, keepdims=True) * (1.0 / d_model)
        mean = jnp.broadcast_to(mean, (LN_ROWS, 128))
        accs = [None] * 4
        for j in range(n_col):
            cen = load(j) - mean
            accs[j % 4] = cen * cen if accs[j % 4] is None else accs[j % 4] + cen * cen
        var = jnp.sum((accs[0] + accs[1]) + (accs[2] + accs[3]), axis=-1, keepdims=True) * (1.0 / d_model)
        rstd = jnp.broadcast_to(lax.rsqrt(var + LN_EPS), (LN_ROWS, 128))
        for j in range(n_col):
            out = (load(j) - mean) * rstd * gain[j:j + 1, :] + bias[j:j + 1, :]
            normed[rows, j * 128:(j + 1) * 128] = out.astype(bf16)
        return carry

    def kv_copy(src, h, dst):
        return pltpu.make_async_remote_copy(src_ref=kv_all.at[src, h], dst_ref=kv_all.at[src, h],
                                            send_sem=kv_send.at[dst, h], recv_sem=kv_recv.at[src, h],
                                            device_id={'cp': dst}, device_id_type=MESH)

    def seg_copy(src, dst):
        return pltpu.make_async_remote_copy(src_ref=seg_all.at[src], dst_ref=seg_all.at[src], send_sem=seg_send.at[dst],
                                            recv_sem=seg_recv.at[src], device_id={'cp': dst}, device_id_type=MESH)

    def kv_half(h):
        with jax.named_scope("ln"):
            lax.fori_loop(h * ln_half, (h + 1) * ln_half, ln_block, 0)
        rows = pl.ds(h * HALF, HALF)
        if h == 0:
            wkv_copy.wait()
        with jax.named_scope("kvdot"):
            part = jnp.dot(normed[rows, :], wkv[...], preferred_element_type=f32)
            k_own = (part[:, :HEAD_DIM] + bkv[0:1, :]).astype(bf16)
            v_own = (part[:, HEAD_DIM:] + bkv[1:2, :]).astype(bf16)
            kv_all[my, h, 0] = k_own
            kv_all[my, h, 1] = v_own.astype(f32).T.astype(bf16)
            k_ref[rows, :] = k_own
            v_ref[rows, :] = v_own
        if h == 0:
            with jax.named_scope("barrier"):
                pl.semaphore_wait(barrier, n_cp)
            for dst in range(1, n_cp):
                @pl.when(my < dst)
                def _():
                    seg_copy(my, dst).start()

        for dst in range(1, n_cp):
            @pl.when(my < dst)
            def _():
                kv_copy(my, h, dst).start()

    for h in range(n_half):
        kv_half(h)

    def tile_copy(c, n):
        return pltpu.make_async_remote_copy(src_ref=send[c].at[n], dst_ref=recv[c].at[n], send_sem=tp_send.at[c, n],
                                            recv_sem=tp_recv.at[c, n], device_id={'tp': partner}, device_id_type=MESH)

    def chunk(c):
        base = c * items
        n_row = CHUNKS[c]
        first = sum(CHUNKS[:c])
        rows = slice(first, first + n_row)

        def q_wait(j):
            return [w_wait(base + j * k_halves + half) for half in range(k_halves)]

        def q_next(j):
            for half in range(k_halves):
                w_next(base + j * k_halves + half)

        def q_dot(j, slots):
            acc = None
            step = TILE_K // 2
            for half in range(k_halves):
                for n in range(2):
                    k0 = half * TILE_K + n * step
                    part = jnp.dot(normed[rows, k0:k0 + step], wbuf[slots[half], n * step:(n + 1) * step, :], preferred_element_type=f32)
                    acc = part if acc is None else acc + part
            return acc

        def q_store(j, acc):
            for i in range(TILE_N // 128):
                cols = pl.ds(pl.multiple_of(j * TILE_N + i * 128, 128), 128)
                row = j * (TILE_N // 128) + i
                qbuf[:, cols] = (acc[:, i * 128:(i + 1) * 128] + bq[pl.ds(row, 1), :]).astype(bf16)

        def q_tile(j, carry):
            with jax.named_scope("qtile"):
                q_store(j, q_dot(j, q_wait(j)))
                q_next(j)
            return carry

        own_keys = first + n_row

        def make_mask():
            if c == 0:
                for src in range(n_cp - 1):
                    @pl.when(src < my)
                    def _():
                        seg_copy(src, src).wait_recv()
                        for h in range(n_half):
                            kv_copy(src, h, src).wait_recv()

            seg_q = jnp.broadcast_to(seg_all[my, c:c + 1, :].astype(f32), (128, 128)).T
            below[...] = jnp.zeros((128, 128), f32)
            for b in range(n_cp * tok // 128):
                src, part = b * 128 // tok, b % (tok // 128)

                @pl.when(b * 128 < my * tok + own_keys)
                def _():
                    below[...] += jnp.where(seg_all[src, part:part + 1, :].astype(f32) < seg_q, 1.0, 0.0)

            prompt = jnp.broadcast_to(jnp.sum(below[...], axis=1, keepdims=True), (128, 128)).T
            key = lax.broadcasted_iota(jnp.int32, (128, 128), 0)
            q_pos = my * tok + first + lax.broadcasted_iota(jnp.int32, (128, 128), 1)
            for b in range(n_cp * tok // 128):
                src, part = b * 128 // tok, b % (tok // 128)

                @pl.when(b * 128 < my * tok + own_keys)
                def _():
                    k_pos = key + b * 128
                    seen = (k_pos.astype(f32) >= prompt) & (k_pos <= q_pos)
                    mask[b * 128:(b + 1) * 128, :] = jnp.where(seen, 0.0, -jnp.inf)

        def heads(j, nb, beside=None):
            cols = pl.ds(pl.multiple_of(j * TILE_N, TILE_N), TILE_N)
            n_head = TILE_N // HEAD_DIM
            keys = nb * tok + own_keys
            parts = [kv_all.at[b * 128 // tok, b % (tok // 128)] for b in range(keys // 128)]
            k_blk = jnp.concatenate([part[0] for part in parts], axis=0)
            v_t = jnp.concatenate([part[1] for part in parts], axis=1)
            q_cols = qbuf[:, cols]
            q_rows = jnp.concatenate([q_cols[:, i * HEAD_DIM:(i + 1) * HEAD_DIM] for i in range(n_head)], axis=0)
            s = lax.dot_general(k_blk, q_rows, (((1,), (1,)), ((), ())), preferred_element_type=f32)
            other = beside() if beside else None
            s = s + jnp.concatenate([mask[:keys, :]] * n_head, axis=1)
            p_wts = jnp.exp2((s - jnp.max(s, axis=0, keepdims=True)) * EXP2_SCALE)
            l_sum = jnp.sum(p_wts, axis=0, keepdims=True)
            o = jnp.dot(v_t, p_wts.astype(bf16), preferred_element_type=f32) / l_sum
            obuf[:, cols] = jnp.concatenate([o[:, i * HEAD_DIM:(i + 1) * HEAD_DIM].T for i in range(n_head)], axis=1).astype(bf16)
            return other

        def attend(j, carry):
            for nb in range(n_cp):
                @pl.when(my == nb)
                def _():
                    with jax.named_scope("attn"):
                        heads(j, nb)
            return carry

        def both(j, carry):
            slots = q_wait(j)
            for nb in range(n_cp):
                @pl.when(my == nb)
                def _():
                    with jax.named_scope("both"):
                        q_store(j, heads(j - lag, nb, lambda: q_dot(j, slots)))
            q_next(j)
            return carry

        lag = jnp.where(my < n_cp // 2, 1, 2)
        lax.fori_loop(0, lag, q_tile, 0)
        with jax.named_scope("mask"):
            make_mask()
        if c == 0:
            lax.fori_loop(lag, q_tiles, both, 0)
        else:
            def turn(j, carry):
                return attend(j - lag, q_tile(j, carry))

            lax.fori_loop(lag, q_tiles, turn, 0)
        lax.fori_loop(q_tiles - lag, q_tiles, attend, 0)

        def o_tile(n, carry):
            with jax.named_scope("otile"):
                g = base + q_items + n
                slot = w_wait(g)
                send[c][n] = jnp.dot(obuf[:n_row, :], wbuf[slot], preferred_element_type=f32).astype(bf16)
                tile_copy(c, n).start()
                w_next(g)
            return carry

        lax.fori_loop(0, o_tiles, o_tile, 0)

    for c in range(n_chunk):
        chunk(c)

    for dst in range(1, n_cp):
        @pl.when(my < dst)
        def _():
            seg_copy(my, dst).wait_send()
            for h in range(n_half):
                kv_copy(my, h, dst).wait_send()

    for c in range(n_chunk):
        first = sum(CHUNKS[:c])
        rows = slice(first, first + CHUNKS[c])

        def finish(n, carry):
            copy = tile_copy(c, n)
            copy.wait_recv()
            copy.wait_send()
            for i in range(TILE_N // 128):
                cols = pl.ds(pl.multiple_of(n * TILE_N + i * 128, 128), 128)
                part = slice(i * 128, (i + 1) * 128)
                both = send[c][n, :, part].astype(f32) + recv[c][n, :, part].astype(f32)
                y_ref[rows, cols] = (y_ref[rows, cols].astype(f32) + both + bo[pl.ds(n * (TILE_N // 128) + i, 1), :]).astype(bf16)
            return carry

        with jax.named_scope("finish"):
            lax.fori_loop(0, o_tiles, finish, 0)


def close_kernel(y_ref, k_ref, v_ref, y_hbm, k_hbm, v_hbm, sem):
    rows = y_ref.shape[0] // 8
    copies = [pltpu.make_async_copy(k_ref, k_hbm, sem.at[8]), pltpu.make_async_copy(v_ref, v_hbm, sem.at[9])]
    copies += [pltpu.make_async_copy(y_ref.at[pl.ds(i * rows, rows), :], y_hbm.at[pl.ds(i * rows, rows), :], sem.at[i]) for i in range(8)]
    for copy in copies:
        copy.start()
    for copy in copies:
        copy.wait()


def solution(mesh):
    n_cp = mesh.shape['cp']

    def local_block(hidden, seg_ids, w_q, b_q, w_kv, b_kv, w_o, b_o, ln_gain, ln_bias):
        tok, d_model = hidden.shape
        q_width = w_q.shape[1]
        o_tiles = d_model // TILE_N
        vmem = pl.BlockSpec(memory_space=pltpu.VMEM)
        hbm = pl.BlockSpec(memory_space=pltpu.HBM)
        bf16, f32 = jnp.bfloat16, jnp.float32
        dma = pltpu.SemaphoreType.DMA
        flops = 2 * tok * d_model * (2 * q_width + 256)
        args = (hidden, seg_ids.reshape(-1, 128), w_q, b_q.reshape(-1, 128), w_kv, b_kv.reshape(-1, 128), w_o,
                b_o.reshape(-1, 128), ln_gain.reshape(-1, 128), ln_bias.reshape(-1, 128))
        args = tuple(pltpu.with_memory_space_constraint(a, pltpu.HBM) for a in args)
        rows = [q_width // 128, 2, d_model // 128, d_model // 128, d_model // 128]
        y, k, v = pl.pallas_call(
            functools.partial(block_kernel, n_cp),
            out_shape=(pltpu.VMEM((tok, d_model), bf16), pltpu.VMEM((tok, HEAD_DIM), bf16), pltpu.VMEM((tok, HEAD_DIM), bf16)),
            in_specs=[hbm] * len(args),
            out_specs=(vmem, vmem, vmem),
            scratch_shapes=[
                pltpu.VMEM((tok, d_model), bf16),
                pltpu.VMEM((d_model, 2 * HEAD_DIM), bf16),
                pltpu.VMEM((SLOTS, TILE_K, TILE_N), bf16),
                pltpu.VMEM((n_cp, tok // HALF, 2, HALF, HEAD_DIM), bf16),
                pltpu.VMEM((n_cp, tok // 128, 128), jnp.int32),
                pltpu.VMEM((128, 128), f32),
                pltpu.VMEM((n_cp * tok, 128), f32),
                pltpu.VMEM((max(CHUNKS), q_width), bf16),
                pltpu.VMEM((max(CHUNKS), q_width), bf16),
                *[pltpu.VMEM((o_tiles, r, TILE_N), bf16) for r in CHUNKS * 2],
                *[pltpu.VMEM((r, 128), bf16) for r in rows],
                *[pltpu.VMEM((r, 128), f32) for r in rows],
                dma((tok // LN_ROWS,)), dma, dma((6,)), dma((SLOTS,)),
                dma((n_cp, tok // HALF)), dma((n_cp, tok // HALF)), dma((n_cp,)), dma((n_cp,)),
                dma((len(CHUNKS), o_tiles)), dma((len(CHUNKS), o_tiles)),
            ],
            compiler_params=pltpu.CompilerParams(collective_id=0, has_side_effects=True, vmem_limit_bytes=56 * 1024 * 1024),
            cost_estimate=pl.CostEstimate(flops=flops, bytes_accessed=2 * 4 * d_model * q_width, transcendentals=0),
        )(*args)
        return pl.pallas_call(
            close_kernel,
            out_shape=tuple(jax.ShapeDtypeStruct(a.shape, bf16) for a in (y, k, v)),
            in_specs=[vmem] * 3,
            out_specs=(hbm,) * 3,
            scratch_shapes=[dma((10,))],
            cost_estimate=pl.CostEstimate(flops=1, bytes_accessed=4 * tok * d_model, transcendentals=0),
        )(*(pltpu.with_memory_space_constraint(a, pltpu.VMEM) for a in (y, k, v)))

    row_spec = P(('dp', 'cp'), None)
    tok_spec = P(('dp', 'cp'))
    return jax.shard_map(local_block, mesh=mesh,
                         in_specs=(row_spec, tok_spec, P(None, 'tp'), P('tp'), P(None, None), P(None), P('tp', None), P(None), P(None), P(None)),
                         out_specs=(row_spec, row_spec, row_spec), check_vma=False)
```

```python
import functools

import jax
import jax.numpy as jnp
from jax import lax
from jax.experimental import pallas as pl
from jax.experimental.pallas import tpu as pltpu
from jax.sharding import PartitionSpec as P

HEAD_DIM = 128
LN_EPS = 1e-5
EXP2_SCALE = HEAD_DIM ** -0.5 * 1.4426950408889634
MESH = pl.DeviceIdType.MESH

CHUNKS = (128, 128)
HALF = 128
TILE_K = 3072
TILE_N = 512
AHEAD = 3
SLOTS = 9
LN_ROWS = 32


def block_kernel(n_cp, hid_hbm, seg_hbm, wq_hbm, bq_hbm, wkv_hbm, bkv_hbm, wo_hbm, bo_hbm, gain_hbm, bias_hbm,
                 y_ref, k_ref, v_ref,
                 normed, wkv, wbuf, kv_all, seg_all, below, mask, qbuf, obuf, send0, send1, recv0, recv1,
                 bq_raw, bkv_raw, bo_raw, gain_raw, bias_raw, bq, bkv, bo, gain, bias,
                 hid_sem, wkv_sem, small_sem, w_sem, kv_send, kv_recv, seg_send, seg_recv, tp_send, tp_recv):
    my = lax.axis_index('cp')
    partner = 1 - lax.axis_index('tp')
    tok, d_model = y_ref.shape
    q_width = qbuf.shape[1]
    n_chunk = len(CHUNKS)
    n_half = tok // HALF
    send, recv = (send0, send1), (recv0, recv1)
    q_tiles = q_width // TILE_N
    k_halves = d_model // TILE_K
    o_tiles = d_model // TILE_N
    q_items = q_tiles * k_halves
    items = q_items + o_tiles
    total = n_chunk * items
    f32, bf16 = jnp.float32, jnp.bfloat16

    def hid_copy(i):
        rows = pl.ds(i * LN_ROWS, LN_ROWS)
        return pltpu.make_async_copy(hid_hbm.at[rows, :], y_ref.at[rows, :], hid_sem.at[i])

    def w_issue(g):
        slot = lax.rem(g, SLOTS)
        item = lax.rem(g, items)

        @pl.when(item < q_items)
        def _():
            col = pl.multiple_of(lax.div(item, k_halves) * TILE_N, TILE_N)
            row = pl.multiple_of(lax.rem(item, k_halves) * TILE_K, TILE_K)
            pltpu.make_async_copy(wq_hbm.at[pl.ds(row, TILE_K), pl.ds(col, TILE_N)], wbuf.at[slot], w_sem.at[slot]).start()

        @pl.when(item >= q_items)
        def _():
            col = pl.multiple_of((item - q_items) * TILE_N, TILE_N)
            pltpu.make_async_copy(wo_hbm.at[:, pl.ds(col, TILE_N)], wbuf.at[slot], w_sem.at[slot]).start()

    def w_wait(g):
        slot = lax.rem(g, SLOTS)
        pltpu.make_async_copy(wo_hbm.at[:, pl.ds(0, TILE_N)], wbuf.at[slot], w_sem.at[slot]).wait()
        return slot

    def w_next(g):
        @pl.when(g + SLOTS < total)
        def _():
            w_issue(g + SLOTS)

    n_ln = tok // LN_ROWS
    ln_half = n_ln // n_half
    small = [pltpu.make_async_copy(src, dst, small_sem.at[i]) for i, (src, dst) in enumerate((
        (gain_hbm, gain_raw), (bias_hbm, bias_raw), (bkv_hbm, bkv_raw), (bq_hbm, bq_raw), (bo_hbm, bo_raw), (seg_hbm, seg_all.at[my])))]
    wkv_copy = pltpu.make_async_copy(wkv_hbm, wkv, wkv_sem)
    hid_copy(0).start()
    for copy in small:
        copy.start()
    for i in range(1, n_ln):
        hid_copy(i).start()

    barrier = pltpu.get_barrier_semaphore()
    for step in range(1, n_cp):
        pl.semaphore_signal(barrier, inc=1, device_id={'cp': lax.rem(my + step, n_cp)}, device_id_type=MESH)
    pl.semaphore_signal(barrier, inc=1, device_id={'tp': partner}, device_id_type=MESH)

    with jax.named_scope("hid"):
        hid_copy(0).wait()
        wkv_copy.start()
        for i in range(1, n_ln):
            hid_copy(i).wait()
            if i >= n_ln - AHEAD:
                w_issue(jnp.int32(i - n_ln + AHEAD))

    with jax.named_scope("small"):
        for copy in small:
            copy.wait()
    gain[...] = gain_raw[...].astype(f32)
    bias[...] = bias_raw[...].astype(f32)
    bkv[...] = bkv_raw[...].astype(f32)
    bq[...] = bq_raw[...].astype(f32)
    bo[...] = bo_raw[...].astype(f32)

    def ln_block(i, carry):
        @pl.when(i < (SLOTS - AHEAD) // 2)
        def _():
            for more in range(2):
                w_issue(i * 2 + more + AHEAD)

        rows = pl.ds(pl.multiple_of(i * LN_ROWS, LN_ROWS), LN_ROWS)
        n_col = d_model // 128

        def load(j):
            return y_ref[rows, j * 128:(j + 1) * 128].astype(f32)

        accs = [load(j) for j in range(4)]
        for j in range(4, n_col):
            accs[j % 4] = accs[j % 4] + load(j)
        mean = jnp.sum((accs[0] + accs[1]) + (accs[2] + accs[3]), axis=-1, keepdims=True) * (1.0 / d_model)
        mean = jnp.broadcast_to(mean, (LN_ROWS, 128))
        accs = [None] * 4
        for j in range(n_col):
            cen = load(j) - mean
            accs[j % 4] = cen * cen if accs[j % 4] is None else accs[j % 4] + cen * cen
        var = jnp.sum((accs[0] + accs[1]) + (accs[2] + accs[3]), axis=-1, keepdims=True) * (1.0 / d_model)
        rstd = jnp.broadcast_to(lax.rsqrt(var + LN_EPS), (LN_ROWS, 128))
        for j in range(n_col):
            out = (load(j) - mean) * rstd * gain[j:j + 1, :] + bias[j:j + 1, :]
            normed[rows, j * 128:(j + 1) * 128] = out.astype(bf16)
        return carry

    def kv_copy(src, h, dst):
        return pltpu.make_async_remote_copy(src_ref=kv_all.at[src, h], dst_ref=kv_all.at[src, h],
                                            send_sem=kv_send.at[dst, h], recv_sem=kv_recv.at[src, h],
                                            device_id={'cp': dst}, device_id_type=MESH)

    def seg_copy(src, dst):
        return pltpu.make_async_remote_copy(src_ref=seg_all.at[src], dst_ref=seg_all.at[src], send_sem=seg_send.at[dst],
                                            recv_sem=seg_recv.at[src], device_id={'cp': dst}, device_id_type=MESH)

    def late(dst):
        return (dst == n_cp - 1) & (my < n_cp // 2)

    def kv_half(h):
        with jax.named_scope("ln"):
            lax.fori_loop(h * ln_half, (h + 1) * ln_half, ln_block, 0)
        rows = pl.ds(h * HALF, HALF)
        if h == 0:
            wkv_copy.wait()
        with jax.named_scope("kvdot"):
            mid = d_model // 2
            low = jnp.dot(normed[rows, :mid], wkv[:mid, :], preferred_element_type=f32)
            high = jnp.dot(normed[rows, mid:], wkv[mid:, :], preferred_element_type=f32)
            k_own = ((low[:, :HEAD_DIM] + bkv[0:1, :]) + high[:, :HEAD_DIM]).astype(bf16)
            v_own = ((low[:, HEAD_DIM:] + bkv[1:2, :]) + high[:, HEAD_DIM:]).astype(bf16)
            kv_all[my, h, 0] = k_own
            kv_all[my, h, 1] = v_own.astype(f32).T.astype(bf16)
            k_ref[rows, :] = k_own
            v_ref[rows, :] = v_own
        if h == 0:
            with jax.named_scope("barrier"):
                pl.semaphore_wait(barrier, n_cp)
            for dst in range(1, n_cp):
                @pl.when(my < dst)
                def _():
                    seg_copy(my, dst).start()

        for dst in range(1, n_cp):
            @pl.when((my < dst) & jnp.logical_not(late(dst)))
            def _():
                kv_copy(my, h, dst).start()

    kv_half(0)

    @pl.when(my < n_cp)
    def _():
        for h in range(1, n_half):
            kv_half(h)

    def tile_copy(c, n):
        return pltpu.make_async_remote_copy(src_ref=send[c].at[n], dst_ref=recv[c].at[n], send_sem=tp_send.at[c, n],
                                            recv_sem=tp_recv.at[c, n], device_id={'tp': partner}, device_id_type=MESH)

    def chunk(c):
        base = c * items
        n_row = CHUNKS[c]
        first = sum(CHUNKS[:c])
        rows = slice(first, first + n_row)

        def q_wait(j):
            return [w_wait(base + j * k_halves + half) for half in range(k_halves)]

        def q_next(j):
            for half in range(k_halves):
                w_next(base + j * k_halves + half)

        def q_dot(j, slots):
            acc = None
            step = TILE_K // 2
            for half in range(k_halves):
                for n in range(2):
                    k0 = half * TILE_K + n * step
                    part = jnp.dot(normed[rows, k0:k0 + step], wbuf[slots[half], n * step:(n + 1) * step, :], preferred_element_type=f32)
                    acc = part if acc is None else acc + part
            return acc

        def q_store(j, acc):
            for i in range(TILE_N // 128):
                cols = pl.ds(pl.multiple_of(j * TILE_N + i * 128, 128), 128)
                row = j * (TILE_N // 128) + i
                qbuf[:, cols] = (acc[:, i * 128:(i + 1) * 128] + bq[pl.ds(row, 1), :]).astype(bf16)

        def q_tile(j, carry):
            with jax.named_scope("qtile"):
                q_store(j, q_dot(j, q_wait(j)))
                q_next(j)
            return carry

        own_keys = first + n_row

        def make_mask():
            if c == 0:
                for src in range(n_cp - 1):
                    @pl.when(src < my)
                    def _():
                        seg_copy(src, src).wait_recv()

            seg_q = jnp.broadcast_to(seg_all[my, c:c + 1, :].astype(f32), (128, 128)).T
            below[...] = jnp.zeros((128, 128), f32)
            for b in range(n_cp * tok // 128):
                src, part = b * 128 // tok, b % (tok // 128)

                @pl.when(b * 128 < my * tok + own_keys)
                def _():
                    below[...] += jnp.where(seg_all[src, part:part + 1, :].astype(f32) < seg_q, 1.0, 0.0)

            prompt = jnp.broadcast_to(jnp.sum(below[...], axis=1, keepdims=True), (128, 128)).T
            key = lax.broadcasted_iota(jnp.int32, (128, 128), 0)
            q_pos = my * tok + first + lax.broadcasted_iota(jnp.int32, (128, 128), 1)
            for b in range(n_cp * tok // 128):
                src, part = b * 128 // tok, b % (tok // 128)

                @pl.when(b * 128 < my * tok + own_keys)
                def _():
                    k_pos = key + b * 128
                    seen = (k_pos.astype(f32) >= prompt) & (k_pos <= q_pos)
                    mask[b * 128:(b + 1) * 128, :] = jnp.where(seen, 0.0, -jnp.inf)

        def heads(j, nb, beside=None):
            cols = pl.ds(pl.multiple_of(j * TILE_N, TILE_N), TILE_N)
            n_head = TILE_N // HEAD_DIM
            keys = nb * tok + own_keys
            parts = [kv_all.at[b * 128 // tok, b % (tok // 128)] for b in range(keys // 128)]
            k_blk = jnp.concatenate([part[0] for part in parts], axis=0)
            v_t = jnp.concatenate([part[1] for part in parts], axis=1)
            q_cols = qbuf[:, cols]
            q_rows = jnp.concatenate([q_cols[:, i * HEAD_DIM:(i + 1) * HEAD_DIM] for i in range(n_head)], axis=0)
            s = lax.dot_general(k_blk, q_rows, (((1,), (1,)), ((), ())), preferred_element_type=f32)
            other = beside() if beside else None
            s = s + jnp.concatenate([mask[:keys, :]] * n_head, axis=1)
            p_wts = jnp.exp2((s - jnp.max(s, axis=0, keepdims=True)) * EXP2_SCALE)
            l_sum = jnp.sum(p_wts, axis=0, keepdims=True)
            o = jnp.dot(v_t, p_wts.astype(bf16), preferred_element_type=f32) / l_sum
            obuf[:, cols] = jnp.concatenate([o[:, i * HEAD_DIM:(i + 1) * HEAD_DIM].T for i in range(n_head)], axis=1).astype(bf16)
            return other

        def attend(j, carry):
            for nb in range(n_cp):
                @pl.when(my == nb)
                def _():
                    with jax.named_scope("attn"):
                        heads(j, nb)
            return carry

        def both(j, carry):
            slots = q_wait(j)
            for nb in range(n_cp):
                @pl.when(my == nb)
                def _():
                    with jax.named_scope("both"):
                        q_store(j, heads(j - lag, nb, lambda: q_dot(j, slots)))
            q_next(j)
            return carry

        lag = jnp.where(my < n_cp // 2, 1, 2)
        q_tile(0, 0)
        if c == 0:
            @pl.when(late(n_cp - 1))
            def _():
                for h in range(n_half):
                    kv_copy(my, h, n_cp - 1).start()

        lax.fori_loop(1, lag, q_tile, 0)
        with jax.named_scope("mask"):
            make_mask()
        if c == 0:
            with jax.named_scope("kvwait"):
                for src in range(n_cp - 1):
                    @pl.when(src < my)
                    def _():
                        for h in range(n_half):
                            kv_copy(src, h, src).wait_recv()
        if c == 0:
            lax.fori_loop(lag, q_tiles, both, 0)
        else:
            def turn(j, carry):
                return attend(j - lag, q_tile(j, carry))

            lax.fori_loop(lag, q_tiles, turn, 0)
        lax.fori_loop(q_tiles - lag, q_tiles, attend, 0)

        def o_tile(n, carry):
            with jax.named_scope("otile"):
                g = base + q_items + n
                slot = w_wait(g)
                send[c][n] = jnp.dot(obuf[:n_row, :], wbuf[slot], preferred_element_type=f32).astype(bf16)
                tile_copy(c, n).start()
                w_next(g)
            return carry

        lax.fori_loop(0, o_tiles, o_tile, 0)

    for c in range(n_chunk):
        chunk(c)

    for dst in range(1, n_cp):
        @pl.when(my < dst)
        def _():
            seg_copy(my, dst).wait_send()
            for h in range(n_half):
                kv_copy(my, h, dst).wait_send()

    for c in range(n_chunk):
        first = sum(CHUNKS[:c])
        rows = slice(first, first + CHUNKS[c])

        def finish(n, carry):
            copy = tile_copy(c, n)
            copy.wait_recv()
            copy.wait_send()
            for i in range(TILE_N // 128):
                cols = pl.ds(pl.multiple_of(n * TILE_N + i * 128, 128), 128)
                part = slice(i * 128, (i + 1) * 128)
                both = send[c][n, :, part].astype(f32) + recv[c][n, :, part].astype(f32)
                y_ref[rows, cols] = (y_ref[rows, cols].astype(f32) + both + bo[pl.ds(n * (TILE_N // 128) + i, 1), :]).astype(bf16)
            return carry

        with jax.named_scope("finish"):
            lax.fori_loop(0, o_tiles, finish, 0)


def close_kernel(y_ref, k_ref, v_ref, y_hbm, k_hbm, v_hbm, sem):
    rows = y_ref.shape[0] // 8
    copies = [pltpu.make_async_copy(k_ref, k_hbm, sem.at[8]), pltpu.make_async_copy(v_ref, v_hbm, sem.at[9])]
    copies += [pltpu.make_async_copy(y_ref.at[pl.ds(i * rows, rows), :], y_hbm.at[pl.ds(i * rows, rows), :], sem.at[i]) for i in range(8)]
    for copy in copies:
        copy.start()
    for copy in copies:
        copy.wait()


def solution(mesh):
    n_cp = mesh.shape['cp']

    def local_block(hidden, seg_ids, w_q, b_q, w_kv, b_kv, w_o, b_o, ln_gain, ln_bias):
        tok, d_model = hidden.shape
        q_width = w_q.shape[1]
        o_tiles = d_model // TILE_N
        vmem = pl.BlockSpec(memory_space=pltpu.VMEM)
        hbm = pl.BlockSpec(memory_space=pltpu.HBM)
        bf16, f32 = jnp.bfloat16, jnp.float32
        dma = pltpu.SemaphoreType.DMA
        flops = 2 * tok * d_model * (2 * q_width + 256)
        args = (hidden, seg_ids.reshape(-1, 128), w_q, b_q.reshape(-1, 128), w_kv, b_kv.reshape(-1, 128), w_o,
                b_o.reshape(-1, 128), ln_gain.reshape(-1, 128), ln_bias.reshape(-1, 128))
        args = tuple(pltpu.with_memory_space_constraint(a, pltpu.HBM) for a in args)
        rows = [q_width // 128, 2, d_model // 128, d_model // 128, d_model // 128]
        y, k, v = pl.pallas_call(
            functools.partial(block_kernel, n_cp),
            out_shape=(pltpu.VMEM((tok, d_model), bf16), pltpu.VMEM((tok, HEAD_DIM), bf16), pltpu.VMEM((tok, HEAD_DIM), bf16)),
            in_specs=[hbm] * len(args),
            out_specs=(vmem, vmem, vmem),
            scratch_shapes=[
                pltpu.VMEM((tok, d_model), bf16),
                pltpu.VMEM((d_model, 2 * HEAD_DIM), bf16),
                pltpu.VMEM((SLOTS, TILE_K, TILE_N), bf16),
                pltpu.VMEM((n_cp, tok // HALF, 2, HALF, HEAD_DIM), bf16),
                pltpu.VMEM((n_cp, tok // 128, 128), jnp.int32),
                pltpu.VMEM((128, 128), f32),
                pltpu.VMEM((n_cp * tok, 128), f32),
                pltpu.VMEM((max(CHUNKS), q_width), bf16),
                pltpu.VMEM((max(CHUNKS), q_width), bf16),
                *[pltpu.VMEM((o_tiles, r, TILE_N), bf16) for r in CHUNKS * 2],
                *[pltpu.VMEM((r, 128), bf16) for r in rows],
                *[pltpu.VMEM((r, 128), f32) for r in rows],
                dma((tok // LN_ROWS,)), dma, dma((6,)), dma((SLOTS,)),
                dma((n_cp, tok // HALF)), dma((n_cp, tok // HALF)), dma((n_cp,)), dma((n_cp,)),
                dma((len(CHUNKS), o_tiles)), dma((len(CHUNKS), o_tiles)),
            ],
            compiler_params=pltpu.CompilerParams(collective_id=0, has_side_effects=True, vmem_limit_bytes=56 * 1024 * 1024),
            cost_estimate=pl.CostEstimate(flops=flops, bytes_accessed=2 * 4 * d_model * q_width, transcendentals=0),
        )(*args)
        return pl.pallas_call(
            close_kernel,
            out_shape=tuple(jax.ShapeDtypeStruct(a.shape, bf16) for a in (y, k, v)),
            in_specs=[vmem] * 3,
            out_specs=(hbm,) * 3,
            scratch_shapes=[dma((10,))],
            cost_estimate=pl.CostEstimate(flops=1, bytes_accessed=4 * tok * d_model, transcendentals=0),
        )(*(pltpu.with_memory_space_constraint(a, pltpu.VMEM) for a in (y, k, v)))

    row_spec = P(('dp', 'cp'), None)
    tok_spec = P(('dp', 'cp'))
    return jax.shard_map(local_block, mesh=mesh,
                         in_specs=(row_spec, tok_spec, P(None, 'tp'), P('tp'), P(None, None), P(None), P('tp', None), P(None), P(None), P(None)),
                         out_specs=(row_spec, row_spec, row_spec), check_vma=False)
```

```python
import functools

import jax
import jax.numpy as jnp
from jax import lax
from jax.experimental import pallas as pl
from jax.experimental.pallas import tpu as pltpu
from jax.sharding import PartitionSpec as P

HEAD_DIM = 128
LN_EPS = 1e-5
EXP2_SCALE = HEAD_DIM ** -0.5 * 1.4426950408889634
MESH = pl.DeviceIdType.MESH

CHUNKS = (128, 128)
HALF = 128
TILE_K = 3072
TILE_N = 512
SLOTS = 10
LN_ROWS = 32


def block_kernel(n_cp, hid_hbm, seg_hbm, wq_hbm, bq_hbm, wkv_hbm, bkv_hbm, wo_hbm, bo_hbm, gain_hbm, bias_hbm,
                 y_ref, k_ref, v_ref,
                 normed, wkv, wbuf, kv_all, seg_all, below, mask, qbuf, obuf, send0, send1, recv0, recv1,
                 bq_raw, bkv_raw, bo_raw, gain_raw, bias_raw, bq, bkv, bo, gain, bias,
                 hid_sem, wkv_sem, small_sem, w_sem, kv_send, kv_recv, seg_send, seg_recv, tp_send, tp_recv):
    my = lax.axis_index('cp')
    partner = 1 - lax.axis_index('tp')
    tok, d_model = y_ref.shape
    q_width = qbuf.shape[1]
    n_chunk = len(CHUNKS)
    n_half = tok // HALF
    send, recv = (send0, send1), (recv0, recv1)
    q_tiles = q_width // TILE_N
    k_halves = d_model // TILE_K
    o_tiles = d_model // TILE_N
    q_items = q_tiles * k_halves
    items = q_items + o_tiles
    total = n_chunk * items
    f32, bf16 = jnp.float32, jnp.bfloat16

    def hid_copy(i):
        rows = pl.ds(i * LN_ROWS, LN_ROWS)
        return pltpu.make_async_copy(hid_hbm.at[rows, :], y_ref.at[rows, :], hid_sem.at[i])

    def w_issue(g):
        slot = lax.rem(g, SLOTS)
        item = lax.rem(g, items)

        @pl.when(item < q_items)
        def _():
            col = pl.multiple_of(lax.div(item, k_halves) * TILE_N, TILE_N)
            row = pl.multiple_of(lax.rem(item, k_halves) * TILE_K, TILE_K)
            pltpu.make_async_copy(wq_hbm.at[pl.ds(row, TILE_K), pl.ds(col, TILE_N)], wbuf.at[slot], w_sem.at[slot]).start()

        @pl.when(item >= q_items)
        def _():
            col = pl.multiple_of((item - q_items) * TILE_N, TILE_N)
            pltpu.make_async_copy(wo_hbm.at[:, pl.ds(col, TILE_N)], wbuf.at[slot], w_sem.at[slot]).start()

    def w_wait(g):
        slot = lax.rem(g, SLOTS)
        pltpu.make_async_copy(wo_hbm.at[:, pl.ds(0, TILE_N)], wbuf.at[slot], w_sem.at[slot]).wait()
        return slot

    def w_next(g):
        @pl.when(g + SLOTS < total)
        def _():
            w_issue(g + SLOTS)

    n_ln = tok // LN_ROWS
    ln_half = n_ln // n_half
    small = [pltpu.make_async_copy(src, dst, small_sem.at[i]) for i, (src, dst) in enumerate((
        (gain_hbm, gain_raw), (bias_hbm, bias_raw), (bkv_hbm, bkv_raw), (bq_hbm, bq_raw), (bo_hbm, bo_raw), (seg_hbm, seg_all.at[my])))]
    wkv_copy = pltpu.make_async_copy(wkv_hbm, wkv, wkv_sem)
    hid_copy(0).start()
    for copy in small:
        copy.start()
    for i in range(1, ln_half):
        hid_copy(i).start()

    barrier = pltpu.get_barrier_semaphore()
    for step in range(1, n_cp):
        pl.semaphore_signal(barrier, inc=1, device_id={'cp': lax.rem(my + step, n_cp)}, device_id_type=MESH)
    pl.semaphore_signal(barrier, inc=1, device_id={'tp': partner}, device_id_type=MESH)

    with jax.named_scope("hid"):
        hid_copy(0).wait()
    for i in range(ln_half, n_ln):
        hid_copy(i).start()
    wkv_copy.start()
    with jax.named_scope("small"):
        for copy in small:
            copy.wait()
    gain[...] = gain_raw[...].astype(f32)
    bias[...] = bias_raw[...].astype(f32)
    bkv[...] = bkv_raw[...].astype(f32)
    bq[...] = bq_raw[...].astype(f32)
    bo[...] = bo_raw[...].astype(f32)

    def ln_block(i, carry):
        @pl.when(i > 0)
        def _():
            hid_copy(i).wait()

        @pl.when(i < SLOTS // 2)
        def _():
            for more in range(2):
                w_issue(i * 2 + more)

        rows = pl.ds(pl.multiple_of(i * LN_ROWS, LN_ROWS), LN_ROWS)
        n_col = d_model // 128

        def load(j):
            return y_ref[rows, j * 128:(j + 1) * 128].astype(f32)

        accs = [load(j) for j in range(4)]
        for j in range(4, n_col):
            accs[j % 4] = accs[j % 4] + load(j)
        mean = jnp.sum((accs[0] + accs[1]) + (accs[2] + accs[3]), axis=-1, keepdims=True) * (1.0 / d_model)
        mean = jnp.broadcast_to(mean, (LN_ROWS, 128))
        accs = [None] * 4
        for j in range(n_col):
            cen = load(j) - mean
            accs[j % 4] = cen * cen if accs[j % 4] is None else accs[j % 4] + cen * cen
        var = jnp.sum((accs[0] + accs[1]) + (accs[2] + accs[3]), axis=-1, keepdims=True) * (1.0 / d_model)
        rstd = jnp.broadcast_to(lax.rsqrt(var + LN_EPS), (LN_ROWS, 128))
        for j in range(n_col):
            out = (load(j) - mean) * rstd * gain[j:j + 1, :] + bias[j:j + 1, :]
            normed[rows, j * 128:(j + 1) * 128] = out.astype(bf16)
        return carry

    def kv_copy(src, h, dst):
        return pltpu.make_async_remote_copy(src_ref=kv_all.at[src, h], dst_ref=kv_all.at[src, h],
                                            send_sem=kv_send.at[dst, h], recv_sem=kv_recv.at[src, h],
                                            device_id={'cp': dst}, device_id_type=MESH)

    def seg_copy(src, dst):
        return pltpu.make_async_remote_copy(src_ref=seg_all.at[src], dst_ref=seg_all.at[src], send_sem=seg_send.at[dst],
                                            recv_sem=seg_recv.at[src], device_id={'cp': dst}, device_id_type=MESH)

    def late(dst):
        return (dst == n_cp - 1) & (my < n_cp // 2)

    def kv_half(h):
        with jax.named_scope("ln"):
            lax.fori_loop(h * ln_half, (h + 1) * ln_half, ln_block, 0)
        rows = pl.ds(h * HALF, HALF)
        if h == 0:
            wkv_copy.wait()
        with jax.named_scope("kvdot"):
            mid = d_model // 2
            low = jnp.dot(normed[rows, :mid], wkv[:mid, :], preferred_element_type=f32)
            high = jnp.dot(normed[rows, mid:], wkv[mid:, :], preferred_element_type=f32)
            k_own = ((low[:, :HEAD_DIM] + bkv[0:1, :]) + high[:, :HEAD_DIM]).astype(bf16)
            v_own = ((low[:, HEAD_DIM:] + bkv[1:2, :]) + high[:, HEAD_DIM:]).astype(bf16)
            kv_all[my, h, 0] = k_own
            kv_all[my, h, 1] = v_own.astype(f32).T.astype(bf16)
            k_ref[rows, :] = k_own
            v_ref[rows, :] = v_own
        if h == 0:
            with jax.named_scope("barrier"):
                pl.semaphore_wait(barrier, n_cp)
            for dst in range(1, n_cp):
                @pl.when(my < dst)
                def _():
                    seg_copy(my, dst).start()

        for dst in range(1, n_cp):
            @pl.when((my < dst) & jnp.logical_not(late(dst)))
            def _():
                kv_copy(my, h, dst).start()

    kv_half(0)

    @pl.when(my < n_cp)
    def _():
        for h in range(1, n_half):
            kv_half(h)

    def tile_copy(c, n):
        return pltpu.make_async_remote_copy(src_ref=send[c].at[n], dst_ref=recv[c].at[n], send_sem=tp_send.at[c, n],
                                            recv_sem=tp_recv.at[c, n], device_id={'tp': partner}, device_id_type=MESH)

    def chunk(c):
        base = c * items
        n_row = CHUNKS[c]
        first = sum(CHUNKS[:c])
        rows = slice(first, first + n_row)

        def q_wait(j):
            return [w_wait(base + j * k_halves + half) for half in range(k_halves)]

        def q_next(j):
            for half in range(k_halves):
                w_next(base + j * k_halves + half)

        def q_dot(j, slots):
            acc = None
            step = TILE_K // 2
            for half in range(k_halves):
                for n in range(2):
                    k0 = half * TILE_K + n * step
                    part = jnp.dot(normed[rows, k0:k0 + step], wbuf[slots[half], n * step:(n + 1) * step, :], preferred_element_type=f32)
                    acc = part if acc is None else acc + part
            return acc

        def q_store(j, acc):
            for i in range(TILE_N // 128):
                cols = pl.ds(pl.multiple_of(j * TILE_N + i * 128, 128), 128)
                row = j * (TILE_N // 128) + i
                qbuf[:, cols] = (acc[:, i * 128:(i + 1) * 128] + bq[pl.ds(row, 1), :]).astype(bf16)

        def q_tile(j, carry):
            with jax.named_scope("qtile"):
                q_store(j, q_dot(j, q_wait(j)))
                q_next(j)
            return carry

        own_keys = first + n_row

        def make_mask():
            if c == 0:
                for src in range(n_cp - 1):
                    @pl.when(src < my)
                    def _():
                        seg_copy(src, src).wait_recv()

            seg_q = jnp.broadcast_to(seg_all[my, c:c + 1, :].astype(f32), (128, 128)).T
            below[...] = jnp.zeros((128, 128), f32)
            for b in range(n_cp * tok // 128):
                src, part = b * 128 // tok, b % (tok // 128)

                @pl.when(b * 128 < my * tok + own_keys)
                def _():
                    below[...] += jnp.where(seg_all[src, part:part + 1, :].astype(f32) < seg_q, 1.0, 0.0)

            prompt = jnp.broadcast_to(jnp.sum(below[...], axis=1, keepdims=True), (128, 128)).T
            key = lax.broadcasted_iota(jnp.int32, (128, 128), 0)
            q_pos = my * tok + first + lax.broadcasted_iota(jnp.int32, (128, 128), 1)
            for b in range(n_cp * tok // 128):
                src, part = b * 128 // tok, b % (tok // 128)

                @pl.when(b * 128 < my * tok + own_keys)
                def _():
                    k_pos = key + b * 128
                    seen = (k_pos.astype(f32) >= prompt) & (k_pos <= q_pos)
                    mask[b * 128:(b + 1) * 128, :] = jnp.where(seen, 0.0, -jnp.inf)

        def heads(j, nb, beside=None):
            cols = pl.ds(pl.multiple_of(j * TILE_N, TILE_N), TILE_N)
            n_head = TILE_N // HEAD_DIM
            keys = nb * tok + own_keys
            parts = [kv_all.at[b * 128 // tok, b % (tok // 128)] for b in range(keys // 128)]
            k_blk = jnp.concatenate([part[0] for part in parts], axis=0)
            v_t = jnp.concatenate([part[1] for part in parts], axis=1)
            q_cols = qbuf[:, cols]
            q_rows = jnp.concatenate([q_cols[:, i * HEAD_DIM:(i + 1) * HEAD_DIM] for i in range(n_head)], axis=0)
            s = lax.dot_general(k_blk, q_rows, (((1,), (1,)), ((), ())), preferred_element_type=f32)
            other = beside() if beside else None
            s = s + jnp.concatenate([mask[:keys, :]] * n_head, axis=1)
            p_wts = jnp.exp2((s - jnp.max(s, axis=0, keepdims=True)) * EXP2_SCALE)
            l_sum = jnp.sum(p_wts, axis=0, keepdims=True)
            o = jnp.dot(v_t, p_wts.astype(bf16), preferred_element_type=f32) / l_sum
            obuf[:, cols] = jnp.concatenate([o[:, i * HEAD_DIM:(i + 1) * HEAD_DIM].T for i in range(n_head)], axis=1).astype(bf16)
            return other

        def attend(j, carry):
            for nb in range(n_cp):
                @pl.when(my == nb)
                def _():
                    with jax.named_scope("attn"):
                        heads(j, nb)
            return carry

        def both(j, carry):
            slots = q_wait(j)
            for nb in range(n_cp):
                @pl.when(my == nb)
                def _():
                    with jax.named_scope("both"):
                        q_store(j, heads(j - lag, nb, lambda: q_dot(j, slots)))
            q_next(j)
            return carry

        lag = jnp.where(my < n_cp // 2, 1, my)
        q_tile(0, 0)
        if c == 0:
            @pl.when(late(n_cp - 1))
            def _():
                for h in range(n_half):
                    kv_copy(my, h, n_cp - 1).start()

        lax.fori_loop(1, lag, q_tile, 0)
        with jax.named_scope("mask"):
            make_mask()
        if c == 0:
            with jax.named_scope("kvwait"):
                for src in range(n_cp - 1):
                    @pl.when(src < my)
                    def _():
                        for h in range(n_half):
                            kv_copy(src, h, src).wait_recv()
        if c == 0:
            lax.fori_loop(lag, q_tiles, both, 0)
        else:
            def turn(j, carry):
                return attend(j - lag, q_tile(j, carry))

            lax.fori_loop(lag, q_tiles, turn, 0)
        lax.fori_loop(q_tiles - lag, q_tiles, attend, 0)

        def o_tile(n, carry):
            with jax.named_scope("otile"):
                g = base + q_items + n
                slot = w_wait(g)
                send[c][n] = jnp.dot(obuf[:n_row, :], wbuf[slot], preferred_element_type=f32).astype(bf16)
                tile_copy(c, n).start()
                w_next(g)
            return carry

        lax.fori_loop(0, o_tiles, o_tile, 0)

    for c in range(n_chunk):
        chunk(c)

    for dst in range(1, n_cp):
        @pl.when(my < dst)
        def _():
            seg_copy(my, dst).wait_send()
            for h in range(n_half):
                kv_copy(my, h, dst).wait_send()

    for c in range(n_chunk):
        first = sum(CHUNKS[:c])
        rows = slice(first, first + CHUNKS[c])

        def finish(n, carry):
            copy = tile_copy(c, n)
            copy.wait_recv()
            copy.wait_send()
            for i in range(TILE_N // 128):
                cols = pl.ds(pl.multiple_of(n * TILE_N + i * 128, 128), 128)
                part = slice(i * 128, (i + 1) * 128)
                both = send[c][n, :, part].astype(f32) + recv[c][n, :, part].astype(f32)
                y_ref[rows, cols] = (y_ref[rows, cols].astype(f32) + both + bo[pl.ds(n * (TILE_N // 128) + i, 1), :]).astype(bf16)
            return carry

        with jax.named_scope("finish"):
            lax.fori_loop(0, o_tiles, finish, 0)


def close_kernel(y_ref, k_ref, v_ref, y_hbm, k_hbm, v_hbm, sem):
    rows = y_ref.shape[0] // 8
    copies = [pltpu.make_async_copy(k_ref, k_hbm, sem.at[8]), pltpu.make_async_copy(v_ref, v_hbm, sem.at[9])]
    copies += [pltpu.make_async_copy(y_ref.at[pl.ds(i * rows, rows), :], y_hbm.at[pl.ds(i * rows, rows), :], sem.at[i]) for i in range(8)]
    for copy in copies:
        copy.start()
    for copy in copies:
        copy.wait()


def solution(mesh):
    n_cp = mesh.shape['cp']

    def local_block(hidden, seg_ids, w_q, b_q, w_kv, b_kv, w_o, b_o, ln_gain, ln_bias):
        tok, d_model = hidden.shape
        q_width = w_q.shape[1]
        o_tiles = d_model // TILE_N
        vmem = pl.BlockSpec(memory_space=pltpu.VMEM)
        hbm = pl.BlockSpec(memory_space=pltpu.HBM)
        bf16, f32 = jnp.bfloat16, jnp.float32
        dma = pltpu.SemaphoreType.DMA
        flops = 2 * tok * d_model * (2 * q_width + 256)
        args = (hidden, seg_ids.reshape(-1, 128), w_q, b_q.reshape(-1, 128), w_kv, b_kv.reshape(-1, 128), w_o,
                b_o.reshape(-1, 128), ln_gain.reshape(-1, 128), ln_bias.reshape(-1, 128))
        args = tuple(pltpu.with_memory_space_constraint(a, pltpu.HBM) for a in args)
        rows = [q_width // 128, 2, d_model // 128, d_model // 128, d_model // 128]
        y, k, v = pl.pallas_call(
            functools.partial(block_kernel, n_cp),
            out_shape=(pltpu.VMEM((tok, d_model), bf16), pltpu.VMEM((tok, HEAD_DIM), bf16), pltpu.VMEM((tok, HEAD_DIM), bf16)),
            in_specs=[hbm] * len(args),
            out_specs=(vmem, vmem, vmem),
            scratch_shapes=[
                pltpu.VMEM((tok, d_model), bf16),
                pltpu.VMEM((d_model, 2 * HEAD_DIM), bf16),
                pltpu.VMEM((SLOTS, TILE_K, TILE_N), bf16),
                pltpu.VMEM((n_cp, tok // HALF, 2, HALF, HEAD_DIM), bf16),
                pltpu.VMEM((n_cp, tok // 128, 128), jnp.int32),
                pltpu.VMEM((128, 128), f32),
                pltpu.VMEM((n_cp * tok, 128), f32),
                pltpu.VMEM((max(CHUNKS), q_width), bf16),
                pltpu.VMEM((max(CHUNKS), q_width), bf16),
                *[pltpu.VMEM((o_tiles, r, TILE_N), bf16) for r in CHUNKS * 2],
                *[pltpu.VMEM((r, 128), bf16) for r in rows],
                *[pltpu.VMEM((r, 128), f32) for r in rows],
                dma((tok // LN_ROWS,)), dma, dma((6,)), dma((SLOTS,)),
                dma((n_cp, tok // HALF)), dma((n_cp, tok // HALF)), dma((n_cp,)), dma((n_cp,)),
                dma((len(CHUNKS), o_tiles)), dma((len(CHUNKS), o_tiles)),
            ],
            compiler_params=pltpu.CompilerParams(collective_id=0, has_side_effects=True, vmem_limit_bytes=56 * 1024 * 1024),
            cost_estimate=pl.CostEstimate(flops=flops, bytes_accessed=2 * 4 * d_model * q_width, transcendentals=0),
        )(*args)
        return pl.pallas_call(
            close_kernel,
            out_shape=tuple(jax.ShapeDtypeStruct(a.shape, bf16) for a in (y, k, v)),
            in_specs=[vmem] * 3,
            out_specs=(hbm,) * 3,
            scratch_shapes=[dma((10,))],
            cost_estimate=pl.CostEstimate(flops=1, bytes_accessed=4 * tok * d_model, transcendentals=0),
        )(*(pltpu.with_memory_space_constraint(a, pltpu.VMEM) for a in (y, k, v)))

    row_spec = P(('dp', 'cp'), None)
    tok_spec = P(('dp', 'cp'))
    return jax.shard_map(local_block, mesh=mesh,
                         in_specs=(row_spec, tok_spec, P(None, 'tp'), P('tp'), P(None, None), P(None), P('tp', None), P(None), P(None), P(None)),
                         out_specs=(row_spec, row_spec, row_spec), check_vma=False)
```

```python
import functools

import jax
import jax.numpy as jnp
from jax import lax
from jax.experimental import pallas as pl
from jax.experimental.pallas import tpu as pltpu
from jax.sharding import PartitionSpec as P

HEAD_DIM = 128
LN_EPS = 1e-5
EXP2_SCALE = HEAD_DIM ** -0.5 * 1.4426950408889634
MESH = pl.DeviceIdType.MESH

CHUNKS = (128, 128)
HALF = 128
TILE_K = 3072
TILE_N = 512
SLOTS = 9
LN_ROWS = 32


def block_kernel(n_cp, hid_hbm, seg_hbm, wq_hbm, bq_hbm, wkv_hbm, bkv_hbm, wo_hbm, bo_hbm, gain_hbm, bias_hbm,
                 y_ref, k_ref, v_ref,
                 normed, wkv, wbuf, kv_all, seg_all, below, mask, qbuf, obuf, send0, send1, recv0, recv1,
                 bq_raw, bkv_raw, bo_raw, gain_raw, bias_raw, bq, bkv, bo, gain, bias,
                 hid_sem, wkv_sem, small_sem, w_sem, kv_send, kv_recv, seg_send, seg_recv, tp_send, tp_recv):
    my = lax.axis_index('cp')
    partner = 1 - lax.axis_index('tp')
    tok, d_model = y_ref.shape
    q_width = qbuf.shape[1]
    n_chunk = len(CHUNKS)
    n_half = tok // HALF
    send, recv = (send0, send1), (recv0, recv1)
    q_tiles = q_width // TILE_N
    k_halves = d_model // TILE_K
    o_tiles = d_model // TILE_N
    q_items = q_tiles * k_halves
    items = q_items + o_tiles
    total = n_chunk * items
    f32, bf16 = jnp.float32, jnp.bfloat16

    def hid_copy(i):
        rows = pl.ds(i * LN_ROWS, LN_ROWS)
        return pltpu.make_async_copy(hid_hbm.at[rows, :], y_ref.at[rows, :], hid_sem.at[i])

    def w_issue(g):
        slot = lax.rem(g, SLOTS)
        item = lax.rem(g, items)

        @pl.when(item < q_items)
        def _():
            col = pl.multiple_of(lax.div(item, k_halves) * TILE_N, TILE_N)
            row = pl.multiple_of(lax.rem(item, k_halves) * TILE_K, TILE_K)
            pltpu.make_async_copy(wq_hbm.at[pl.ds(row, TILE_K), pl.ds(col, TILE_N)], wbuf.at[slot], w_sem.at[slot]).start()

        @pl.when(item >= q_items)
        def _():
            col = pl.multiple_of((item - q_items) * TILE_N, TILE_N)
            pltpu.make_async_copy(wo_hbm.at[:, pl.ds(col, TILE_N)], wbuf.at[slot], w_sem.at[slot]).start()

    def w_wait(g):
        slot = lax.rem(g, SLOTS)
        pltpu.make_async_copy(wo_hbm.at[:, pl.ds(0, TILE_N)], wbuf.at[slot], w_sem.at[slot]).wait()
        return slot

    def w_next(g):
        @pl.when(g + SLOTS < total)
        def _():
            w_issue(g + SLOTS)

    n_ln = tok // LN_ROWS
    ln_half = n_ln // n_half
    small = [pltpu.make_async_copy(src, dst, small_sem.at[i]) for i, (src, dst) in enumerate((
        (gain_hbm, gain_raw), (bias_hbm, bias_raw), (bkv_hbm, bkv_raw), (bq_hbm, bq_raw), (bo_hbm, bo_raw), (seg_hbm, seg_all.at[my])))]
    wkv_copy = pltpu.make_async_copy(wkv_hbm, wkv, wkv_sem)
    hid_copy(0).start()
    for copy in small:
        copy.start()
    for i in range(1, ln_half):
        hid_copy(i).start()

    barrier = pltpu.get_barrier_semaphore()
    for step in range(1, n_cp):
        pl.semaphore_signal(barrier, inc=1, device_id={'cp': lax.rem(my + step, n_cp)}, device_id_type=MESH)
    pl.semaphore_signal(barrier, inc=1, device_id={'tp': partner}, device_id_type=MESH)

    with jax.named_scope("hid"):
        hid_copy(0).wait()
    wkv_copy.start()
    for i in range(ln_half, n_ln):
        hid_copy(i).start()
    with jax.named_scope("small"):
        for copy in small:
            copy.wait()
    gain[...] = gain_raw[...].astype(f32)
    bias[...] = bias_raw[...].astype(f32)
    bkv[...] = bkv_raw[...].astype(f32)
    bq[...] = bq_raw[...].astype(f32)
    bo[...] = bo_raw[...].astype(f32)

    def ln_block(i, carry):
        @pl.when(i > 0)
        def _():
            hid_copy(i).wait()

        @pl.when((i > 0) & (i < ln_half))
        def _():
            w_issue(i - 1)

        @pl.when((i >= ln_half) & (i < SLOTS - 2))
        def _():
            for more in range(2):
                w_issue(i * 2 + more - ln_half - 1)

        rows = pl.ds(pl.multiple_of(i * LN_ROWS, LN_ROWS), LN_ROWS)
        n_col = d_model // 128

        def load(j):
            return y_ref[rows, j * 128:(j + 1) * 128].astype(f32)

        accs = [load(j) for j in range(4)]
        for j in range(4, n_col):
            accs[j % 4] = accs[j % 4] + load(j)
        mean = jnp.sum((accs[0] + accs[1]) + (accs[2] + accs[3]), axis=-1, keepdims=True) * (1.0 / d_model)
        mean = jnp.broadcast_to(mean, (LN_ROWS, 128))
        accs = [None] * 4
        for j in range(n_col):
            cen = load(j) - mean
            accs[j % 4] = cen * cen if accs[j % 4] is None else accs[j % 4] + cen * cen
        var = jnp.sum((accs[0] + accs[1]) + (accs[2] + accs[3]), axis=-1, keepdims=True) * (1.0 / d_model)
        rstd = jnp.broadcast_to(lax.rsqrt(var + LN_EPS), (LN_ROWS, 128))
        for j in range(n_col):
            out = (load(j) - mean) * rstd * gain[j:j + 1, :] + bias[j:j + 1, :]
            normed[rows, j * 128:(j + 1) * 128] = out.astype(bf16)
        return carry

    def kv_copy(src, h, dst):
        return pltpu.make_async_remote_copy(src_ref=kv_all.at[src, h], dst_ref=kv_all.at[src, h],
                                            send_sem=kv_send.at[dst, h], recv_sem=kv_recv.at[src, h],
                                            device_id={'cp': dst}, device_id_type=MESH)

    def seg_copy(src, dst):
        return pltpu.make_async_remote_copy(src_ref=seg_all.at[src], dst_ref=seg_all.at[src], send_sem=seg_send.at[dst],
                                            recv_sem=seg_recv.at[src], device_id={'cp': dst}, device_id_type=MESH)

    def late(dst):
        return (dst == n_cp - 1) & (my < n_cp // 2)

    def kv_half(h):
        with jax.named_scope("ln"):
            lax.fori_loop(h * ln_half, (h + 1) * ln_half, ln_block, 0)
        rows = pl.ds(h * HALF, HALF)
        if h == 0:
            wkv_copy.wait()
        with jax.named_scope("kvdot"):
            mid = d_model // 2
            low = jnp.dot(normed[rows, :mid], wkv[:mid, :], preferred_element_type=f32)
            high = jnp.dot(normed[rows, mid:], wkv[mid:, :], preferred_element_type=f32)
            k_own = ((low[:, :HEAD_DIM] + bkv[0:1, :]) + high[:, :HEAD_DIM]).astype(bf16)
            v_own = ((low[:, HEAD_DIM:] + bkv[1:2, :]) + high[:, HEAD_DIM:]).astype(bf16)
            kv_all[my, h, 0] = k_own
            kv_all[my, h, 1] = v_own.astype(f32).T.astype(bf16)
            k_ref[rows, :] = k_own
            v_ref[rows, :] = v_own
        if h == 0:
            with jax.named_scope("barrier"):
                pl.semaphore_wait(barrier, n_cp)
            for dst in range(1, n_cp):
                @pl.when(my < dst)
                def _():
                    seg_copy(my, dst).start()

        for dst in range(1, n_cp):
            @pl.when((my < dst) & jnp.logical_not(late(dst)))
            def _():
                kv_copy(my, h, dst).start()

    kv_half(0)

    @pl.when(my < n_cp)
    def _():
        for h in range(1, n_half):
            kv_half(h)

    def tile_copy(c, n):
        return pltpu.make_async_remote_copy(src_ref=send[c].at[n], dst_ref=recv[c].at[n], send_sem=tp_send.at[c, n],
                                            recv_sem=tp_recv.at[c, n], device_id={'tp': partner}, device_id_type=MESH)

    def chunk(c):
        base = c * items
        n_row = CHUNKS[c]
        first = sum(CHUNKS[:c])
        rows = slice(first, first + n_row)

        def q_wait(j):
            return [w_wait(base + j * k_halves + half) for half in range(k_halves)]

        def q_next(j):
            for half in range(k_halves):
                w_next(base + j * k_halves + half)

        def q_dot(j, slots):
            acc = None
            step = TILE_K // 2
            for half in range(k_halves):
                for n in range(2):
                    k0 = half * TILE_K + n * step
                    part = jnp.dot(normed[rows, k0:k0 + step], wbuf[slots[half], n * step:(n + 1) * step, :], preferred_element_type=f32)
                    acc = part if acc is None else acc + part
            return acc

        def q_store(j, acc):
            for i in range(TILE_N // 128):
                cols = pl.ds(pl.multiple_of(j * TILE_N + i * 128, 128), 128)
                row = j * (TILE_N // 128) + i
                qbuf[:, cols] = (acc[:, i * 128:(i + 1) * 128] + bq[pl.ds(row, 1), :]).astype(bf16)

        def q_tile(j, carry):
            with jax.named_scope("qtile"):
                acc = None
                step = TILE_K // 2
                for half in range(k_halves):
                    slot = w_wait(base + j * k_halves + half)
                    for n in range(2):
                        k0 = half * TILE_K + n * step
                        part = jnp.dot(normed[rows, k0:k0 + step], wbuf[slot, n * step:(n + 1) * step, :], preferred_element_type=f32)
                        acc = part if acc is None else acc + part
                    w_next(base + j * k_halves + half)
                q_store(j, acc)
            return carry

        own_keys = first + n_row

        def make_mask():
            if c == 0:
                for src in range(n_cp - 1):
                    @pl.when(src < my)
                    def _():
                        seg_copy(src, src).wait_recv()

            seg_q = jnp.broadcast_to(seg_all[my, c:c + 1, :].astype(f32), (128, 128)).T
            below[...] = jnp.zeros((128, 128), f32)
            for b in range(n_cp * tok // 128):
                src, part = b * 128 // tok, b % (tok // 128)

                @pl.when(b * 128 < my * tok + own_keys)
                def _():
                    below[...] += jnp.where(seg_all[src, part:part + 1, :].astype(f32) < seg_q, 1.0, 0.0)

            prompt = jnp.broadcast_to(jnp.sum(below[...], axis=1, keepdims=True), (128, 128)).T
            key = lax.broadcasted_iota(jnp.int32, (128, 128), 0)
            q_pos = my * tok + first + lax.broadcasted_iota(jnp.int32, (128, 128), 1)
            for b in range(n_cp * tok // 128):
                src, part = b * 128 // tok, b % (tok // 128)

                @pl.when(b * 128 < my * tok + own_keys)
                def _():
                    k_pos = key + b * 128
                    seen = (k_pos.astype(f32) >= prompt) & (k_pos <= q_pos)
                    mask[b * 128:(b + 1) * 128, :] = jnp.where(seen, 0.0, -jnp.inf)

        def heads(j, nb, beside=None):
            cols = pl.ds(pl.multiple_of(j * TILE_N, TILE_N), TILE_N)
            n_head = TILE_N // HEAD_DIM
            keys = nb * tok + own_keys
            parts = [kv_all.at[b * 128 // tok, b % (tok // 128)] for b in range(keys // 128)]
            k_blk = jnp.concatenate([part[0] for part in parts], axis=0)
            v_t = jnp.concatenate([part[1] for part in parts], axis=1)
            q_cols = qbuf[:, cols]
            q_rows = jnp.concatenate([q_cols[:, i * HEAD_DIM:(i + 1) * HEAD_DIM] for i in range(n_head)], axis=0)
            s = lax.dot_general(k_blk, q_rows, (((1,), (1,)), ((), ())), preferred_element_type=f32)
            other = beside() if beside else None
            s = s + jnp.concatenate([mask[:keys, :]] * n_head, axis=1)
            p_wts = jnp.exp2((s - jnp.max(s, axis=0, keepdims=True)) * EXP2_SCALE)
            l_sum = jnp.sum(p_wts, axis=0, keepdims=True)
            o = jnp.dot(v_t, p_wts.astype(bf16), preferred_element_type=f32) / l_sum
            obuf[:, cols] = jnp.concatenate([o[:, i * HEAD_DIM:(i + 1) * HEAD_DIM].T for i in range(n_head)], axis=1).astype(bf16)
            return other

        def attend(j, carry):
            for nb in range(n_cp):
                @pl.when(my == nb)
                def _():
                    with jax.named_scope("attn"):
                        heads(j, nb)
            return carry

        def both(j, carry):
            slots = q_wait(j)
            for nb in range(n_cp // 2, n_cp):
                @pl.when(my == nb)
                def _():
                    with jax.named_scope("both"):
                        q_store(j, heads(j - lag, nb, lambda: q_dot(j, slots)))
            q_next(j)
            return carry

        lag = jnp.where(my < n_cp // 2, 1, my)
        q_tile(0, 0)
        if c == 0:
            @pl.when(late(n_cp - 1))
            def _():
                for h in range(n_half):
                    kv_copy(my, h, n_cp - 1).start()

        lax.fori_loop(1, lag, q_tile, 0)
        with jax.named_scope("mask"):
            make_mask()
        if c == 0:
            with jax.named_scope("kvwait"):
                for src in range(n_cp - 1):
                    @pl.when(src < my)
                    def _():
                        for h in range(n_half):
                            kv_copy(src, h, src).wait_recv()
        def turn(j, carry):
            return q_tile(j, attend(j - lag, carry))

        split = jnp.where(my < n_cp // 2, q_tiles, lag) if c == 0 else q_tiles
        lax.fori_loop(lag, split, turn, 0)
        if c == 0:
            lax.fori_loop(split, q_tiles, both, 0)
        lax.fori_loop(q_tiles - lag, q_tiles, attend, 0)

        def o_tile(n, carry):
            with jax.named_scope("otile"):
                g = base + q_items + n
                slot = w_wait(g)
                send[c][n] = jnp.dot(obuf[:n_row, :], wbuf[slot], preferred_element_type=f32).astype(bf16)
                tile_copy(c, n).start()
                w_next(g)
            return carry

        lax.fori_loop(0, o_tiles, o_tile, 0)

    for c in range(n_chunk):
        chunk(c)

    for dst in range(1, n_cp):
        @pl.when(my < dst)
        def _():
            seg_copy(my, dst).wait_send()
            for h in range(n_half):
                kv_copy(my, h, dst).wait_send()

    for c in range(n_chunk):
        first = sum(CHUNKS[:c])
        rows = slice(first, first + CHUNKS[c])

        def finish(n, carry):
            copy = tile_copy(c, n)
            copy.wait_recv()
            copy.wait_send()
            for i in range(TILE_N // 128):
                cols = pl.ds(pl.multiple_of(n * TILE_N + i * 128, 128), 128)
                part = slice(i * 128, (i + 1) * 128)
                both = send[c][n, :, part].astype(f32) + recv[c][n, :, part].astype(f32)
                y_ref[rows, cols] = (y_ref[rows, cols].astype(f32) + both + bo[pl.ds(n * (TILE_N // 128) + i, 1), :]).astype(bf16)
            return carry

        with jax.named_scope("finish"):
            lax.fori_loop(0, o_tiles, finish, 0)


def close_kernel(y_ref, k_ref, v_ref, y_hbm, k_hbm, v_hbm, sem):
    rows = y_ref.shape[0] // 8
    copies = [pltpu.make_async_copy(k_ref, k_hbm, sem.at[8]), pltpu.make_async_copy(v_ref, v_hbm, sem.at[9])]
    copies += [pltpu.make_async_copy(y_ref.at[pl.ds(i * rows, rows), :], y_hbm.at[pl.ds(i * rows, rows), :], sem.at[i]) for i in range(8)]
    for copy in copies:
        copy.start()
    for copy in copies:
        copy.wait()


def solution(mesh):
    n_cp = mesh.shape['cp']

    def local_block(hidden, seg_ids, w_q, b_q, w_kv, b_kv, w_o, b_o, ln_gain, ln_bias):
        tok, d_model = hidden.shape
        q_width = w_q.shape[1]
        o_tiles = d_model // TILE_N
        vmem = pl.BlockSpec(memory_space=pltpu.VMEM)
        hbm = pl.BlockSpec(memory_space=pltpu.HBM)
        bf16, f32 = jnp.bfloat16, jnp.float32
        dma = pltpu.SemaphoreType.DMA
        flops = 2 * tok * d_model * (2 * q_width + 256)
        args = (hidden, seg_ids.reshape(-1, 128), w_q, b_q.reshape(-1, 128), w_kv, b_kv.reshape(-1, 128), w_o,
                b_o.reshape(-1, 128), ln_gain.reshape(-1, 128), ln_bias.reshape(-1, 128))
        args = tuple(pltpu.with_memory_space_constraint(a, pltpu.HBM) for a in args)
        rows = [q_width // 128, 2, d_model // 128, d_model // 128, d_model // 128]
        y, k, v = pl.pallas_call(
            functools.partial(block_kernel, n_cp),
            out_shape=(pltpu.VMEM((tok, d_model), bf16), pltpu.VMEM((tok, HEAD_DIM), bf16), pltpu.VMEM((tok, HEAD_DIM), bf16)),
            in_specs=[hbm] * len(args),
            out_specs=(vmem, vmem, vmem),
            scratch_shapes=[
                pltpu.VMEM((tok, d_model), bf16),
                pltpu.VMEM((d_model, 2 * HEAD_DIM), bf16),
                pltpu.VMEM((SLOTS, TILE_K, TILE_N), bf16),
                pltpu.VMEM((n_cp, tok // HALF, 2, HALF, HEAD_DIM), bf16),
                pltpu.VMEM((n_cp, tok // 128, 128), jnp.int32),
                pltpu.VMEM((128, 128), f32),
                pltpu.VMEM((n_cp * tok, 128), f32),
                pltpu.VMEM((max(CHUNKS), q_width), bf16),
                pltpu.VMEM((max(CHUNKS), q_width), bf16),
                *[pltpu.VMEM((o_tiles, r, TILE_N), bf16) for r in CHUNKS * 2],
                *[pltpu.VMEM((r, 128), bf16) for r in rows],
                *[pltpu.VMEM((r, 128), f32) for r in rows],
                dma((tok // LN_ROWS,)), dma, dma((6,)), dma((SLOTS,)),
                dma((n_cp, tok // HALF)), dma((n_cp, tok // HALF)), dma((n_cp,)), dma((n_cp,)),
                dma((len(CHUNKS), o_tiles)), dma((len(CHUNKS), o_tiles)),
            ],
            compiler_params=pltpu.CompilerParams(collective_id=0, has_side_effects=True, vmem_limit_bytes=56 * 1024 * 1024),
            cost_estimate=pl.CostEstimate(flops=flops, bytes_accessed=2 * 4 * d_model * q_width, transcendentals=0),
        )(*args)
        return pl.pallas_call(
            close_kernel,
            out_shape=tuple(jax.ShapeDtypeStruct(a.shape, bf16) for a in (y, k, v)),
            in_specs=[vmem] * 3,
            out_specs=(hbm,) * 3,
            scratch_shapes=[dma((10,))],
            cost_estimate=pl.CostEstimate(flops=1, bytes_accessed=4 * tok * d_model, transcendentals=0),
        )(*(pltpu.with_memory_space_constraint(a, pltpu.VMEM) for a in (y, k, v)))

    row_spec = P(('dp', 'cp'), None)
    tok_spec = P(('dp', 'cp'))
    return jax.shard_map(local_block, mesh=mesh,
                         in_specs=(row_spec, tok_spec, P(None, 'tp'), P('tp'), P(None, None), P(None), P('tp', None), P(None), P(None), P(None)),
                         out_specs=(row_spec, row_spec, row_spec), check_vma=False)
```

```python
import functools

import jax
import jax.numpy as jnp
from jax import lax
from jax.experimental import pallas as pl
from jax.experimental.pallas import tpu as pltpu
from jax.sharding import PartitionSpec as P

HEAD_DIM = 128
LN_EPS = 1e-5
EXP2_SCALE = HEAD_DIM ** -0.5 * 1.4426950408889634
MESH = pl.DeviceIdType.MESH

CHUNKS = (128, 128)
HALF = 128
TILE_K = 3072
TILE_N = 512
SLOTS = 9
LN_ROWS = 32
WKV_PARTS = 6


def block_kernel(n_cp, hid_hbm, seg_hbm, wq_hbm, bq_hbm, wkv_hbm, bkv_hbm, wo_hbm, bo_hbm, gain_hbm, bias_hbm,
                 y_ref, k_ref, v_ref,
                 normed, wkv, wbuf, kv_all, seg_all, below, mask, qbuf, obuf, send0, send1, recv0, recv1,
                 bq_raw, bkv_raw, bo_raw, gain_raw, bias_raw, bq, bkv, bo, gain, bias,
                 hid_sem, wkv_sem, small_sem, w_sem, kv_send, kv_recv, seg_send, seg_recv, tp_send, tp_recv):
    my = lax.axis_index('cp')
    partner = 1 - lax.axis_index('tp')
    tok, d_model = y_ref.shape
    q_width = qbuf.shape[1]
    n_chunk = len(CHUNKS)
    n_half = tok // HALF
    send, recv = (send0, send1), (recv0, recv1)
    q_tiles = q_width // TILE_N
    k_halves = d_model // TILE_K
    o_tiles = d_model // TILE_N
    q_items = q_tiles * k_halves
    items = q_items + o_tiles
    total = n_chunk * items
    f32, bf16 = jnp.float32, jnp.bfloat16

    def hid_copy(i):
        rows = pl.ds(i * LN_ROWS, LN_ROWS)
        return pltpu.make_async_copy(hid_hbm.at[rows, :], y_ref.at[rows, :], hid_sem.at[i])

    def w_issue(g):
        slot = lax.rem(g, SLOTS)
        item = lax.rem(g, items)

        @pl.when(item < q_items)
        def _():
            col = pl.multiple_of(lax.div(item, k_halves) * TILE_N, TILE_N)
            row = pl.multiple_of(lax.rem(item, k_halves) * TILE_K, TILE_K)
            pltpu.make_async_copy(wq_hbm.at[pl.ds(row, TILE_K), pl.ds(col, TILE_N)], wbuf.at[slot], w_sem.at[slot]).start()

        @pl.when(item >= q_items)
        def _():
            col = pl.multiple_of((item - q_items) * TILE_N, TILE_N)
            pltpu.make_async_copy(wo_hbm.at[:, pl.ds(col, TILE_N)], wbuf.at[slot], w_sem.at[slot]).start()

    def w_wait(g):
        slot = lax.rem(g, SLOTS)
        pltpu.make_async_copy(wo_hbm.at[:, pl.ds(0, TILE_N)], wbuf.at[slot], w_sem.at[slot]).wait()
        return slot

    def w_next(g):
        @pl.when(g + SLOTS < total)
        def _():
            w_issue(g + SLOTS)

    n_ln = tok // LN_ROWS
    ln_half = n_ln // n_half
    small = [pltpu.make_async_copy(src, dst, small_sem.at[i]) for i, (src, dst) in enumerate((
        (gain_hbm, gain_raw), (bias_hbm, bias_raw), (bkv_hbm, bkv_raw), (bq_hbm, bq_raw), (bo_hbm, bo_raw), (seg_hbm, seg_all.at[my])))]
    wkv_rows = d_model // WKV_PARTS
    wkv_copies = [pltpu.make_async_copy(wkv_hbm.at[pl.ds(i * wkv_rows, wkv_rows), :], wkv.at[pl.ds(i * wkv_rows, wkv_rows), :], wkv_sem.at[i])
                  for i in range(WKV_PARTS)]
    hid_copy(0).start()
    for copy in small:
        copy.start()
    for i in range(1, ln_half):
        hid_copy(i).start()

    barrier = pltpu.get_barrier_semaphore()
    for step in range(1, n_cp):
        pl.semaphore_signal(barrier, inc=1, device_id={'cp': lax.rem(my + step, n_cp)}, device_id_type=MESH)
    pl.semaphore_signal(barrier, inc=1, device_id={'tp': partner}, device_id_type=MESH)

    with jax.named_scope("hid"):
        hid_copy(0).wait()
    for copy in wkv_copies:
        copy.start()
    for i in range(ln_half, n_ln):
        hid_copy(i).start()
    with jax.named_scope("small"):
        for copy in small:
            copy.wait()
    gain[...] = gain_raw[...].astype(f32)
    bias[...] = bias_raw[...].astype(f32)
    bkv[...] = bkv_raw[...].astype(f32)
    bq[...] = bq_raw[...].astype(f32)
    bo[...] = bo_raw[...].astype(f32)

    def ln_block(i, carry):
        @pl.when(i > 0)
        def _():
            hid_copy(i).wait()

        @pl.when((i > 0) & (i < ln_half))
        def _():
            w_issue(i - 1)

        @pl.when((i >= ln_half) & (i < SLOTS - 2))
        def _():
            for more in range(2):
                w_issue(i * 2 + more - ln_half - 1)

        rows = pl.ds(pl.multiple_of(i * LN_ROWS, LN_ROWS), LN_ROWS)
        n_col = d_model // 128

        def load(j):
            return y_ref[rows, j * 128:(j + 1) * 128].astype(f32)

        accs = [load(j) for j in range(4)]
        for j in range(4, n_col):
            accs[j % 4] = accs[j % 4] + load(j)
        mean = jnp.sum((accs[0] + accs[1]) + (accs[2] + accs[3]), axis=-1, keepdims=True) * (1.0 / d_model)
        mean = jnp.broadcast_to(mean, (LN_ROWS, 128))
        accs = [None] * 4
        for j in range(n_col):
            cen = load(j) - mean
            accs[j % 4] = cen * cen if accs[j % 4] is None else accs[j % 4] + cen * cen
        var = jnp.sum((accs[0] + accs[1]) + (accs[2] + accs[3]), axis=-1, keepdims=True) * (1.0 / d_model)
        rstd = jnp.broadcast_to(lax.rsqrt(var + LN_EPS), (LN_ROWS, 128))
        for j in range(n_col):
            out = (load(j) - mean) * rstd * gain[j:j + 1, :] + bias[j:j + 1, :]
            normed[rows, j * 128:(j + 1) * 128] = out.astype(bf16)
        return carry

    def kv_copy(src, h, dst):
        return pltpu.make_async_remote_copy(src_ref=kv_all.at[src, h], dst_ref=kv_all.at[src, h],
                                            send_sem=kv_send.at[dst, h], recv_sem=kv_recv.at[src, h],
                                            device_id={'cp': dst}, device_id_type=MESH)

    def seg_copy(src, dst):
        return pltpu.make_async_remote_copy(src_ref=seg_all.at[src], dst_ref=seg_all.at[src], send_sem=seg_send.at[dst],
                                            recv_sem=seg_recv.at[src], device_id={'cp': dst}, device_id_type=MESH)

    def late(dst):
        return (dst == n_cp - 1) & (my < n_cp // 2)

    def kv_half(h):
        with jax.named_scope("ln"):
            lax.fori_loop(h * ln_half, (h + 1) * ln_half, ln_block, 0)
        rows = pl.ds(h * HALF, HALF)
        if h == 0:
            for copy in wkv_copies:
                copy.wait()
        with jax.named_scope("kvdot"):
            mid = d_model // 2
            low = jnp.dot(normed[rows, :mid], wkv[:mid, :], preferred_element_type=f32)
            high = jnp.dot(normed[rows, mid:], wkv[mid:, :], preferred_element_type=f32)
            k_own = ((low[:, :HEAD_DIM] + bkv[0:1, :]) + high[:, :HEAD_DIM]).astype(bf16)
            v_own = ((low[:, HEAD_DIM:] + bkv[1:2, :]) + high[:, HEAD_DIM:]).astype(bf16)
            kv_all[my, h, 0] = k_own
            kv_all[my, h, 1] = v_own.astype(f32).T.astype(bf16)
            k_ref[rows, :] = k_own
            v_ref[rows, :] = v_own
        if h == 0:
            with jax.named_scope("barrier"):
                pl.semaphore_wait(barrier, n_cp)
            for dst in range(1, n_cp):
                @pl.when(my < dst)
                def _():
                    seg_copy(my, dst).start()

        for dst in range(1, n_cp):
            @pl.when((my < dst) & jnp.logical_not(late(dst)))
            def _():
                kv_copy(my, h, dst).start()

    kv_half(0)

    @pl.when(my < n_cp)
    def _():
        for h in range(1, n_half):
            kv_half(h)

    def tile_copy(c, n):
        return pltpu.make_async_remote_copy(src_ref=send[c].at[n], dst_ref=recv[c].at[n], send_sem=tp_send.at[c, n],
                                            recv_sem=tp_recv.at[c, n], device_id={'tp': partner}, device_id_type=MESH)

    def chunk(c):
        base = c * items
        n_row = CHUNKS[c]
        first = sum(CHUNKS[:c])
        rows = slice(first, first + n_row)

        def q_wait(j):
            return [w_wait(base + j * k_halves + half) for half in range(k_halves)]

        def q_next(j):
            for half in range(k_halves):
                w_next(base + j * k_halves + half)

        def q_dot(j, slots):
            acc = None
            step = TILE_K // 2
            for half in range(k_halves):
                for n in range(2):
                    k0 = half * TILE_K + n * step
                    part = jnp.dot(normed[rows, k0:k0 + step], wbuf[slots[half], n * step:(n + 1) * step, :], preferred_element_type=f32)
                    acc = part if acc is None else acc + part
            return acc

        def q_store(j, acc):
            for i in range(TILE_N // 128):
                cols = pl.ds(pl.multiple_of(j * TILE_N + i * 128, 128), 128)
                row = j * (TILE_N // 128) + i
                qbuf[:, cols] = (acc[:, i * 128:(i + 1) * 128] + bq[pl.ds(row, 1), :]).astype(bf16)

        def q_tile(j, carry):
            with jax.named_scope("qtile"):
                acc = None
                step = TILE_K // 2
                for half in range(k_halves):
                    slot = w_wait(base + j * k_halves + half)
                    for n in range(2):
                        k0 = half * TILE_K + n * step
                        part = jnp.dot(normed[rows, k0:k0 + step], wbuf[slot, n * step:(n + 1) * step, :], preferred_element_type=f32)
                        acc = part if acc is None else acc + part
                    w_next(base + j * k_halves + half)
                q_store(j, acc)
            return carry

        own_keys = first + n_row

        def make_mask():
            if c == 0:
                for src in range(n_cp - 1):
                    @pl.when(src < my)
                    def _():
                        seg_copy(src, src).wait_recv()

            seg_q = jnp.broadcast_to(seg_all[my, c:c + 1, :].astype(f32), (128, 128)).T
            below[...] = jnp.zeros((128, 128), f32)
            for b in range(n_cp * tok // 128):
                src, part = b * 128 // tok, b % (tok // 128)

                @pl.when(b * 128 < my * tok + own_keys)
                def _():
                    below[...] += jnp.where(seg_all[src, part:part + 1, :].astype(f32) < seg_q, 1.0, 0.0)

            prompt = jnp.broadcast_to(jnp.sum(below[...], axis=1, keepdims=True), (128, 128)).T
            key = lax.broadcasted_iota(jnp.int32, (128, 128), 0)
            q_pos = my * tok + first + lax.broadcasted_iota(jnp.int32, (128, 128), 1)
            for b in range(n_cp * tok // 128):
                src, part = b * 128 // tok, b % (tok // 128)

                @pl.when(b * 128 < my * tok + own_keys)
                def _():
                    k_pos = key + b * 128
                    seen = (k_pos.astype(f32) >= prompt) & (k_pos <= q_pos)
                    mask[b * 128:(b + 1) * 128, :] = jnp.where(seen, 0.0, -jnp.inf)

        def heads(j, nb, beside=None):
            cols = pl.ds(pl.multiple_of(j * TILE_N, TILE_N), TILE_N)
            n_head = TILE_N // HEAD_DIM
            keys = nb * tok + own_keys
            parts = [kv_all.at[b * 128 // tok, b % (tok // 128)] for b in range(keys // 128)]
            k_blk = jnp.concatenate([part[0] for part in parts], axis=0)
            v_t = jnp.concatenate([part[1] for part in parts], axis=1)
            q_cols = qbuf[:, cols]
            q_rows = jnp.concatenate([q_cols[:, i * HEAD_DIM:(i + 1) * HEAD_DIM] for i in range(n_head)], axis=0)
            s = lax.dot_general(k_blk, q_rows, (((1,), (1,)), ((), ())), preferred_element_type=f32)
            other = beside() if beside else None
            s = s + jnp.concatenate([mask[:keys, :]] * n_head, axis=1)
            p_wts = jnp.exp2((s - jnp.max(s, axis=0, keepdims=True)) * EXP2_SCALE)
            l_sum = jnp.sum(p_wts, axis=0, keepdims=True)
            o = jnp.dot(v_t, p_wts.astype(bf16), preferred_element_type=f32) / l_sum
            obuf[:, cols] = jnp.concatenate([o[:, i * HEAD_DIM:(i + 1) * HEAD_DIM].T for i in range(n_head)], axis=1).astype(bf16)
            return other

        def attend(j, carry):
            for nb in range(n_cp):
                @pl.when(my == nb)
                def _():
                    with jax.named_scope("attn"):
                        heads(j, nb)
            return carry

        def both(j, carry):
            slots = q_wait(j)
            for nb in range(n_cp // 2, n_cp):
                @pl.when(my == nb)
                def _():
                    with jax.named_scope("both"):
                        q_store(j, heads(j - lag, nb, lambda: q_dot(j, slots)))
            q_next(j)
            return carry

        lag = jnp.where(my < n_cp // 2, 1, my)
        q_tile(0, 0)
        if c == 0:
            @pl.when(late(n_cp - 1))
            def _():
                for h in range(n_half):
                    kv_copy(my, h, n_cp - 1).start()

        lax.fori_loop(1, lag, q_tile, 0)
        with jax.named_scope("mask"):
            make_mask()
        if c == 0:
            with jax.named_scope("kvwait"):
                for src in range(n_cp - 1):
                    @pl.when(src < my)
                    def _():
                        for h in range(n_half):
                            kv_copy(src, h, src).wait_recv()
        def turn(j, carry):
            return q_tile(j, attend(j - lag, carry))

        split = jnp.where(my < n_cp // 2, q_tiles, lag) if c == 0 else q_tiles
        lax.fori_loop(lag, split, turn, 0)
        if c == 0:
            lax.fori_loop(split, q_tiles, both, 0)
        lax.fori_loop(q_tiles - lag, q_tiles, attend, 0)

        def o_tile(n, carry):
            with jax.named_scope("otile"):
                g = base + q_items + n
                slot = w_wait(g)
                send[c][n] = jnp.dot(obuf[:n_row, :], wbuf[slot], preferred_element_type=f32).astype(bf16)
                tile_copy(c, n).start()
                w_next(g)
            return carry

        lax.fori_loop(0, o_tiles, o_tile, 0)

    for c in range(n_chunk):
        chunk(c)

    for dst in range(1, n_cp):
        @pl.when(my < dst)
        def _():
            seg_copy(my, dst).wait_send()
            for h in range(n_half):
                kv_copy(my, h, dst).wait_send()

    for c in range(n_chunk):
        first = sum(CHUNKS[:c])
        rows = slice(first, first + CHUNKS[c])

        def finish(n, carry):
            copy = tile_copy(c, n)
            copy.wait_recv()
            copy.wait_send()
            for i in range(TILE_N // 128):
                cols = pl.ds(pl.multiple_of(n * TILE_N + i * 128, 128), 128)
                part = slice(i * 128, (i + 1) * 128)
                both = send[c][n, :, part].astype(f32) + recv[c][n, :, part].astype(f32)
                y_ref[rows, cols] = (y_ref[rows, cols].astype(f32) + both + bo[pl.ds(n * (TILE_N // 128) + i, 1), :]).astype(bf16)
            return carry

        with jax.named_scope("finish"):
            lax.fori_loop(0, o_tiles, finish, 0)


def close_kernel(y_ref, k_ref, v_ref, y_hbm, k_hbm, v_hbm, sem):
    rows = y_ref.shape[0] // 8
    copies = [pltpu.make_async_copy(k_ref, k_hbm, sem.at[8]), pltpu.make_async_copy(v_ref, v_hbm, sem.at[9])]
    copies += [pltpu.make_async_copy(y_ref.at[pl.ds(i * rows, rows), :], y_hbm.at[pl.ds(i * rows, rows), :], sem.at[i]) for i in range(8)]
    for copy in copies:
        copy.start()
    for copy in copies:
        copy.wait()


def solution(mesh):
    n_cp = mesh.shape['cp']

    def local_block(hidden, seg_ids, w_q, b_q, w_kv, b_kv, w_o, b_o, ln_gain, ln_bias):
        tok, d_model = hidden.shape
        q_width = w_q.shape[1]
        o_tiles = d_model // TILE_N
        vmem = pl.BlockSpec(memory_space=pltpu.VMEM)
        hbm = pl.BlockSpec(memory_space=pltpu.HBM)
        bf16, f32 = jnp.bfloat16, jnp.float32
        dma = pltpu.SemaphoreType.DMA
        flops = 2 * tok * d_model * (2 * q_width + 256)
        args = (hidden, seg_ids.reshape(-1, 128), w_q, b_q.reshape(-1, 128), w_kv, b_kv.reshape(-1, 128), w_o,
                b_o.reshape(-1, 128), ln_gain.reshape(-1, 128), ln_bias.reshape(-1, 128))
        args = tuple(pltpu.with_memory_space_constraint(a, pltpu.HBM) for a in args)
        rows = [q_width // 128, 2, d_model // 128, d_model // 128, d_model // 128]
        y, k, v = pl.pallas_call(
            functools.partial(block_kernel, n_cp),
            out_shape=(pltpu.VMEM((tok, d_model), bf16), pltpu.VMEM((tok, HEAD_DIM), bf16), pltpu.VMEM((tok, HEAD_DIM), bf16)),
            in_specs=[hbm] * len(args),
            out_specs=(vmem, vmem, vmem),
            scratch_shapes=[
                pltpu.VMEM((tok, d_model), bf16),
                pltpu.VMEM((d_model, 2 * HEAD_DIM), bf16),
                pltpu.VMEM((SLOTS, TILE_K, TILE_N), bf16),
                pltpu.VMEM((n_cp, tok // HALF, 2, HALF, HEAD_DIM), bf16),
                pltpu.VMEM((n_cp, tok // 128, 128), jnp.int32),
                pltpu.VMEM((128, 128), f32),
                pltpu.VMEM((n_cp * tok, 128), f32),
                pltpu.VMEM((max(CHUNKS), q_width), bf16),
                pltpu.VMEM((max(CHUNKS), q_width), bf16),
                *[pltpu.VMEM((o_tiles, r, TILE_N), bf16) for r in CHUNKS * 2],
                *[pltpu.VMEM((r, 128), bf16) for r in rows],
                *[pltpu.VMEM((r, 128), f32) for r in rows],
                dma((tok // LN_ROWS,)), dma((WKV_PARTS,)), dma((6,)), dma((SLOTS,)),
                dma((n_cp, tok // HALF)), dma((n_cp, tok // HALF)), dma((n_cp,)), dma((n_cp,)),
                dma((len(CHUNKS), o_tiles)), dma((len(CHUNKS), o_tiles)),
            ],
            compiler_params=pltpu.CompilerParams(collective_id=0, has_side_effects=True, vmem_limit_bytes=56 * 1024 * 1024),
            cost_estimate=pl.CostEstimate(flops=flops, bytes_accessed=2 * 4 * d_model * q_width, transcendentals=0),
        )(*args)
        return pl.pallas_call(
            close_kernel,
            out_shape=tuple(jax.ShapeDtypeStruct(a.shape, bf16) for a in (y, k, v)),
            in_specs=[vmem] * 3,
            out_specs=(hbm,) * 3,
            scratch_shapes=[dma((10,))],
            cost_estimate=pl.CostEstimate(flops=1, bytes_accessed=4 * tok * d_model, transcendentals=0),
        )(*(pltpu.with_memory_space_constraint(a, pltpu.VMEM) for a in (y, k, v)))

    row_spec = P(('dp', 'cp'), None)
    tok_spec = P(('dp', 'cp'))
    return jax.shard_map(local_block, mesh=mesh,
                         in_specs=(row_spec, tok_spec, P(None, 'tp'), P('tp'), P(None, None), P(None), P('tp', None), P(None), P(None), P(None)),
                         out_specs=(row_spec, row_spec, row_spec), check_vma=False)
```

```python
import functools

import jax
import jax.numpy as jnp
from jax import lax
from jax.experimental import pallas as pl
from jax.experimental.pallas import tpu as pltpu
from jax.sharding import PartitionSpec as P

HEAD_DIM = 128
LN_EPS = 1e-5
EXP2_SCALE = HEAD_DIM ** -0.5 * 1.4426950408889634
MESH = pl.DeviceIdType.MESH

CHUNKS = (128, 128)
HALF = 128
TILE_K = 3072
TILE_N = 512
SLOTS = 9
LN_ROWS = 32
WKV_PARTS = 6


def block_kernel(n_cp, hid_hbm, seg_hbm, wq_hbm, bq_hbm, wkv_hbm, bkv_hbm, wo_hbm, bo_hbm, gain_hbm, bias_hbm,
                 y_ref, k_ref, v_ref,
                 normed, wkv, wbuf, kv_all, seg_all, below, mask, qbuf, obuf, send0, send1, recv0, recv1,
                 bq_raw, bkv_raw, bo_raw, gain_raw, bias_raw, bq, bkv, bo, gain, bias,
                 hid_sem, wkv_sem, small_sem, w_sem, kv_send, kv_recv, seg_send, seg_recv, tp_send, tp_recv):
    my = lax.axis_index('cp')
    partner = 1 - lax.axis_index('tp')
    tok, d_model = y_ref.shape
    q_width = qbuf.shape[1]
    n_chunk = len(CHUNKS)
    n_half = tok // HALF
    send, recv = (send0, send1), (recv0, recv1)
    q_tiles = q_width // TILE_N
    k_halves = d_model // TILE_K
    o_tiles = d_model // TILE_N
    q_items = q_tiles * k_halves
    items = q_items + o_tiles
    total = n_chunk * items
    f32, bf16 = jnp.float32, jnp.bfloat16

    def hid_copy(i):
        rows = pl.ds(i * LN_ROWS, LN_ROWS)
        return pltpu.make_async_copy(hid_hbm.at[rows, :], y_ref.at[rows, :], hid_sem.at[i])

    def w_issue(g):
        slot = lax.rem(g, SLOTS)
        item = lax.rem(g, items)

        @pl.when(item < q_items)
        def _():
            col = pl.multiple_of(lax.div(item, k_halves) * TILE_N, TILE_N)
            row = pl.multiple_of(lax.rem(item, k_halves) * TILE_K, TILE_K)
            pltpu.make_async_copy(wq_hbm.at[pl.ds(row, TILE_K), pl.ds(col, TILE_N)], wbuf.at[slot], w_sem.at[slot]).start()

        @pl.when(item >= q_items)
        def _():
            col = pl.multiple_of((item - q_items) * TILE_N, TILE_N)
            pltpu.make_async_copy(wo_hbm.at[:, pl.ds(col, TILE_N)], wbuf.at[slot], w_sem.at[slot]).start()

    def w_wait(g):
        slot = lax.rem(g, SLOTS)
        pltpu.make_async_copy(wo_hbm.at[:, pl.ds(0, TILE_N)], wbuf.at[slot], w_sem.at[slot]).wait()
        return slot

    def w_next(g):
        @pl.when(g + SLOTS < total)
        def _():
            w_issue(g + SLOTS)

    n_ln = tok // LN_ROWS
    ln_half = n_ln // n_half
    small = [pltpu.make_async_copy(src, dst, small_sem.at[i]) for i, (src, dst) in enumerate((
        (gain_hbm, gain_raw), (bias_hbm, bias_raw), (bkv_hbm, bkv_raw), (bq_hbm, bq_raw), (bo_hbm, bo_raw), (seg_hbm, seg_all.at[my])))]
    wkv_rows = d_model // WKV_PARTS
    wkv_copies = [pltpu.make_async_copy(wkv_hbm.at[pl.ds(i * wkv_rows, wkv_rows), :], wkv.at[pl.ds(i * wkv_rows, wkv_rows), :], wkv_sem.at[i])
                  for i in range(WKV_PARTS)]
    hid_copy(0).start()
    for copy in small:
        copy.start()
    for i in range(1, ln_half):
        hid_copy(i).start()
    for copy in wkv_copies:
        copy.start()

    barrier = pltpu.get_barrier_semaphore()
    for step in range(1, n_cp):
        pl.semaphore_signal(barrier, inc=1, device_id={'cp': lax.rem(my + step, n_cp)}, device_id_type=MESH)
    pl.semaphore_signal(barrier, inc=1, device_id={'tp': partner}, device_id_type=MESH)

    with jax.named_scope("hid"):
        hid_copy(0).wait()
    for i in range(ln_half, n_ln):
        hid_copy(i).start()
    with jax.named_scope("small"):
        for copy in small:
            copy.wait()
    gain[...] = gain_raw[...].astype(f32)
    bias[...] = bias_raw[...].astype(f32)
    bkv[...] = bkv_raw[...].astype(f32)
    bq[...] = bq_raw[...].astype(f32)
    bo[...] = bo_raw[...].astype(f32)

    def ln_block(i, carry):
        @pl.when(i > 0)
        def _():
            hid_copy(i).wait()

        @pl.when((i > 0) & (i < ln_half))
        def _():
            w_issue(i - 1)

        @pl.when((i >= ln_half) & (i < SLOTS - 2))
        def _():
            for more in range(2):
                w_issue(i * 2 + more - ln_half - 1)

        rows = pl.ds(pl.multiple_of(i * LN_ROWS, LN_ROWS), LN_ROWS)
        n_col = d_model // 128

        def load(j):
            return y_ref[rows, j * 128:(j + 1) * 128].astype(f32)

        accs = [load(j) for j in range(4)]
        for j in range(4, n_col):
            accs[j % 4] = accs[j % 4] + load(j)
        mean = jnp.sum((accs[0] + accs[1]) + (accs[2] + accs[3]), axis=-1, keepdims=True) * (1.0 / d_model)
        mean = jnp.broadcast_to(mean, (LN_ROWS, 128))
        accs = [None] * 4
        for j in range(n_col):
            cen = load(j) - mean
            accs[j % 4] = cen * cen if accs[j % 4] is None else accs[j % 4] + cen * cen
        var = jnp.sum((accs[0] + accs[1]) + (accs[2] + accs[3]), axis=-1, keepdims=True) * (1.0 / d_model)
        rstd = jnp.broadcast_to(lax.rsqrt(var + LN_EPS), (LN_ROWS, 128))
        for j in range(n_col):
            out = (load(j) - mean) * rstd * gain[j:j + 1, :] + bias[j:j + 1, :]
            normed[rows, j * 128:(j + 1) * 128] = out.astype(bf16)
        return carry

    def kv_copy(src, h, dst):
        return pltpu.make_async_remote_copy(src_ref=kv_all.at[src, h], dst_ref=kv_all.at[src, h],
                                            send_sem=kv_send.at[dst, h], recv_sem=kv_recv.at[src, h],
                                            device_id={'cp': dst}, device_id_type=MESH)

    def seg_copy(src, dst):
        return pltpu.make_async_remote_copy(src_ref=seg_all.at[src], dst_ref=seg_all.at[src], send_sem=seg_send.at[dst],
                                            recv_sem=seg_recv.at[src], device_id={'cp': dst}, device_id_type=MESH)

    def late(dst):
        return (dst == n_cp - 1) & (my < n_cp // 2)

    def kv_half(h):
        with jax.named_scope("ln"):
            lax.fori_loop(h * ln_half, (h + 1) * ln_half, ln_block, 0)
        rows = pl.ds(h * HALF, HALF)
        if h == 0:
            for copy in wkv_copies:
                copy.wait()
        with jax.named_scope("kvdot"):
            mid = d_model // 2
            low = jnp.dot(normed[rows, :mid], wkv[:mid, :], preferred_element_type=f32)
            high = jnp.dot(normed[rows, mid:], wkv[mid:, :], preferred_element_type=f32)
            k_own = ((low[:, :HEAD_DIM] + bkv[0:1, :]) + high[:, :HEAD_DIM]).astype(bf16)
            v_own = ((low[:, HEAD_DIM:] + bkv[1:2, :]) + high[:, HEAD_DIM:]).astype(bf16)
            kv_all[my, h, 0] = k_own
            kv_all[my, h, 1] = v_own.astype(f32).T.astype(bf16)
            k_ref[rows, :] = k_own
            v_ref[rows, :] = v_own
        if h == 0:
            with jax.named_scope("barrier"):
                pl.semaphore_wait(barrier, n_cp)
            for dst in range(1, n_cp):
                @pl.when(my < dst)
                def _():
                    seg_copy(my, dst).start()

        for dst in range(1, n_cp):
            @pl.when((my < dst) & jnp.logical_not(late(dst)))
            def _():
                kv_copy(my, h, dst).start()

    kv_half(0)

    @pl.when(my < n_cp)
    def _():
        for h in range(1, n_half):
            kv_half(h)

    def tile_copy(c, n):
        return pltpu.make_async_remote_copy(src_ref=send[c].at[n], dst_ref=recv[c].at[n], send_sem=tp_send.at[c, n],
                                            recv_sem=tp_recv.at[c, n], device_id={'tp': partner}, device_id_type=MESH)

    def chunk(c):
        base = c * items
        n_row = CHUNKS[c]
        first = sum(CHUNKS[:c])
        rows = slice(first, first + n_row)

        def q_wait(j):
            return [w_wait(base + j * k_halves + half) for half in range(k_halves)]

        def q_next(j):
            for half in range(k_halves):
                w_next(base + j * k_halves + half)

        def q_dot(j, slots):
            acc = None
            step = TILE_K // 2
            for half in range(k_halves):
                for n in range(2):
                    k0 = half * TILE_K + n * step
                    part = jnp.dot(normed[rows, k0:k0 + step], wbuf[slots[half], n * step:(n + 1) * step, :], preferred_element_type=f32)
                    acc = part if acc is None else acc + part
            return acc

        def q_store(j, acc):
            for i in range(TILE_N // 128):
                cols = pl.ds(pl.multiple_of(j * TILE_N + i * 128, 128), 128)
                row = j * (TILE_N // 128) + i
                qbuf[:, cols] = (acc[:, i * 128:(i + 1) * 128] + bq[pl.ds(row, 1), :]).astype(bf16)

        def q_tile(j, carry):
            with jax.named_scope("qtile"):
                acc = None
                step = TILE_K // 2
                for half in range(k_halves):
                    slot = w_wait(base + j * k_halves + half)
                    for n in range(2):
                        k0 = half * TILE_K + n * step
                        part = jnp.dot(normed[rows, k0:k0 + step], wbuf[slot, n * step:(n + 1) * step, :], preferred_element_type=f32)
                        acc = part if acc is None else acc + part
                    w_next(base + j * k_halves + half)
                q_store(j, acc)
            return carry

        own_keys = first + n_row

        def make_mask():
            if c == 0:
                for src in range(n_cp - 1):
                    @pl.when(src < my)
                    def _():
                        seg_copy(src, src).wait_recv()

            seg_q = jnp.broadcast_to(seg_all[my, c:c + 1, :].astype(f32), (128, 128)).T
            below[...] = jnp.zeros((128, 128), f32)
            for b in range(n_cp * tok // 128):
                src, part = b * 128 // tok, b % (tok // 128)

                @pl.when(b * 128 < my * tok + own_keys)
                def _():
                    below[...] += jnp.where(seg_all[src, part:part + 1, :].astype(f32) < seg_q, 1.0, 0.0)

            prompt = jnp.broadcast_to(jnp.sum(below[...], axis=1, keepdims=True), (128, 128)).T
            key = lax.broadcasted_iota(jnp.int32, (128, 128), 0)
            q_pos = my * tok + first + lax.broadcasted_iota(jnp.int32, (128, 128), 1)
            for b in range(n_cp * tok // 128):
                src, part = b * 128 // tok, b % (tok // 128)

                @pl.when(b * 128 < my * tok + own_keys)
                def _():
                    k_pos = key + b * 128
                    seen = (k_pos.astype(f32) >= prompt) & (k_pos <= q_pos)
                    mask[b * 128:(b + 1) * 128, :] = jnp.where(seen, 0.0, -jnp.inf)

        def heads(j, nb, beside=None):
            cols = pl.ds(pl.multiple_of(j * TILE_N, TILE_N), TILE_N)
            n_head = TILE_N // HEAD_DIM
            keys = nb * tok + own_keys
            parts = [kv_all.at[b * 128 // tok, b % (tok // 128)] for b in range(keys // 128)]
            k_blk = jnp.concatenate([part[0] for part in parts], axis=0)
            v_t = jnp.concatenate([part[1] for part in parts], axis=1)
            q_cols = qbuf[:, cols]
            q_rows = jnp.concatenate([q_cols[:, i * HEAD_DIM:(i + 1) * HEAD_DIM] for i in range(n_head)], axis=0)
            s = lax.dot_general(k_blk, q_rows, (((1,), (1,)), ((), ())), preferred_element_type=f32)
            other = beside() if beside else None
            s = s + jnp.concatenate([mask[:keys, :]] * n_head, axis=1)
            p_wts = jnp.exp2((s - jnp.max(s, axis=0, keepdims=True)) * EXP2_SCALE)
            l_sum = jnp.sum(p_wts, axis=0, keepdims=True)
            o = jnp.dot(v_t, p_wts.astype(bf16), preferred_element_type=f32) / l_sum
            obuf[:, cols] = jnp.concatenate([o[:, i * HEAD_DIM:(i + 1) * HEAD_DIM].T for i in range(n_head)], axis=1).astype(bf16)
            return other

        def attend(j, carry):
            for nb in range(n_cp):
                @pl.when(my == nb)
                def _():
                    with jax.named_scope("attn"):
                        heads(j, nb)
            return carry

        def both(j, carry):
            slots = q_wait(j)
            for nb in range(n_cp // 2, n_cp):
                @pl.when(my == nb)
                def _():
                    with jax.named_scope("both"):
                        q_store(j, heads(j - lag, nb, lambda: q_dot(j, slots)))
            q_next(j)
            return carry

        lag = jnp.where(my < n_cp // 2, 1, my)
        q_tile(0, 0)
        if c == 0:
            @pl.when(late(n_cp - 1))
            def _():
                for h in range(n_half):
                    kv_copy(my, h, n_cp - 1).start()

        lax.fori_loop(1, lag, q_tile, 0)
        with jax.named_scope("mask"):
            make_mask()
        if c == 0:
            with jax.named_scope("kvwait"):
                for src in range(n_cp - 1):
                    @pl.when(src < my)
                    def _():
                        for h in range(n_half):
                            kv_copy(src, h, src).wait_recv()
        def turn(j, carry):
            return q_tile(j, attend(j - lag, carry))

        split = jnp.where(my < n_cp // 2, q_tiles, lag) if c == 0 else q_tiles
        lax.fori_loop(lag, split, turn, 0)
        if c == 0:
            lax.fori_loop(split, q_tiles, both, 0)
        lax.fori_loop(q_tiles - lag, q_tiles, attend, 0)

        def o_tile(n, carry):
            with jax.named_scope("otile"):
                g = base + q_items + n
                slot = w_wait(g)
                send[c][n] = jnp.dot(obuf[:n_row, :], wbuf[slot], preferred_element_type=f32).astype(bf16)
                tile_copy(c, n).start()
                w_next(g)
            return carry

        lax.fori_loop(0, o_tiles, o_tile, 0)

    for c in range(n_chunk):
        chunk(c)

    for dst in range(1, n_cp):
        @pl.when(my < dst)
        def _():
            seg_copy(my, dst).wait_send()
            for h in range(n_half):
                kv_copy(my, h, dst).wait_send()

    for c in range(n_chunk):
        first = sum(CHUNKS[:c])
        rows = slice(first, first + CHUNKS[c])

        def finish(n, carry):
            copy = tile_copy(c, n)
            copy.wait_recv()
            copy.wait_send()
            for i in range(TILE_N // 128):
                cols = pl.ds(pl.multiple_of(n * TILE_N + i * 128, 128), 128)
                part = slice(i * 128, (i + 1) * 128)
                both = send[c][n, :, part].astype(f32) + recv[c][n, :, part].astype(f32)
                y_ref[rows, cols] = (y_ref[rows, cols].astype(f32) + both + bo[pl.ds(n * (TILE_N // 128) + i, 1), :]).astype(bf16)
            return carry

        with jax.named_scope("finish"):
            lax.fori_loop(0, o_tiles, finish, 0)


def close_kernel(y_ref, k_ref, v_ref, y_hbm, k_hbm, v_hbm, sem):
    rows = y_ref.shape[0] // 8
    copies = [pltpu.make_async_copy(k_ref, k_hbm, sem.at[8]), pltpu.make_async_copy(v_ref, v_hbm, sem.at[9])]
    copies += [pltpu.make_async_copy(y_ref.at[pl.ds(i * rows, rows), :], y_hbm.at[pl.ds(i * rows, rows), :], sem.at[i]) for i in range(8)]
    for copy in copies:
        copy.start()
    for copy in copies:
        copy.wait()


def solution(mesh):
    n_cp = mesh.shape['cp']

    def local_block(hidden, seg_ids, w_q, b_q, w_kv, b_kv, w_o, b_o, ln_gain, ln_bias):
        tok, d_model = hidden.shape
        q_width = w_q.shape[1]
        o_tiles = d_model // TILE_N
        vmem = pl.BlockSpec(memory_space=pltpu.VMEM)
        hbm = pl.BlockSpec(memory_space=pltpu.HBM)
        bf16, f32 = jnp.bfloat16, jnp.float32
        dma = pltpu.SemaphoreType.DMA
        flops = 2 * tok * d_model * (2 * q_width + 256)
        args = (hidden, seg_ids.reshape(-1, 128), w_q, b_q.reshape(-1, 128), w_kv, b_kv.reshape(-1, 128), w_o,
                b_o.reshape(-1, 128), ln_gain.reshape(-1, 128), ln_bias.reshape(-1, 128))
        args = tuple(pltpu.with_memory_space_constraint(a, pltpu.HBM) for a in args)
        rows = [q_width // 128, 2, d_model // 128, d_model // 128, d_model // 128]
        y, k, v = pl.pallas_call(
            functools.partial(block_kernel, n_cp),
            out_shape=(pltpu.VMEM((tok, d_model), bf16), pltpu.VMEM((tok, HEAD_DIM), bf16), pltpu.VMEM((tok, HEAD_DIM), bf16)),
            in_specs=[hbm] * len(args),
            out_specs=(vmem, vmem, vmem),
            scratch_shapes=[
                pltpu.VMEM((tok, d_model), bf16),
                pltpu.VMEM((d_model, 2 * HEAD_DIM), bf16),
                pltpu.VMEM((SLOTS, TILE_K, TILE_N), bf16),
                pltpu.VMEM((n_cp, tok // HALF, 2, HALF, HEAD_DIM), bf16),
                pltpu.VMEM((n_cp, tok // 128, 128), jnp.int32),
                pltpu.VMEM((128, 128), f32),
                pltpu.VMEM((n_cp * tok, 128), f32),
                pltpu.VMEM((max(CHUNKS), q_width), bf16),
                pltpu.VMEM((max(CHUNKS), q_width), bf16),
                *[pltpu.VMEM((o_tiles, r, TILE_N), bf16) for r in CHUNKS * 2],
                *[pltpu.VMEM((r, 128), bf16) for r in rows],
                *[pltpu.VMEM((r, 128), f32) for r in rows],
                dma((tok // LN_ROWS,)), dma((WKV_PARTS,)), dma((6,)), dma((SLOTS,)),
                dma((n_cp, tok // HALF)), dma((n_cp, tok // HALF)), dma((n_cp,)), dma((n_cp,)),
                dma((len(CHUNKS), o_tiles)), dma((len(CHUNKS), o_tiles)),
            ],
            compiler_params=pltpu.CompilerParams(collective_id=0, has_side_effects=True, vmem_limit_bytes=56 * 1024 * 1024),
            cost_estimate=pl.CostEstimate(flops=flops, bytes_accessed=2 * 4 * d_model * q_width, transcendentals=0),
        )(*args)
        return pl.pallas_call(
            close_kernel,
            out_shape=tuple(jax.ShapeDtypeStruct(a.shape, bf16) for a in (y, k, v)),
            in_specs=[vmem] * 3,
            out_specs=(hbm,) * 3,
            scratch_shapes=[dma((10,))],
            cost_estimate=pl.CostEstimate(flops=1, bytes_accessed=4 * tok * d_model, transcendentals=0),
        )(*(pltpu.with_memory_space_constraint(a, pltpu.VMEM) for a in (y, k, v)))

    row_spec = P(('dp', 'cp'), None)
    tok_spec = P(('dp', 'cp'))
    return jax.shard_map(local_block, mesh=mesh,
                         in_specs=(row_spec, tok_spec, P(None, 'tp'), P('tp'), P(None, None), P(None), P('tp', None), P(None), P(None), P(None)),
                         out_specs=(row_spec, row_spec, row_spec), check_vma=False)
```

```python
import functools

import jax
import jax.numpy as jnp
from jax import lax
from jax.experimental import pallas as pl
from jax.experimental.pallas import tpu as pltpu
from jax.sharding import PartitionSpec as P

HEAD_DIM = 128
LN_EPS = 1e-5
EXP2_SCALE = HEAD_DIM ** -0.5 * 1.4426950408889634
MESH = pl.DeviceIdType.MESH

CHUNKS = (128, 128)
HALF = 128
TILE_K = 3072
TILE_N = 512
SLOTS = 9
LN_ROWS = 32
WKV_PARTS = 6


def block_kernel(n_cp, hid_hbm, seg_hbm, wq_hbm, bq_hbm, wkv_hbm, bkv_hbm, wo_hbm, bo_hbm, gain_hbm, bias_hbm,
                 y_ref, k_ref, v_ref,
                 normed, wkv, wbuf, kv_all, seg_all, below, mask, qbuf, obuf, send0, send1, recv0, recv1,
                 bq_raw, bkv_raw, bo_raw, gain_raw, bias_raw, bq, bkv, bo, gain, bias,
                 hid_sem, wkv_sem, small_sem, w_sem, kv_send, kv_recv, seg_send, seg_recv, tp_send, tp_recv):
    my = lax.axis_index('cp')
    partner = 1 - lax.axis_index('tp')
    tok, d_model = y_ref.shape
    q_width = qbuf.shape[1]
    n_chunk = len(CHUNKS)
    n_half = tok // HALF
    send, recv = (send0, send1), (recv0, recv1)
    q_tiles = q_width // TILE_N
    k_halves = d_model // TILE_K
    o_tiles = d_model // TILE_N
    q_items = q_tiles * k_halves
    items = q_items + o_tiles
    total = n_chunk * items
    f32, bf16 = jnp.float32, jnp.bfloat16

    def hid_copy(i):
        rows = pl.ds(i * LN_ROWS, LN_ROWS)
        return pltpu.make_async_copy(hid_hbm.at[rows, :], y_ref.at[rows, :], hid_sem.at[i])

    def w_issue(g):
        slot = lax.rem(g, SLOTS)
        item = lax.rem(g, items)

        @pl.when(item < q_items)
        def _():
            col = pl.multiple_of(lax.div(item, k_halves) * TILE_N, TILE_N)
            row = pl.multiple_of(lax.rem(item, k_halves) * TILE_K, TILE_K)
            pltpu.make_async_copy(wq_hbm.at[pl.ds(row, TILE_K), pl.ds(col, TILE_N)], wbuf.at[slot], w_sem.at[slot]).start()

        @pl.when(item >= q_items)
        def _():
            col = pl.multiple_of((item - q_items) * TILE_N, TILE_N)
            pltpu.make_async_copy(wo_hbm.at[:, pl.ds(col, TILE_N)], wbuf.at[slot], w_sem.at[slot]).start()

    def w_wait(g):
        slot = lax.rem(g, SLOTS)
        pltpu.make_async_copy(wo_hbm.at[:, pl.ds(0, TILE_N)], wbuf.at[slot], w_sem.at[slot]).wait()
        return slot

    def w_next(g):
        @pl.when(g + SLOTS < total)
        def _():
            w_issue(g + SLOTS)

    n_ln = tok // LN_ROWS
    ln_half = n_ln // n_half
    small = [pltpu.make_async_copy(src, dst, small_sem.at[i]) for i, (src, dst) in enumerate((
        (gain_hbm, gain_raw), (bias_hbm, bias_raw), (bkv_hbm, bkv_raw), (bq_hbm, bq_raw), (bo_hbm, bo_raw), (seg_hbm, seg_all.at[my])))]
    wkv_rows = d_model // WKV_PARTS
    wkv_copies = [pltpu.make_async_copy(wkv_hbm.at[pl.ds(i * wkv_rows, wkv_rows), :], wkv.at[pl.ds(i * wkv_rows, wkv_rows), :], wkv_sem.at[i])
                  for i in range(WKV_PARTS)]
    for copy in small:
        copy.start()
    hid_copy(0).start()
    for i in range(1, ln_half):
        hid_copy(i).start()
    for copy in wkv_copies:
        copy.start()

    barrier = pltpu.get_barrier_semaphore()
    for step in range(1, n_cp):
        pl.semaphore_signal(barrier, inc=1, device_id={'cp': lax.rem(my + step, n_cp)}, device_id_type=MESH)
    pl.semaphore_signal(barrier, inc=1, device_id={'tp': partner}, device_id_type=MESH)

    with jax.named_scope("hid"):
        hid_copy(0).wait()
    for i in range(ln_half, n_ln):
        hid_copy(i).start()
    with jax.named_scope("small"):
        for copy in small:
            copy.wait()
    gain[...] = gain_raw[...].astype(f32)
    bias[...] = bias_raw[...].astype(f32)
    bkv[...] = bkv_raw[...].astype(f32)
    bq[...] = bq_raw[...].astype(f32)
    bo[...] = bo_raw[...].astype(f32)

    def ln_block(i, carry):
        @pl.when(i > 0)
        def _():
            hid_copy(i).wait()

        @pl.when((i > 0) & (i < ln_half))
        def _():
            w_issue(i - 1)

        @pl.when((i >= ln_half) & (i < SLOTS - 2))
        def _():
            for more in range(2):
                w_issue(i * 2 + more - ln_half - 1)

        rows = pl.ds(pl.multiple_of(i * LN_ROWS, LN_ROWS), LN_ROWS)
        n_col = d_model // 128

        def load(j):
            return y_ref[rows, j * 128:(j + 1) * 128].astype(f32)

        accs = [load(j) for j in range(4)]
        for j in range(4, n_col):
            accs[j % 4] = accs[j % 4] + load(j)
        mean = jnp.sum((accs[0] + accs[1]) + (accs[2] + accs[3]), axis=-1, keepdims=True) * (1.0 / d_model)
        mean = jnp.broadcast_to(mean, (LN_ROWS, 128))
        accs = [None] * 4
        for j in range(n_col):
            cen = load(j) - mean
            accs[j % 4] = cen * cen if accs[j % 4] is None else accs[j % 4] + cen * cen
        var = jnp.sum((accs[0] + accs[1]) + (accs[2] + accs[3]), axis=-1, keepdims=True) * (1.0 / d_model)
        rstd = jnp.broadcast_to(lax.rsqrt(var + LN_EPS), (LN_ROWS, 128))
        for j in range(n_col):
            out = (load(j) - mean) * rstd * gain[j:j + 1, :] + bias[j:j + 1, :]
            normed[rows, j * 128:(j + 1) * 128] = out.astype(bf16)
        return carry

    def kv_copy(src, h, dst):
        return pltpu.make_async_remote_copy(src_ref=kv_all.at[src, h], dst_ref=kv_all.at[src, h],
                                            send_sem=kv_send.at[dst, h], recv_sem=kv_recv.at[src, h],
                                            device_id={'cp': dst}, device_id_type=MESH)

    def seg_copy(src, dst):
        return pltpu.make_async_remote_copy(src_ref=seg_all.at[src], dst_ref=seg_all.at[src], send_sem=seg_send.at[dst],
                                            recv_sem=seg_recv.at[src], device_id={'cp': dst}, device_id_type=MESH)

    def late(dst):
        return (dst == n_cp - 1) & (my < n_cp // 2)

    def kv_half(h):
        with jax.named_scope("ln"):
            lax.fori_loop(h * ln_half, (h + 1) * ln_half, ln_block, 0)
        rows = pl.ds(h * HALF, HALF)
        if h == 0:
            for copy in wkv_copies:
                copy.wait()
        with jax.named_scope("kvdot"):
            mid = d_model // 2
            low = jnp.dot(normed[rows, :mid], wkv[:mid, :], preferred_element_type=f32)
            high = jnp.dot(normed[rows, mid:], wkv[mid:, :], preferred_element_type=f32)
            k_own = ((low[:, :HEAD_DIM] + bkv[0:1, :]) + high[:, :HEAD_DIM]).astype(bf16)
            v_own = ((low[:, HEAD_DIM:] + bkv[1:2, :]) + high[:, HEAD_DIM:]).astype(bf16)
            kv_all[my, h, 0] = k_own
            kv_all[my, h, 1] = v_own.astype(f32).T.astype(bf16)
            k_ref[rows, :] = k_own
            v_ref[rows, :] = v_own
        if h == 0:
            with jax.named_scope("barrier"):
                pl.semaphore_wait(barrier, n_cp)
            for dst in range(1, n_cp):
                @pl.when(my < dst)
                def _():
                    seg_copy(my, dst).start()

        for dst in range(1, n_cp):
            @pl.when((my < dst) & jnp.logical_not(late(dst)))
            def _():
                kv_copy(my, h, dst).start()

    kv_half(0)

    @pl.when(my < n_cp)
    def _():
        for h in range(1, n_half):
            kv_half(h)

    def tile_copy(c, n):
        return pltpu.make_async_remote_copy(src_ref=send[c].at[n], dst_ref=recv[c].at[n], send_sem=tp_send.at[c, n],
                                            recv_sem=tp_recv.at[c, n], device_id={'tp': partner}, device_id_type=MESH)

    def chunk(c):
        base = c * items
        n_row = CHUNKS[c]
        first = sum(CHUNKS[:c])
        rows = slice(first, first + n_row)

        def q_wait(j):
            return [w_wait(base + j * k_halves + half) for half in range(k_halves)]

        def q_next(j):
            for half in range(k_halves):
                w_next(base + j * k_halves + half)

        def q_dot(j, slots):
            acc = None
            step = TILE_K // 2
            for half in range(k_halves):
                for n in range(2):
                    k0 = half * TILE_K + n * step
                    part = jnp.dot(normed[rows, k0:k0 + step], wbuf[slots[half], n * step:(n + 1) * step, :], preferred_element_type=f32)
                    acc = part if acc is None else acc + part
            return acc

        def q_store(j, acc):
            for i in range(TILE_N // 128):
                cols = pl.ds(pl.multiple_of(j * TILE_N + i * 128, 128), 128)
                row = j * (TILE_N // 128) + i
                qbuf[:, cols] = (acc[:, i * 128:(i + 1) * 128] + bq[pl.ds(row, 1), :]).astype(bf16)

        def q_tile(j, carry):
            with jax.named_scope("qtile"):
                acc = None
                step = TILE_K // 2
                for half in range(k_halves):
                    slot = w_wait(base + j * k_halves + half)
                    for n in range(2):
                        k0 = half * TILE_K + n * step
                        part = jnp.dot(normed[rows, k0:k0 + step], wbuf[slot, n * step:(n + 1) * step, :], preferred_element_type=f32)
                        acc = part if acc is None else acc + part
                    w_next(base + j * k_halves + half)
                q_store(j, acc)
            return carry

        own_keys = first + n_row

        def make_mask():
            if c == 0:
                for src in range(n_cp - 1):
                    @pl.when(src < my)
                    def _():
                        seg_copy(src, src).wait_recv()

            seg_q = jnp.broadcast_to(seg_all[my, c:c + 1, :].astype(f32), (128, 128)).T
            below[...] = jnp.zeros((128, 128), f32)
            for b in range(n_cp * tok // 128):
                src, part = b * 128 // tok, b % (tok // 128)

                @pl.when(b * 128 < my * tok + own_keys)
                def _():
                    below[...] += jnp.where(seg_all[src, part:part + 1, :].astype(f32) < seg_q, 1.0, 0.0)

            prompt = jnp.broadcast_to(jnp.sum(below[...], axis=1, keepdims=True), (128, 128)).T
            key = lax.broadcasted_iota(jnp.int32, (128, 128), 0)
            q_pos = my * tok + first + lax.broadcasted_iota(jnp.int32, (128, 128), 1)
            for b in range(n_cp * tok // 128):
                src, part = b * 128 // tok, b % (tok // 128)

                @pl.when(b * 128 < my * tok + own_keys)
                def _():
                    k_pos = key + b * 128
                    seen = (k_pos.astype(f32) >= prompt) & (k_pos <= q_pos)
                    mask[b * 128:(b + 1) * 128, :] = jnp.where(seen, 0.0, -jnp.inf)

        def heads(j, nb, beside=None):
            cols = pl.ds(pl.multiple_of(j * TILE_N, TILE_N), TILE_N)
            n_head = TILE_N // HEAD_DIM
            keys = nb * tok + own_keys
            parts = [kv_all.at[b * 128 // tok, b % (tok // 128)] for b in range(keys // 128)]
            k_blk = jnp.concatenate([part[0] for part in parts], axis=0)
            v_t = jnp.concatenate([part[1] for part in parts], axis=1)
            q_cols = qbuf[:, cols]
            q_rows = jnp.concatenate([q_cols[:, i * HEAD_DIM:(i + 1) * HEAD_DIM] for i in range(n_head)], axis=0)
            s = lax.dot_general(k_blk, q_rows, (((1,), (1,)), ((), ())), preferred_element_type=f32)
            other = beside() if beside else None
            s = s + jnp.concatenate([mask[:keys, :]] * n_head, axis=1)
            p_wts = jnp.exp2((s - jnp.max(s, axis=0, keepdims=True)) * EXP2_SCALE)
            l_sum = jnp.sum(p_wts, axis=0, keepdims=True)
            o = jnp.dot(v_t, p_wts.astype(bf16), preferred_element_type=f32) / l_sum
            obuf[:, cols] = jnp.concatenate([o[:, i * HEAD_DIM:(i + 1) * HEAD_DIM].T for i in range(n_head)], axis=1).astype(bf16)
            return other

        def attend(j, carry):
            for nb in range(n_cp):
                @pl.when(my == nb)
                def _():
                    with jax.named_scope("attn"):
                        heads(j, nb)
            return carry

        def both(j, carry):
            slots = q_wait(j)
            for nb in range(n_cp // 2, n_cp):
                @pl.when(my == nb)
                def _():
                    with jax.named_scope("both"):
                        q_store(j, heads(j - lag, nb, lambda: q_dot(j, slots)))
            q_next(j)
            return carry

        lag = jnp.where(my < n_cp // 2, 1, my)
        q_tile(0, 0)
        if c == 0:
            @pl.when(late(n_cp - 1))
            def _():
                for h in range(n_half):
                    kv_copy(my, h, n_cp - 1).start()

        lax.fori_loop(1, lag, q_tile, 0)
        with jax.named_scope("mask"):
            make_mask()
        if c == 0:
            with jax.named_scope("kvwait"):
                for src in range(n_cp - 1):
                    @pl.when(src < my)
                    def _():
                        for h in range(n_half):
                            kv_copy(src, h, src).wait_recv()
        def turn(j, carry):
            return q_tile(j, attend(j - lag, carry))

        split = jnp.where(my < n_cp // 2, q_tiles, lag) if c == 0 else q_tiles
        lax.fori_loop(lag, split, turn, 0)
        if c == 0:
            lax.fori_loop(split, q_tiles, both, 0)
        lax.fori_loop(q_tiles - lag, q_tiles, attend, 0)

        def o_tile(n, carry):
            with jax.named_scope("otile"):
                g = base + q_items + n
                slot = w_wait(g)
                send[c][n] = jnp.dot(obuf[:n_row, :], wbuf[slot], preferred_element_type=f32).astype(bf16)
                tile_copy(c, n).start()
                w_next(g)
            return carry

        lax.fori_loop(0, o_tiles, o_tile, 0)

    for c in range(n_chunk):
        chunk(c)

    for dst in range(1, n_cp):
        @pl.when(my < dst)
        def _():
            seg_copy(my, dst).wait_send()
            for h in range(n_half):
                kv_copy(my, h, dst).wait_send()

    for c in range(n_chunk):
        first = sum(CHUNKS[:c])
        rows = slice(first, first + CHUNKS[c])

        def finish(n, carry):
            copy = tile_copy(c, n)
            copy.wait_recv()
            copy.wait_send()
            for i in range(TILE_N // 128):
                cols = pl.ds(pl.multiple_of(n * TILE_N + i * 128, 128), 128)
                part = slice(i * 128, (i + 1) * 128)
                both = send[c][n, :, part].astype(f32) + recv[c][n, :, part].astype(f32)
                y_ref[rows, cols] = (y_ref[rows, cols].astype(f32) + both + bo[pl.ds(n * (TILE_N // 128) + i, 1), :]).astype(bf16)
            return carry

        with jax.named_scope("finish"):
            lax.fori_loop(0, o_tiles, finish, 0)


def close_kernel(y_ref, k_ref, v_ref, y_hbm, k_hbm, v_hbm, sem):
    rows = y_ref.shape[0] // 8
    copies = [pltpu.make_async_copy(k_ref, k_hbm, sem.at[8]), pltpu.make_async_copy(v_ref, v_hbm, sem.at[9])]
    copies += [pltpu.make_async_copy(y_ref.at[pl.ds(i * rows, rows), :], y_hbm.at[pl.ds(i * rows, rows), :], sem.at[i]) for i in range(8)]
    for copy in copies:
        copy.start()
    for copy in copies:
        copy.wait()


def solution(mesh):
    n_cp = mesh.shape['cp']

    def local_block(hidden, seg_ids, w_q, b_q, w_kv, b_kv, w_o, b_o, ln_gain, ln_bias):
        tok, d_model = hidden.shape
        q_width = w_q.shape[1]
        o_tiles = d_model // TILE_N
        vmem = pl.BlockSpec(memory_space=pltpu.VMEM)
        hbm = pl.BlockSpec(memory_space=pltpu.HBM)
        bf16, f32 = jnp.bfloat16, jnp.float32
        dma = pltpu.SemaphoreType.DMA
        flops = 2 * tok * d_model * (2 * q_width + 256)
        args = (hidden, seg_ids.reshape(-1, 128), w_q, b_q.reshape(-1, 128), w_kv, b_kv.reshape(-1, 128), w_o,
                b_o.reshape(-1, 128), ln_gain.reshape(-1, 128), ln_bias.reshape(-1, 128))
        args = tuple(pltpu.with_memory_space_constraint(a, pltpu.HBM) for a in args)
        rows = [q_width // 128, 2, d_model // 128, d_model // 128, d_model // 128]
        y, k, v = pl.pallas_call(
            functools.partial(block_kernel, n_cp),
            out_shape=(pltpu.VMEM((tok, d_model), bf16), pltpu.VMEM((tok, HEAD_DIM), bf16), pltpu.VMEM((tok, HEAD_DIM), bf16)),
            in_specs=[hbm] * len(args),
            out_specs=(vmem, vmem, vmem),
            scratch_shapes=[
                pltpu.VMEM((tok, d_model), bf16),
                pltpu.VMEM((d_model, 2 * HEAD_DIM), bf16),
                pltpu.VMEM((SLOTS, TILE_K, TILE_N), bf16),
                pltpu.VMEM((n_cp, tok // HALF, 2, HALF, HEAD_DIM), bf16),
                pltpu.VMEM((n_cp, tok // 128, 128), jnp.int32),
                pltpu.VMEM((128, 128), f32),
                pltpu.VMEM((n_cp * tok, 128), f32),
                pltpu.VMEM((max(CHUNKS), q_width), bf16),
                pltpu.VMEM((max(CHUNKS), q_width), bf16),
                *[pltpu.VMEM((o_tiles, r, TILE_N), bf16) for r in CHUNKS * 2],
                *[pltpu.VMEM((r, 128), bf16) for r in rows],
                *[pltpu.VMEM((r, 128), f32) for r in rows],
                dma((tok // LN_ROWS,)), dma((WKV_PARTS,)), dma((6,)), dma((SLOTS,)),
                dma((n_cp, tok // HALF)), dma((n_cp, tok // HALF)), dma((n_cp,)), dma((n_cp,)),
                dma((len(CHUNKS), o_tiles)), dma((len(CHUNKS), o_tiles)),
            ],
            compiler_params=pltpu.CompilerParams(collective_id=0, has_side_effects=True, vmem_limit_bytes=56 * 1024 * 1024),
            cost_estimate=pl.CostEstimate(flops=flops, bytes_accessed=2 * 4 * d_model * q_width, transcendentals=0),
        )(*args)
        return pl.pallas_call(
            close_kernel,
            out_shape=tuple(jax.ShapeDtypeStruct(a.shape, bf16) for a in (y, k, v)),
            in_specs=[vmem] * 3,
            out_specs=(hbm,) * 3,
            scratch_shapes=[dma((10,))],
            cost_estimate=pl.CostEstimate(flops=1, bytes_accessed=4 * tok * d_model, transcendentals=0),
        )(*(pltpu.with_memory_space_constraint(a, pltpu.VMEM) for a in (y, k, v)))

    row_spec = P(('dp', 'cp'), None)
    tok_spec = P(('dp', 'cp'))
    return jax.shard_map(local_block, mesh=mesh,
                         in_specs=(row_spec, tok_spec, P(None, 'tp'), P('tp'), P(None, None), P(None), P('tp', None), P(None), P(None), P(None)),
                         out_specs=(row_spec, row_spec, row_spec), check_vma=False)
```

```python
import functools

import jax
import jax.numpy as jnp
from jax import lax
from jax.experimental import pallas as pl
from jax.experimental.pallas import tpu as pltpu
from jax.sharding import PartitionSpec as P

HEAD_DIM = 128
LN_EPS = 1e-5
EXP2_SCALE = HEAD_DIM ** -0.5 * 1.4426950408889634
MESH = pl.DeviceIdType.MESH

CHUNKS = (128, 128)
HALF = 128
TILE_K = 3072
TILE_N = 512
SLOTS = 9
LN_ROWS = 32
WKV_PARTS = 6


def block_kernel(n_cp, hid_hbm, seg_hbm, wq_hbm, bq_hbm, wkv_hbm, bkv_hbm, wo_hbm, bo_hbm, gain_hbm, bias_hbm,
                 y_ref, k_ref, v_ref,
                 normed, wkv, wbuf, kv_all, seg_all, below, ln_mean, ln_rstd, mask, qbuf, obuf, send0, send1, recv0, recv1,
                 bq_raw, bkv_raw, bo_raw, gain_raw, bias_raw, bq, bkv, bo, gain, bias,
                 hid_sem, wkv_sem, small_sem, w_sem, kv_send, kv_recv, seg_send, seg_recv, tp_send, tp_recv):
    my = lax.axis_index('cp')
    partner = 1 - lax.axis_index('tp')
    tok, d_model = y_ref.shape
    q_width = qbuf.shape[1]
    n_chunk = len(CHUNKS)
    n_half = tok // HALF
    send, recv = (send0, send1), (recv0, recv1)
    q_tiles = q_width // TILE_N
    k_halves = d_model // TILE_K
    o_tiles = d_model // TILE_N
    q_items = q_tiles * k_halves
    items = q_items + o_tiles
    total = n_chunk * items
    f32, bf16 = jnp.float32, jnp.bfloat16

    def hid_copy(i):
        rows = pl.ds(i * LN_ROWS, LN_ROWS)
        return pltpu.make_async_copy(hid_hbm.at[rows, :], y_ref.at[rows, :], hid_sem.at[i])

    def w_issue(g):
        slot = lax.rem(g, SLOTS)
        item = lax.rem(g, items)

        @pl.when(item < q_items)
        def _():
            col = pl.multiple_of(lax.div(item, k_halves) * TILE_N, TILE_N)
            row = pl.multiple_of(lax.rem(item, k_halves) * TILE_K, TILE_K)
            pltpu.make_async_copy(wq_hbm.at[pl.ds(row, TILE_K), pl.ds(col, TILE_N)], wbuf.at[slot], w_sem.at[slot]).start()

        @pl.when(item >= q_items)
        def _():
            col = pl.multiple_of((item - q_items) * TILE_N, TILE_N)
            pltpu.make_async_copy(wo_hbm.at[:, pl.ds(col, TILE_N)], wbuf.at[slot], w_sem.at[slot]).start()

    def w_wait(g):
        slot = lax.rem(g, SLOTS)
        pltpu.make_async_copy(wo_hbm.at[:, pl.ds(0, TILE_N)], wbuf.at[slot], w_sem.at[slot]).wait()
        return slot

    def w_next(g):
        @pl.when(g + SLOTS < total)
        def _():
            w_issue(g + SLOTS)

    n_ln = tok // LN_ROWS
    ln_half = n_ln // n_half
    small = [pltpu.make_async_copy(src, dst, small_sem.at[i]) for i, (src, dst) in enumerate((
        (gain_hbm, gain_raw), (bias_hbm, bias_raw), (bkv_hbm, bkv_raw), (bq_hbm, bq_raw), (bo_hbm, bo_raw), (seg_hbm, seg_all.at[my])))]
    wkv_rows = d_model // WKV_PARTS
    wkv_copies = [pltpu.make_async_copy(wkv_hbm.at[pl.ds(i * wkv_rows, wkv_rows), :], wkv.at[pl.ds(i * wkv_rows, wkv_rows), :], wkv_sem.at[i])
                  for i in range(WKV_PARTS)]
    for copy in small:
        copy.start()
    hid_copy(0).start()
    for i in range(1, ln_half):
        hid_copy(i).start()
    for copy in wkv_copies:
        copy.start()

    barrier = pltpu.get_barrier_semaphore()
    for step in range(1, n_cp):
        pl.semaphore_signal(barrier, inc=1, device_id={'cp': lax.rem(my + step, n_cp)}, device_id_type=MESH)
    pl.semaphore_signal(barrier, inc=1, device_id={'tp': partner}, device_id_type=MESH)

    with jax.named_scope("hid"):
        hid_copy(0).wait()
    for i in range(ln_half, n_ln):
        hid_copy(i).start()
    def small_arrays():
        with jax.named_scope("small"):
            for copy in small:
                copy.wait()
        gain[...] = gain_raw[...].astype(f32)
        bias[...] = bias_raw[...].astype(f32)
        bkv[...] = bkv_raw[...].astype(f32)
        bq[...] = bq_raw[...].astype(f32)
        bo[...] = bo_raw[...].astype(f32)

    def ln_block(i, carry):
        @pl.when(i > 0)
        def _():
            hid_copy(i).wait()

        @pl.when((i > 0) & (i < ln_half))
        def _():
            w_issue(i - 1)

        @pl.when((i >= ln_half) & (i < SLOTS - 2))
        def _():
            for more in range(2):
                w_issue(i * 2 + more - ln_half - 1)

        rows = pl.ds(pl.multiple_of(i * LN_ROWS, LN_ROWS), LN_ROWS)
        n_col = d_model // 128

        def load(j):
            return y_ref[rows, j * 128:(j + 1) * 128].astype(f32)

        accs = [load(j) for j in range(4)]
        for j in range(4, n_col):
            accs[j % 4] = accs[j % 4] + load(j)
        mean = jnp.sum((accs[0] + accs[1]) + (accs[2] + accs[3]), axis=-1, keepdims=True) * (1.0 / d_model)
        mean = jnp.broadcast_to(mean, (LN_ROWS, 128))
        ln_mean[rows, :] = mean
        accs = [None] * 4
        for j in range(n_col):
            cen = load(j) - mean
            accs[j % 4] = cen * cen if accs[j % 4] is None else accs[j % 4] + cen * cen
        var = jnp.sum((accs[0] + accs[1]) + (accs[2] + accs[3]), axis=-1, keepdims=True) * (1.0 / d_model)
        ln_rstd[rows, :] = jnp.broadcast_to(lax.rsqrt(var + LN_EPS), (LN_ROWS, 128))
        return carry

    def ln_scale(i, carry):
        rows = pl.ds(pl.multiple_of(i * LN_ROWS, LN_ROWS), LN_ROWS)
        mean, rstd = ln_mean[rows, :], ln_rstd[rows, :]
        for j in range(d_model // 128):
            out = (y_ref[rows, j * 128:(j + 1) * 128].astype(f32) - mean) * rstd * gain[j:j + 1, :] + bias[j:j + 1, :]
            normed[rows, j * 128:(j + 1) * 128] = out.astype(bf16)
        return carry

    def kv_copy(src, h, dst):
        return pltpu.make_async_remote_copy(src_ref=kv_all.at[src, h], dst_ref=kv_all.at[src, h],
                                            send_sem=kv_send.at[dst, h], recv_sem=kv_recv.at[src, h],
                                            device_id={'cp': dst}, device_id_type=MESH)

    def seg_copy(src, dst):
        return pltpu.make_async_remote_copy(src_ref=seg_all.at[src], dst_ref=seg_all.at[src], send_sem=seg_send.at[dst],
                                            recv_sem=seg_recv.at[src], device_id={'cp': dst}, device_id_type=MESH)

    def late(dst):
        return (dst == n_cp - 1) & (my < n_cp // 2)

    def kv_half(h):
        with jax.named_scope("ln"):
            lax.fori_loop(h * ln_half, (h + 1) * ln_half, ln_block, 0)
            if h == 0:
                small_arrays()
            lax.fori_loop(h * ln_half, (h + 1) * ln_half, ln_scale, 0)
        rows = pl.ds(h * HALF, HALF)
        if h == 0:
            for copy in wkv_copies:
                copy.wait()
        with jax.named_scope("kvdot"):
            mid = d_model // 2
            low = jnp.dot(normed[rows, :mid], wkv[:mid, :], preferred_element_type=f32)
            high = jnp.dot(normed[rows, mid:], wkv[mid:, :], preferred_element_type=f32)
            k_own = ((low[:, :HEAD_DIM] + bkv[0:1, :]) + high[:, :HEAD_DIM]).astype(bf16)
            v_own = ((low[:, HEAD_DIM:] + bkv[1:2, :]) + high[:, HEAD_DIM:]).astype(bf16)
            kv_all[my, h, 0] = k_own
            kv_all[my, h, 1] = v_own.astype(f32).T.astype(bf16)
            k_ref[rows, :] = k_own
            v_ref[rows, :] = v_own
        if h == 0:
            with jax.named_scope("barrier"):
                pl.semaphore_wait(barrier, n_cp)
            for dst in range(1, n_cp):
                @pl.when(my < dst)
                def _():
                    seg_copy(my, dst).start()

        for dst in range(1, n_cp):
            @pl.when((my < dst) & jnp.logical_not(late(dst)))
            def _():
                kv_copy(my, h, dst).start()

    kv_half(0)

    @pl.when(my < n_cp)
    def _():
        for h in range(1, n_half):
            kv_half(h)

    def tile_copy(c, n):
        return pltpu.make_async_remote_copy(src_ref=send[c].at[n], dst_ref=recv[c].at[n], send_sem=tp_send.at[c, n],
                                            recv_sem=tp_recv.at[c, n], device_id={'tp': partner}, device_id_type=MESH)

    def chunk(c):
        base = c * items
        n_row = CHUNKS[c]
        first = sum(CHUNKS[:c])
        rows = slice(first, first + n_row)

        def q_wait(j):
            return [w_wait(base + j * k_halves + half) for half in range(k_halves)]

        def q_next(j):
            for half in range(k_halves):
                w_next(base + j * k_halves + half)

        def q_dot(j, slots):
            acc = None
            step = TILE_K // 2
            for half in range(k_halves):
                for n in range(2):
                    k0 = half * TILE_K + n * step
                    part = jnp.dot(normed[rows, k0:k0 + step], wbuf[slots[half], n * step:(n + 1) * step, :], preferred_element_type=f32)
                    acc = part if acc is None else acc + part
            return acc

        def q_store(j, acc):
            for i in range(TILE_N // 128):
                cols = pl.ds(pl.multiple_of(j * TILE_N + i * 128, 128), 128)
                row = j * (TILE_N // 128) + i
                qbuf[:, cols] = (acc[:, i * 128:(i + 1) * 128] + bq[pl.ds(row, 1), :]).astype(bf16)

        def q_tile(j, carry):
            with jax.named_scope("qtile"):
                acc = None
                step = TILE_K // 2
                for half in range(k_halves):
                    slot = w_wait(base + j * k_halves + half)
                    for n in range(2):
                        k0 = half * TILE_K + n * step
                        part = jnp.dot(normed[rows, k0:k0 + step], wbuf[slot, n * step:(n + 1) * step, :], preferred_element_type=f32)
                        acc = part if acc is None else acc + part
                    w_next(base + j * k_halves + half)
                q_store(j, acc)
            return carry

        own_keys = first + n_row

        def make_mask():
            if c == 0:
                for src in range(n_cp - 1):
                    @pl.when(src < my)
                    def _():
                        seg_copy(src, src).wait_recv()

            seg_q = jnp.broadcast_to(seg_all[my, c:c + 1, :].astype(f32), (128, 128)).T
            below[...] = jnp.zeros((128, 128), f32)
            for b in range(n_cp * tok // 128):
                src, part = b * 128 // tok, b % (tok // 128)

                @pl.when(b * 128 < my * tok + own_keys)
                def _():
                    below[...] += jnp.where(seg_all[src, part:part + 1, :].astype(f32) < seg_q, 1.0, 0.0)

            prompt = jnp.broadcast_to(jnp.sum(below[...], axis=1, keepdims=True), (128, 128)).T
            key = lax.broadcasted_iota(jnp.int32, (128, 128), 0)
            q_pos = my * tok + first + lax.broadcasted_iota(jnp.int32, (128, 128), 1)
            for b in range(n_cp * tok // 128):
                src, part = b * 128 // tok, b % (tok // 128)

                @pl.when(b * 128 < my * tok + own_keys)
                def _():
                    k_pos = key + b * 128
                    seen = (k_pos.astype(f32) >= prompt) & (k_pos <= q_pos)
                    mask[b * 128:(b + 1) * 128, :] = jnp.where(seen, 0.0, -jnp.inf)

        def heads(j, nb, beside=None):
            cols = pl.ds(pl.multiple_of(j * TILE_N, TILE_N), TILE_N)
            n_head = TILE_N // HEAD_DIM
            keys = nb * tok + own_keys
            parts = [kv_all.at[b * 128 // tok, b % (tok // 128)] for b in range(keys // 128)]
            k_blk = jnp.concatenate([part[0] for part in parts], axis=0)
            v_t = jnp.concatenate([part[1] for part in parts], axis=1)
            q_cols = qbuf[:, cols]
            q_rows = jnp.concatenate([q_cols[:, i * HEAD_DIM:(i + 1) * HEAD_DIM] for i in range(n_head)], axis=0)
            s = lax.dot_general(k_blk, q_rows, (((1,), (1,)), ((), ())), preferred_element_type=f32)
            other = beside() if beside else None
            s = s + jnp.concatenate([mask[:keys, :]] * n_head, axis=1)
            p_wts = jnp.exp2((s - jnp.max(s, axis=0, keepdims=True)) * EXP2_SCALE)
            l_sum = jnp.sum(p_wts, axis=0, keepdims=True)
            o = jnp.dot(v_t, p_wts.astype(bf16), preferred_element_type=f32) / l_sum
            obuf[:, cols] = jnp.concatenate([o[:, i * HEAD_DIM:(i + 1) * HEAD_DIM].T for i in range(n_head)], axis=1).astype(bf16)
            return other

        def attend(j, carry):
            for nb in range(n_cp):
                @pl.when(my == nb)
                def _():
                    with jax.named_scope("attn"):
                        heads(j, nb)
            return carry

        def both(j, carry):
            slots = q_wait(j)
            for nb in range(n_cp // 2, n_cp):
                @pl.when(my == nb)
                def _():
                    with jax.named_scope("both"):
                        q_store(j, heads(j - lag, nb, lambda: q_dot(j, slots)))
            q_next(j)
            return carry

        lag = jnp.where(my < n_cp // 2, 1, my)
        q_tile(0, 0)
        if c == 0:
            @pl.when(late(n_cp - 1))
            def _():
                for h in range(n_half):
                    kv_copy(my, h, n_cp - 1).start()

        lax.fori_loop(1, lag, q_tile, 0)
        with jax.named_scope("mask"):
            make_mask()
        if c == 0:
            with jax.named_scope("kvwait"):
                for src in range(n_cp - 1):
                    @pl.when(src < my)
                    def _():
                        for h in range(n_half):
                            kv_copy(src, h, src).wait_recv()
        def turn(j, carry):
            return q_tile(j, attend(j - lag, carry))

        split = jnp.where(my < n_cp // 2, q_tiles, lag) if c == 0 else q_tiles
        lax.fori_loop(lag, split, turn, 0)
        if c == 0:
            lax.fori_loop(split, q_tiles, both, 0)
        lax.fori_loop(q_tiles - lag, q_tiles, attend, 0)

        def o_tile(n, carry):
            with jax.named_scope("otile"):
                g = base + q_items + n
                slot = w_wait(g)
                send[c][n] = jnp.dot(obuf[:n_row, :], wbuf[slot], preferred_element_type=f32).astype(bf16)
                tile_copy(c, n).start()
                w_next(g)
            return carry

        lax.fori_loop(0, o_tiles, o_tile, 0)

    for c in range(n_chunk):
        chunk(c)

    for dst in range(1, n_cp):
        @pl.when(my < dst)
        def _():
            seg_copy(my, dst).wait_send()
            for h in range(n_half):
                kv_copy(my, h, dst).wait_send()

    for c in range(n_chunk):
        first = sum(CHUNKS[:c])
        rows = slice(first, first + CHUNKS[c])

        def finish(n, carry):
            copy = tile_copy(c, n)
            copy.wait_recv()
            copy.wait_send()
            for i in range(TILE_N // 128):
                cols = pl.ds(pl.multiple_of(n * TILE_N + i * 128, 128), 128)
                part = slice(i * 128, (i + 1) * 128)
                both = send[c][n, :, part].astype(f32) + recv[c][n, :, part].astype(f32)
                y_ref[rows, cols] = (y_ref[rows, cols].astype(f32) + both + bo[pl.ds(n * (TILE_N // 128) + i, 1), :]).astype(bf16)
            return carry

        with jax.named_scope("finish"):
            lax.fori_loop(0, o_tiles, finish, 0)


def close_kernel(y_ref, k_ref, v_ref, y_hbm, k_hbm, v_hbm, sem):
    rows = y_ref.shape[0] // 8
    copies = [pltpu.make_async_copy(k_ref, k_hbm, sem.at[8]), pltpu.make_async_copy(v_ref, v_hbm, sem.at[9])]
    copies += [pltpu.make_async_copy(y_ref.at[pl.ds(i * rows, rows), :], y_hbm.at[pl.ds(i * rows, rows), :], sem.at[i]) for i in range(8)]
    for copy in copies:
        copy.start()
    for copy in copies:
        copy.wait()


def solution(mesh):
    n_cp = mesh.shape['cp']

    def local_block(hidden, seg_ids, w_q, b_q, w_kv, b_kv, w_o, b_o, ln_gain, ln_bias):
        tok, d_model = hidden.shape
        q_width = w_q.shape[1]
        o_tiles = d_model // TILE_N
        vmem = pl.BlockSpec(memory_space=pltpu.VMEM)
        hbm = pl.BlockSpec(memory_space=pltpu.HBM)
        bf16, f32 = jnp.bfloat16, jnp.float32
        dma = pltpu.SemaphoreType.DMA
        flops = 2 * tok * d_model * (2 * q_width + 256)
        args = (hidden, seg_ids.reshape(-1, 128), w_q, b_q.reshape(-1, 128), w_kv, b_kv.reshape(-1, 128), w_o,
                b_o.reshape(-1, 128), ln_gain.reshape(-1, 128), ln_bias.reshape(-1, 128))
        args = tuple(pltpu.with_memory_space_constraint(a, pltpu.HBM) for a in args)
        rows = [q_width // 128, 2, d_model // 128, d_model // 128, d_model // 128]
        y, k, v = pl.pallas_call(
            functools.partial(block_kernel, n_cp),
            out_shape=(pltpu.VMEM((tok, d_model), bf16), pltpu.VMEM((tok, HEAD_DIM), bf16), pltpu.VMEM((tok, HEAD_DIM), bf16)),
            in_specs=[hbm] * len(args),
            out_specs=(vmem, vmem, vmem),
            scratch_shapes=[
                pltpu.VMEM((tok, d_model), bf16),
                pltpu.VMEM((d_model, 2 * HEAD_DIM), bf16),
                pltpu.VMEM((SLOTS, TILE_K, TILE_N), bf16),
                pltpu.VMEM((n_cp, tok // HALF, 2, HALF, HEAD_DIM), bf16),
                pltpu.VMEM((n_cp, tok // 128, 128), jnp.int32),
                pltpu.VMEM((128, 128), f32),
                pltpu.VMEM((tok, 128), f32),
                pltpu.VMEM((tok, 128), f32),
                pltpu.VMEM((n_cp * tok, 128), f32),
                pltpu.VMEM((max(CHUNKS), q_width), bf16),
                pltpu.VMEM((max(CHUNKS), q_width), bf16),
                *[pltpu.VMEM((o_tiles, r, TILE_N), bf16) for r in CHUNKS * 2],
                *[pltpu.VMEM((r, 128), bf16) for r in rows],
                *[pltpu.VMEM((r, 128), f32) for r in rows],
                dma((tok // LN_ROWS,)), dma((WKV_PARTS,)), dma((6,)), dma((SLOTS,)),
                dma((n_cp, tok // HALF)), dma((n_cp, tok // HALF)), dma((n_cp,)), dma((n_cp,)),
                dma((len(CHUNKS), o_tiles)), dma((len(CHUNKS), o_tiles)),
            ],
            compiler_params=pltpu.CompilerParams(collective_id=0, has_side_effects=True, vmem_limit_bytes=56 * 1024 * 1024),
            cost_estimate=pl.CostEstimate(flops=flops, bytes_accessed=2 * 4 * d_model * q_width, transcendentals=0),
        )(*args)
        return pl.pallas_call(
            close_kernel,
            out_shape=tuple(jax.ShapeDtypeStruct(a.shape, bf16) for a in (y, k, v)),
            in_specs=[vmem] * 3,
            out_specs=(hbm,) * 3,
            scratch_shapes=[dma((10,))],
            cost_estimate=pl.CostEstimate(flops=1, bytes_accessed=4 * tok * d_model, transcendentals=0),
        )(*(pltpu.with_memory_space_constraint(a, pltpu.VMEM) for a in (y, k, v)))

    row_spec = P(('dp', 'cp'), None)
    tok_spec = P(('dp', 'cp'))
    return jax.shard_map(local_block, mesh=mesh,
                         in_specs=(row_spec, tok_spec, P(None, 'tp'), P('tp'), P(None, None), P(None), P('tp', None), P(None), P(None), P(None)),
                         out_specs=(row_spec, row_spec, row_spec), check_vma=False)
```

```python
import functools

import jax
import jax.numpy as jnp
from jax import lax
from jax.experimental import pallas as pl
from jax.experimental.pallas import tpu as pltpu
from jax.sharding import PartitionSpec as P

HEAD_DIM = 128
LN_EPS = 1e-5
EXP2_SCALE = HEAD_DIM ** -0.5 * 1.4426950408889634
MESH = pl.DeviceIdType.MESH

CHUNKS = (128, 128)
HALF = 128
TILE_K = 3072
TILE_N = 512
AHEAD = 3
SLOTS = 9
LN_ROWS = 32


def block_kernel(n_cp, hid_hbm, seg_hbm, wq_hbm, bq_hbm, wkv_hbm, bkv_hbm, wo_hbm, bo_hbm, gain_hbm, bias_hbm,
                 y_ref, k_ref, v_ref,
                 normed, wkv, wbuf, kv_all, seg_all, below, mask, qbuf, obuf, send0, send1, recv0, recv1,
                 bq_raw, bkv_raw, bo_raw, gain_raw, bias_raw, bq, bkv, bo, gain, bias,
                 hid_sem, wkv_sem, small_sem, w_sem, kv_send, kv_recv, seg_send, seg_recv, tp_send, tp_recv):
    my = lax.axis_index('cp')
    partner = 1 - lax.axis_index('tp')
    tok, d_model = y_ref.shape
    q_width = qbuf.shape[1]
    n_chunk = len(CHUNKS)
    n_half = tok // HALF
    send, recv = (send0, send1), (recv0, recv1)
    q_tiles = q_width // TILE_N
    k_halves = d_model // TILE_K
    o_tiles = d_model // TILE_N
    q_items = q_tiles * k_halves
    items = q_items + o_tiles
    total = n_chunk * items
    f32, bf16 = jnp.float32, jnp.bfloat16

    def hid_copy(i):
        rows = pl.ds(i * LN_ROWS, LN_ROWS)
        return pltpu.make_async_copy(hid_hbm.at[rows, :], y_ref.at[rows, :], hid_sem.at[i])

    def w_issue(g):
        slot = lax.rem(g, SLOTS)
        item = lax.rem(g, items)

        @pl.when(item < q_items)
        def _():
            col = pl.multiple_of(lax.div(item, k_halves) * TILE_N, TILE_N)
            row = pl.multiple_of(lax.rem(item, k_halves) * TILE_K, TILE_K)
            pltpu.make_async_copy(wq_hbm.at[pl.ds(row, TILE_K), pl.ds(col, TILE_N)], wbuf.at[slot], w_sem.at[slot]).start()

        @pl.when(item >= q_items)
        def _():
            col = pl.multiple_of((item - q_items) * TILE_N, TILE_N)
            pltpu.make_async_copy(wo_hbm.at[:, pl.ds(col, TILE_N)], wbuf.at[slot], w_sem.at[slot]).start()

    def w_wait(g):
        slot = lax.rem(g, SLOTS)
        pltpu.make_async_copy(wo_hbm.at[:, pl.ds(0, TILE_N)], wbuf.at[slot], w_sem.at[slot]).wait()
        return slot

    def w_next(g):
        @pl.when(g + SLOTS < total)
        def _():
            w_issue(g + SLOTS)

    n_ln = tok // LN_ROWS
    ln_half = n_ln // n_half
    small = [pltpu.make_async_copy(src, dst, small_sem.at[i]) for i, (src, dst) in enumerate((
        (gain_hbm, gain_raw), (bias_hbm, bias_raw), (bkv_hbm, bkv_raw), (bq_hbm, bq_raw), (bo_hbm, bo_raw), (seg_hbm, seg_all.at[my])))]
    wkv_copy = pltpu.make_async_copy(wkv_hbm, wkv, wkv_sem)
    hid_copy(0).start()
    for copy in small:
        copy.start()
    for i in range(1, n_ln):
        hid_copy(i).start()

    barrier = pltpu.get_barrier_semaphore()
    for step in range(1, n_cp):
        pl.semaphore_signal(barrier, inc=1, device_id={'cp': lax.rem(my + step, n_cp)}, device_id_type=MESH)
    pl.semaphore_signal(barrier, inc=1, device_id={'tp': partner}, device_id_type=MESH)

    with jax.named_scope("hid"):
        hid_copy(0).wait()
        wkv_copy.start()
        for i in range(1, n_ln):
            hid_copy(i).wait()
            if i >= n_ln - AHEAD:
                w_issue(jnp.int32(i - n_ln + AHEAD))

    with jax.named_scope("small"):
        for copy in small:
            copy.wait()
    gain[...] = gain_raw[...].astype(f32)
    bias[...] = bias_raw[...].astype(f32)
    bkv[...] = bkv_raw[...].astype(f32)
    bq[...] = bq_raw[...].astype(f32)
    bo[...] = bo_raw[...].astype(f32)

    def ln_block(i, carry):
        @pl.when(i < (SLOTS - AHEAD) // 2)
        def _():
            for more in range(2):
                w_issue(i * 2 + more + AHEAD)

        rows = pl.ds(pl.multiple_of(i * LN_ROWS, LN_ROWS), LN_ROWS)
        n_col = d_model // 128

        def load(j):
            return y_ref[rows, j * 128:(j + 1) * 128].astype(f32)

        accs = [load(j) for j in range(4)]
        for j in range(4, n_col):
            accs[j % 4] = accs[j % 4] + load(j)
        mean = jnp.sum((accs[0] + accs[1]) + (accs[2] + accs[3]), axis=-1, keepdims=True) * (1.0 / d_model)
        mean = jnp.broadcast_to(mean, (LN_ROWS, 128))
        accs = [None] * 4
        for j in range(n_col):
            cen = load(j) - mean
            accs[j % 4] = cen * cen if accs[j % 4] is None else accs[j % 4] + cen * cen
        var = jnp.sum((accs[0] + accs[1]) + (accs[2] + accs[3]), axis=-1, keepdims=True) * (1.0 / d_model)
        rstd = jnp.broadcast_to(lax.rsqrt(var + LN_EPS), (LN_ROWS, 128))
        for j in range(n_col):
            out = (load(j) - mean) * rstd * gain[j:j + 1, :] + bias[j:j + 1, :]
            normed[rows, j * 128:(j + 1) * 128] = out.astype(bf16)
        return carry

    def kv_copy(src, h, dst):
        return pltpu.make_async_remote_copy(src_ref=kv_all.at[src, h], dst_ref=kv_all.at[src, h],
                                            send_sem=kv_send.at[dst, h], recv_sem=kv_recv.at[src, h],
                                            device_id={'cp': dst}, device_id_type=MESH)

    def seg_copy(src, dst):
        return pltpu.make_async_remote_copy(src_ref=seg_all.at[src], dst_ref=seg_all.at[src], send_sem=seg_send.at[dst],
                                            recv_sem=seg_recv.at[src], device_id={'cp': dst}, device_id_type=MESH)

    def late(dst):
        return (dst == n_cp - 1) & (my < n_cp // 2)

    def kv_half(h):
        with jax.named_scope("ln"):
            lax.fori_loop(h * ln_half, (h + 1) * ln_half, ln_block, 0)
        rows = pl.ds(h * HALF, HALF)
        if h == 0:
            wkv_copy.wait()
        with jax.named_scope("kvdot"):
            mid = d_model // 2
            low = jnp.dot(normed[rows, :mid], wkv[:mid, :], preferred_element_type=f32)
            high = jnp.dot(normed[rows, mid:], wkv[mid:, :], preferred_element_type=f32)
            k_own = ((low[:, :HEAD_DIM] + bkv[0:1, :]) + high[:, :HEAD_DIM]).astype(bf16)
            v_own = ((low[:, HEAD_DIM:] + bkv[1:2, :]) + high[:, HEAD_DIM:]).astype(bf16)
            kv_all[my, h, 0] = k_own
            kv_all[my, h, 1] = v_own.astype(f32).T.astype(bf16)
            k_ref[rows, :] = k_own
            v_ref[rows, :] = v_own
        if h == 0:
            with jax.named_scope("barrier"):
                pl.semaphore_wait(barrier, n_cp)
            for dst in range(1, n_cp):
                @pl.when(my < dst)
                def _():
                    seg_copy(my, dst).start()

        for dst in range(1, n_cp):
            @pl.when((my < dst) & jnp.logical_not(late(dst)))
            def _():
                kv_copy(my, h, dst).start()

    kv_half(0)

    @pl.when(my < n_cp)
    def _():
        for h in range(1, n_half):
            kv_half(h)

    def tile_copy(c, n):
        return pltpu.make_async_remote_copy(src_ref=send[c].at[n], dst_ref=recv[c].at[n], send_sem=tp_send.at[c, n],
                                            recv_sem=tp_recv.at[c, n], device_id={'tp': partner}, device_id_type=MESH)

    def chunk(c):
        base = c * items
        n_row = CHUNKS[c]
        first = sum(CHUNKS[:c])
        rows = slice(first, first + n_row)

        def q_wait(j):
            return [w_wait(base + j * k_halves + half) for half in range(k_halves)]

        def q_next(j):
            for half in range(k_halves):
                w_next(base + j * k_halves + half)

        def q_dot(j, slots):
            acc = None
            step = TILE_K // 2
            for half in range(k_halves):
                for n in range(2):
                    k0 = half * TILE_K + n * step
                    part = jnp.dot(normed[rows, k0:k0 + step], wbuf[slots[half], n * step:(n + 1) * step, :], preferred_element_type=f32)
                    acc = part if acc is None else acc + part
            return acc

        def q_store(j, acc):
            for i in range(TILE_N // 128):
                cols = pl.ds(pl.multiple_of(j * TILE_N + i * 128, 128), 128)
                row = j * (TILE_N // 128) + i
                qbuf[:, cols] = (acc[:, i * 128:(i + 1) * 128] + bq[pl.ds(row, 1), :]).astype(bf16)

        def q_tile(j, carry):
            with jax.named_scope("qtile"):
                q_store(j, q_dot(j, q_wait(j)))
                q_next(j)
            return carry

        own_keys = first + n_row

        def make_mask():
            if c == 0:
                for src in range(n_cp - 1):
                    @pl.when(src < my)
                    def _():
                        seg_copy(src, src).wait_recv()

            seg_q = jnp.broadcast_to(seg_all[my, c:c + 1, :].astype(f32), (128, 128)).T
            below[...] = jnp.zeros((128, 128), f32)
            for b in range(n_cp * tok // 128):
                src, part = b * 128 // tok, b % (tok // 128)

                @pl.when(b * 128 < my * tok + own_keys)
                def _():
                    below[...] += jnp.where(seg_all[src, part:part + 1, :].astype(f32) < seg_q, 1.0, 0.0)

            prompt = jnp.broadcast_to(jnp.sum(below[...], axis=1, keepdims=True), (128, 128)).T
            key = lax.broadcasted_iota(jnp.int32, (128, 128), 0)
            q_pos = my * tok + first + lax.broadcasted_iota(jnp.int32, (128, 128), 1)
            for b in range(n_cp * tok // 128):
                src, part = b * 128 // tok, b % (tok // 128)

                @pl.when(b * 128 < my * tok + own_keys)
                def _():
                    k_pos = key + b * 128
                    seen = (k_pos.astype(f32) >= prompt) & (k_pos <= q_pos)
                    mask[b * 128:(b + 1) * 128, :] = jnp.where(seen, 0.0, -jnp.inf)

        def heads(j, nb, beside=None):
            cols = pl.ds(pl.multiple_of(j * TILE_N, TILE_N), TILE_N)
            n_head = TILE_N // HEAD_DIM
            keys = nb * tok + own_keys
            parts = [kv_all.at[b * 128 // tok, b % (tok // 128)] for b in range(keys // 128)]
            k_blk = jnp.concatenate([part[0] for part in parts], axis=0)
            v_t = jnp.concatenate([part[1] for part in parts], axis=1)
            q_cols = qbuf[:, cols]
            q_rows = jnp.concatenate([q_cols[:, i * HEAD_DIM:(i + 1) * HEAD_DIM] for i in range(n_head)], axis=0)
            s = lax.dot_general(k_blk, q_rows, (((1,), (1,)), ((), ())), preferred_element_type=f32)
            other = beside() if beside else None
            s = s + jnp.concatenate([mask[:keys, :]] * n_head, axis=1)
            p_wts = jnp.exp2((s - jnp.max(s, axis=0, keepdims=True)) * EXP2_SCALE)
            l_sum = jnp.sum(p_wts, axis=0, keepdims=True)
            o = jnp.dot(v_t, p_wts.astype(bf16), preferred_element_type=f32) / l_sum
            obuf[:, cols] = jnp.concatenate([o[:, i * HEAD_DIM:(i + 1) * HEAD_DIM].T for i in range(n_head)], axis=1).astype(bf16)
            return other

        def attend(j, carry):
            for nb in range(n_cp):
                @pl.when(my == nb)
                def _():
                    with jax.named_scope("attn"):
                        heads(j, nb)
            return carry

        def both(j, carry):
            slots = q_wait(j)
            for nb in range(n_cp):
                @pl.when(my == nb)
                def _():
                    with jax.named_scope("both"):
                        q_store(j, heads(j - lag, nb, lambda: q_dot(j, slots)))
            q_next(j)
            return carry

        lag = jnp.where(my < n_cp // 2, 1, 2)
        q_tile(0, 0)
        lax.fori_loop(1, lag, q_tile, 0)
        with jax.named_scope("mask"):
            make_mask()
        if c == 0:
            @pl.when(late(n_cp - 1))
            def _():
                for h in range(n_half):
                    kv_copy(my, h, n_cp - 1).start()

        if c == 0:
            with jax.named_scope("kvwait"):
                for src in range(n_cp - 1):
                    @pl.when(src < my)
                    def _():
                        for h in range(n_half):
                            kv_copy(src, h, src).wait_recv()
        if c == 0:
            lax.fori_loop(lag, q_tiles, both, 0)
        else:
            def turn(j, carry):
                return attend(j - lag, q_tile(j, carry))

            lax.fori_loop(lag, q_tiles, turn, 0)
        lax.fori_loop(q_tiles - lag, q_tiles, attend, 0)

        def o_tile(n, carry):
            with jax.named_scope("otile"):
                g = base + q_items + n
                slot = w_wait(g)
                send[c][n] = jnp.dot(obuf[:n_row, :], wbuf[slot], preferred_element_type=f32).astype(bf16)
                tile_copy(c, n).start()
                w_next(g)
            return carry

        lax.fori_loop(0, o_tiles, o_tile, 0)

    for c in range(n_chunk):
        chunk(c)

    for dst in range(1, n_cp):
        @pl.when(my < dst)
        def _():
            seg_copy(my, dst).wait_send()
            for h in range(n_half):
                kv_copy(my, h, dst).wait_send()

    for c in range(n_chunk):
        first = sum(CHUNKS[:c])
        rows = slice(first, first + CHUNKS[c])

        def finish(n, carry):
            copy = tile_copy(c, n)
            copy.wait_recv()
            copy.wait_send()
            for i in range(TILE_N // 128):
                cols = pl.ds(pl.multiple_of(n * TILE_N + i * 128, 128), 128)
                part = slice(i * 128, (i + 1) * 128)
                both = send[c][n, :, part].astype(f32) + recv[c][n, :, part].astype(f32)
                y_ref[rows, cols] = (y_ref[rows, cols].astype(f32) + both + bo[pl.ds(n * (TILE_N // 128) + i, 1), :]).astype(bf16)
            return carry

        with jax.named_scope("finish"):
            lax.fori_loop(0, o_tiles, finish, 0)


def close_kernel(y_ref, k_ref, v_ref, y_hbm, k_hbm, v_hbm, sem):
    rows = y_ref.shape[0] // 8
    copies = [pltpu.make_async_copy(k_ref, k_hbm, sem.at[8]), pltpu.make_async_copy(v_ref, v_hbm, sem.at[9])]
    copies += [pltpu.make_async_copy(y_ref.at[pl.ds(i * rows, rows), :], y_hbm.at[pl.ds(i * rows, rows), :], sem.at[i]) for i in range(8)]
    for copy in copies:
        copy.start()
    for copy in copies:
        copy.wait()


def solution(mesh):
    n_cp = mesh.shape['cp']

    def local_block(hidden, seg_ids, w_q, b_q, w_kv, b_kv, w_o, b_o, ln_gain, ln_bias):
        tok, d_model = hidden.shape
        q_width = w_q.shape[1]
        o_tiles = d_model // TILE_N
        vmem = pl.BlockSpec(memory_space=pltpu.VMEM)
        hbm = pl.BlockSpec(memory_space=pltpu.HBM)
        bf16, f32 = jnp.bfloat16, jnp.float32
        dma = pltpu.SemaphoreType.DMA
        flops = 2 * tok * d_model * (2 * q_width + 256)
        args = (hidden, seg_ids.reshape(-1, 128), w_q, b_q.reshape(-1, 128), w_kv, b_kv.reshape(-1, 128), w_o,
                b_o.reshape(-1, 128), ln_gain.reshape(-1, 128), ln_bias.reshape(-1, 128))
        args = tuple(pltpu.with_memory_space_constraint(a, pltpu.HBM) for a in args)
        rows = [q_width // 128, 2, d_model // 128, d_model // 128, d_model // 128]
        y, k, v = pl.pallas_call(
            functools.partial(block_kernel, n_cp),
            out_shape=(pltpu.VMEM((tok, d_model), bf16), pltpu.VMEM((tok, HEAD_DIM), bf16), pltpu.VMEM((tok, HEAD_DIM), bf16)),
            in_specs=[hbm] * len(args),
            out_specs=(vmem, vmem, vmem),
            scratch_shapes=[
                pltpu.VMEM((tok, d_model), bf16),
                pltpu.VMEM((d_model, 2 * HEAD_DIM), bf16),
                pltpu.VMEM((SLOTS, TILE_K, TILE_N), bf16),
                pltpu.VMEM((n_cp, tok // HALF, 2, HALF, HEAD_DIM), bf16),
                pltpu.VMEM((n_cp, tok // 128, 128), jnp.int32),
                pltpu.VMEM((128, 128), f32),
                pltpu.VMEM((n_cp * tok, 128), f32),
                pltpu.VMEM((max(CHUNKS), q_width), bf16),
                pltpu.VMEM((max(CHUNKS), q_width), bf16),
                *[pltpu.VMEM((o_tiles, r, TILE_N), bf16) for r in CHUNKS * 2],
                *[pltpu.VMEM((r, 128), bf16) for r in rows],
                *[pltpu.VMEM((r, 128), f32) for r in rows],
                dma((tok // LN_ROWS,)), dma, dma((6,)), dma((SLOTS,)),
                dma((n_cp, tok // HALF)), dma((n_cp, tok // HALF)), dma((n_cp,)), dma((n_cp,)),
                dma((len(CHUNKS), o_tiles)), dma((len(CHUNKS), o_tiles)),
            ],
            compiler_params=pltpu.CompilerParams(collective_id=0, has_side_effects=True, vmem_limit_bytes=56 * 1024 * 1024),
            cost_estimate=pl.CostEstimate(flops=flops, bytes_accessed=2 * 4 * d_model * q_width, transcendentals=0),
        )(*args)
        return pl.pallas_call(
            close_kernel,
            out_shape=tuple(jax.ShapeDtypeStruct(a.shape, bf16) for a in (y, k, v)),
            in_specs=[vmem] * 3,
            out_specs=(hbm,) * 3,
            scratch_shapes=[dma((10,))],
            cost_estimate=pl.CostEstimate(flops=1, bytes_accessed=4 * tok * d_model, transcendentals=0),
        )(*(pltpu.with_memory_space_constraint(a, pltpu.VMEM) for a in (y, k, v)))

    row_spec = P(('dp', 'cp'), None)
    tok_spec = P(('dp', 'cp'))
    return jax.shard_map(local_block, mesh=mesh,
                         in_specs=(row_spec, tok_spec, P(None, 'tp'), P('tp'), P(None, None), P(None), P('tp', None), P(None), P(None), P(None)),
                         out_specs=(row_spec, row_spec, row_spec), check_vma=False)
```

```python
import functools

import jax
import jax.numpy as jnp
from jax import lax
from jax.experimental import pallas as pl
from jax.experimental.pallas import tpu as pltpu
from jax.sharding import PartitionSpec as P

HEAD_DIM = 128
LN_EPS = 1e-5
EXP2_SCALE = HEAD_DIM ** -0.5 * 1.4426950408889634
MESH = pl.DeviceIdType.MESH

CHUNKS = (128, 128)
HALF = 128
TILE_K = 3072
TILE_N = 512
AHEAD = 3
SLOTS = 9
LN_ROWS = 32


def block_kernel(n_cp, hid_hbm, seg_hbm, wq_hbm, bq_hbm, wkv_hbm, bkv_hbm, wo_hbm, bo_hbm, gain_hbm, bias_hbm,
                 y_ref, k_ref, v_ref,
                 normed, wkv, wbuf, kv_all, seg_all, below, mask, qbuf, obuf, send0, send1, recv0, recv1,
                 bq_raw, bkv_raw, bo_raw, gain_raw, bias_raw, bq, bkv, bo, gain, bias,
                 hid_sem, wkv_sem, small_sem, w_sem, kv_send, kv_recv, seg_send, seg_recv, tp_send, tp_recv):
    my = lax.axis_index('cp')
    partner = 1 - lax.axis_index('tp')
    tok, d_model = y_ref.shape
    q_width = qbuf.shape[1]
    n_chunk = len(CHUNKS)
    n_half = tok // HALF
    send, recv = (send0, send1), (recv0, recv1)
    q_tiles = q_width // TILE_N
    k_halves = d_model // TILE_K
    o_tiles = d_model // TILE_N
    q_items = q_tiles * k_halves
    items = q_items + o_tiles
    total = n_chunk * items
    f32, bf16 = jnp.float32, jnp.bfloat16

    def hid_copy(i):
        rows = pl.ds(i * LN_ROWS, LN_ROWS)
        return pltpu.make_async_copy(hid_hbm.at[rows, :], y_ref.at[rows, :], hid_sem.at[i])

    def w_issue(g):
        slot = lax.rem(g, SLOTS)
        item = lax.rem(g, items)

        @pl.when(item < q_items)
        def _():
            col = pl.multiple_of(lax.div(item, k_halves) * TILE_N, TILE_N)
            row = pl.multiple_of(lax.rem(item, k_halves) * TILE_K, TILE_K)
            pltpu.make_async_copy(wq_hbm.at[pl.ds(row, TILE_K), pl.ds(col, TILE_N)], wbuf.at[slot], w_sem.at[slot]).start()

        @pl.when(item >= q_items)
        def _():
            col = pl.multiple_of((item - q_items) * TILE_N, TILE_N)
            pltpu.make_async_copy(wo_hbm.at[:, pl.ds(col, TILE_N)], wbuf.at[slot], w_sem.at[slot]).start()

    def w_wait(g):
        slot = lax.rem(g, SLOTS)
        pltpu.make_async_copy(wo_hbm.at[:, pl.ds(0, TILE_N)], wbuf.at[slot], w_sem.at[slot]).wait()
        return slot

    def w_next(g):
        @pl.when(g + SLOTS < total)
        def _():
            w_issue(g + SLOTS)

    n_ln = tok // LN_ROWS
    ln_half = n_ln // n_half
    small = [pltpu.make_async_copy(src, dst, small_sem.at[i]) for i, (src, dst) in enumerate((
        (gain_hbm, gain_raw), (bias_hbm, bias_raw), (bkv_hbm, bkv_raw), (bq_hbm, bq_raw), (bo_hbm, bo_raw), (seg_hbm, seg_all.at[my])))]
    wkv_copy = pltpu.make_async_copy(wkv_hbm, wkv, wkv_sem)
    hid_copy(0).start()
    for copy in small:
        copy.start()
    for i in range(1, n_ln):
        hid_copy(i).start()

    barrier = pltpu.get_barrier_semaphore()
    for step in range(1, n_cp):
        pl.semaphore_signal(barrier, inc=1, device_id={'cp': lax.rem(my + step, n_cp)}, device_id_type=MESH)
    pl.semaphore_signal(barrier, inc=1, device_id={'tp': partner}, device_id_type=MESH)

    with jax.named_scope("hid"):
        hid_copy(0).wait()
        wkv_copy.start()
        for i in range(1, n_ln):
            hid_copy(i).wait()
            if i >= n_ln - AHEAD:
                w_issue(jnp.int32(i - n_ln + AHEAD))

    with jax.named_scope("small"):
        for copy in small:
            copy.wait()
    gain[...] = gain_raw[...].astype(f32)
    bias[...] = bias_raw[...].astype(f32)
    bkv[...] = bkv_raw[...].astype(f32)
    bq[...] = bq_raw[...].astype(f32)
    bo[...] = bo_raw[...].astype(f32)

    def ln_block(i, carry):
        @pl.when(i < (SLOTS - AHEAD) // 2)
        def _():
            for more in range(2):
                w_issue(i * 2 + more + AHEAD)

        rows = pl.ds(pl.multiple_of(i * LN_ROWS, LN_ROWS), LN_ROWS)
        n_col = d_model // 128

        def load(j):
            return y_ref[rows, j * 128:(j + 1) * 128].astype(f32)

        accs = [load(j) for j in range(4)]
        for j in range(4, n_col):
            accs[j % 4] = accs[j % 4] + load(j)
        mean = jnp.sum((accs[0] + accs[1]) + (accs[2] + accs[3]), axis=-1, keepdims=True) * (1.0 / d_model)
        mean = jnp.broadcast_to(mean, (LN_ROWS, 128))
        accs = [None] * 4
        for j in range(n_col):
            cen = load(j) - mean
            accs[j % 4] = cen * cen if accs[j % 4] is None else accs[j % 4] + cen * cen
        var = jnp.sum((accs[0] + accs[1]) + (accs[2] + accs[3]), axis=-1, keepdims=True) * (1.0 / d_model)
        rstd = jnp.broadcast_to(lax.rsqrt(var + LN_EPS), (LN_ROWS, 128))
        for j in range(n_col):
            out = (load(j) - mean) * rstd * gain[j:j + 1, :] + bias[j:j + 1, :]
            normed[rows, j * 128:(j + 1) * 128] = out.astype(bf16)
        return carry

    def kv_copy(src, h, dst):
        return pltpu.make_async_remote_copy(src_ref=kv_all.at[src, h], dst_ref=kv_all.at[src, h],
                                            send_sem=kv_send.at[dst, h], recv_sem=kv_recv.at[src, h],
                                            device_id={'cp': dst}, device_id_type=MESH)

    def seg_copy(src, dst):
        return pltpu.make_async_remote_copy(src_ref=seg_all.at[src], dst_ref=seg_all.at[src], send_sem=seg_send.at[dst],
                                            recv_sem=seg_recv.at[src], device_id={'cp': dst}, device_id_type=MESH)

    def late(dst):
        return (dst == n_cp - 1) & (my < n_cp // 2)

    def kv_half(h):
        with jax.named_scope("ln"):
            lax.fori_loop(h * ln_half, (h + 1) * ln_half, ln_block, 0)
        rows = pl.ds(h * HALF, HALF)
        if h == 0:
            wkv_copy.wait()
        with jax.named_scope("kvdot"):
            mid = d_model // 2
            low = jnp.dot(normed[rows, :mid], wkv[:mid, :], preferred_element_type=f32)
            high = jnp.dot(normed[rows, mid:], wkv[mid:, :], preferred_element_type=f32)
            k_own = ((low[:, :HEAD_DIM] + bkv[0:1, :]) + high[:, :HEAD_DIM]).astype(bf16)
            v_own = ((low[:, HEAD_DIM:] + bkv[1:2, :]) + high[:, HEAD_DIM:]).astype(bf16)
            kv_all[my, h, 0] = k_own
            kv_all[my, h, 1] = v_own.astype(f32).T.astype(bf16)
            k_ref[rows, :] = k_own
            v_ref[rows, :] = v_own
        if h == 0:
            with jax.named_scope("barrier"):
                pl.semaphore_wait(barrier, n_cp)
            for dst in range(1, n_cp):
                @pl.when(my < dst)
                def _():
                    seg_copy(my, dst).start()

        for dst in range(1, n_cp):
            @pl.when((my < dst) & jnp.logical_not(late(dst)))
            def _():
                kv_copy(my, h, dst).start()

    kv_half(0)

    @pl.when(my < n_cp)
    def _():
        for h in range(1, n_half):
            kv_half(h)

    def tile_copy(c, n):
        return pltpu.make_async_remote_copy(src_ref=send[c].at[n], dst_ref=recv[c].at[n], send_sem=tp_send.at[c, n],
                                            recv_sem=tp_recv.at[c, n], device_id={'tp': partner}, device_id_type=MESH)

    def chunk(c):
        base = c * items
        n_row = CHUNKS[c]
        first = sum(CHUNKS[:c])
        rows = slice(first, first + n_row)

        def q_wait(j):
            return [w_wait(base + j * k_halves + half) for half in range(k_halves)]

        def q_next(j):
            for half in range(k_halves):
                w_next(base + j * k_halves + half)

        def q_dot(j, slots):
            acc = None
            step = TILE_K // 2
            for half in range(k_halves):
                for n in range(2):
                    k0 = half * TILE_K + n * step
                    part = jnp.dot(normed[rows, k0:k0 + step], wbuf[slots[half], n * step:(n + 1) * step, :], preferred_element_type=f32)
                    acc = part if acc is None else acc + part
            return acc

        def q_store(j, acc):
            for i in range(TILE_N // 128):
                cols = pl.ds(pl.multiple_of(j * TILE_N + i * 128, 128), 128)
                row = j * (TILE_N // 128) + i
                qbuf[:, cols] = (acc[:, i * 128:(i + 1) * 128] + bq[pl.ds(row, 1), :]).astype(bf16)

        def q_tile(j, carry):
            with jax.named_scope("qtile"):
                q_store(j, q_dot(j, q_wait(j)))
                q_next(j)
            return carry

        own_keys = first + n_row

        def make_mask():
            if c == 0:
                for src in range(n_cp - 1):
                    @pl.when(src < my)
                    def _():
                        seg_copy(src, src).wait_recv()

            seg_q = jnp.broadcast_to(seg_all[my, c:c + 1, :].astype(f32), (128, 128)).T
            below[...] = jnp.zeros((128, 128), f32)
            for b in range(n_cp * tok // 128):
                src, part = b * 128 // tok, b % (tok // 128)

                @pl.when(b * 128 < my * tok + own_keys)
                def _():
                    below[...] += jnp.where(seg_all[src, part:part + 1, :].astype(f32) < seg_q, 1.0, 0.0)

            prompt = jnp.broadcast_to(jnp.sum(below[...], axis=1, keepdims=True), (128, 128)).T
            key = lax.broadcasted_iota(jnp.int32, (128, 128), 0)
            q_pos = my * tok + first + lax.broadcasted_iota(jnp.int32, (128, 128), 1)
            for b in range(n_cp * tok // 128):
                src, part = b * 128 // tok, b % (tok // 128)

                @pl.when(b * 128 < my * tok + own_keys)
                def _():
                    k_pos = key + b * 128
                    seen = (k_pos.astype(f32) >= prompt) & (k_pos <= q_pos)
                    mask[b * 128:(b + 1) * 128, :] = jnp.where(seen, 0.0, -jnp.inf)

        def heads(j, nb, beside=None):
            cols = pl.ds(pl.multiple_of(j * TILE_N, TILE_N), TILE_N)
            n_head = TILE_N // HEAD_DIM
            keys = nb * tok + own_keys
            parts = [kv_all.at[b * 128 // tok, b % (tok // 128)] for b in range(keys // 128)]
            k_blk = jnp.concatenate([part[0] for part in parts], axis=0)
            v_t = jnp.concatenate([part[1] for part in parts], axis=1)
            q_cols = qbuf[:, cols]
            q_rows = jnp.concatenate([q_cols[:, i * HEAD_DIM:(i + 1) * HEAD_DIM] for i in range(n_head)], axis=0)
            s = lax.dot_general(k_blk, q_rows, (((1,), (1,)), ((), ())), preferred_element_type=f32)
            other = beside() if beside else None
            s = s + jnp.concatenate([mask[:keys, :]] * n_head, axis=1)
            p_wts = jnp.exp2((s - jnp.max(s, axis=0, keepdims=True)) * EXP2_SCALE)
            l_sum = jnp.sum(p_wts, axis=0, keepdims=True)
            o = jnp.dot(v_t, p_wts.astype(bf16), preferred_element_type=f32) / l_sum
            obuf[:, cols] = jnp.concatenate([o[:, i * HEAD_DIM:(i + 1) * HEAD_DIM].T for i in range(n_head)], axis=1).astype(bf16)
            return other

        def attend(j, carry):
            for nb in range(n_cp):
                @pl.when(my == nb)
                def _():
                    with jax.named_scope("attn"):
                        heads(j, nb)
            return carry

        def both(j, carry):
            slots = q_wait(j)
            for nb in range(n_cp):
                @pl.when(my == nb)
                def _():
                    with jax.named_scope("both"):
                        q_store(j, heads(j - lag, nb, lambda: q_dot(j, slots)))
            q_next(j)
            return carry

        lag = jnp.where(my < n_cp // 2, 1, my)
        q_tile(0, 0)
        lax.fori_loop(1, lag, q_tile, 0)
        with jax.named_scope("mask"):
            make_mask()
        if c == 0:
            @pl.when(late(n_cp - 1))
            def _():
                for h in range(n_half):
                    kv_copy(my, h, n_cp - 1).start()

        if c == 0:
            with jax.named_scope("kvwait"):
                for src in range(n_cp - 1):
                    @pl.when(src < my)
                    def _():
                        for h in range(n_half):
                            kv_copy(src, h, src).wait_recv()
        if c == 0:
            lax.fori_loop(lag, q_tiles, both, 0)
        else:
            def turn(j, carry):
                return attend(j - lag, q_tile(j, carry))

            lax.fori_loop(lag, q_tiles, turn, 0)
        lax.fori_loop(q_tiles - lag, q_tiles, attend, 0)

        def o_tile(n, carry):
            with jax.named_scope("otile"):
                g = base + q_items + n
                slot = w_wait(g)
                send[c][n] = jnp.dot(obuf[:n_row, :], wbuf[slot], preferred_element_type=f32).astype(bf16)
                tile_copy(c, n).start()
                w_next(g)
            return carry

        lax.fori_loop(0, o_tiles, o_tile, 0)

    for c in range(n_chunk):
        chunk(c)

    for dst in range(1, n_cp):
        @pl.when(my < dst)
        def _():
            seg_copy(my, dst).wait_send()
            for h in range(n_half):
                kv_copy(my, h, dst).wait_send()

    for c in range(n_chunk):
        first = sum(CHUNKS[:c])
        rows = slice(first, first + CHUNKS[c])

        def finish(n, carry):
            copy = tile_copy(c, n)
            copy.wait_recv()
            copy.wait_send()
            for i in range(TILE_N // 128):
                cols = pl.ds(pl.multiple_of(n * TILE_N + i * 128, 128), 128)
                part = slice(i * 128, (i + 1) * 128)
                both = send[c][n, :, part].astype(f32) + recv[c][n, :, part].astype(f32)
                y_ref[rows, cols] = (y_ref[rows, cols].astype(f32) + both + bo[pl.ds(n * (TILE_N // 128) + i, 1), :]).astype(bf16)
            return carry

        with jax.named_scope("finish"):
            lax.fori_loop(0, o_tiles, finish, 0)


def close_kernel(y_ref, k_ref, v_ref, y_hbm, k_hbm, v_hbm, sem):
    rows = y_ref.shape[0] // 8
    copies = [pltpu.make_async_copy(k_ref, k_hbm, sem.at[8]), pltpu.make_async_copy(v_ref, v_hbm, sem.at[9])]
    copies += [pltpu.make_async_copy(y_ref.at[pl.ds(i * rows, rows), :], y_hbm.at[pl.ds(i * rows, rows), :], sem.at[i]) for i in range(8)]
    for copy in copies:
        copy.start()
    for copy in copies:
        copy.wait()


def solution(mesh):
    n_cp = mesh.shape['cp']

    def local_block(hidden, seg_ids, w_q, b_q, w_kv, b_kv, w_o, b_o, ln_gain, ln_bias):
        tok, d_model = hidden.shape
        q_width = w_q.shape[1]
        o_tiles = d_model // TILE_N
        vmem = pl.BlockSpec(memory_space=pltpu.VMEM)
        hbm = pl.BlockSpec(memory_space=pltpu.HBM)
        bf16, f32 = jnp.bfloat16, jnp.float32
        dma = pltpu.SemaphoreType.DMA
        flops = 2 * tok * d_model * (2 * q_width + 256)
        args = (hidden, seg_ids.reshape(-1, 128), w_q, b_q.reshape(-1, 128), w_kv, b_kv.reshape(-1, 128), w_o,
                b_o.reshape(-1, 128), ln_gain.reshape(-1, 128), ln_bias.reshape(-1, 128))
        args = tuple(pltpu.with_memory_space_constraint(a, pltpu.HBM) for a in args)
        rows = [q_width // 128, 2, d_model // 128, d_model // 128, d_model // 128]
        y, k, v = pl.pallas_call(
            functools.partial(block_kernel, n_cp),
            out_shape=(pltpu.VMEM((tok, d_model), bf16), pltpu.VMEM((tok, HEAD_DIM), bf16), pltpu.VMEM((tok, HEAD_DIM), bf16)),
            in_specs=[hbm] * len(args),
            out_specs=(vmem, vmem, vmem),
            scratch_shapes=[
                pltpu.VMEM((tok, d_model), bf16),
                pltpu.VMEM((d_model, 2 * HEAD_DIM), bf16),
                pltpu.VMEM((SLOTS, TILE_K, TILE_N), bf16),
                pltpu.VMEM((n_cp, tok // HALF, 2, HALF, HEAD_DIM), bf16),
                pltpu.VMEM((n_cp, tok // 128, 128), jnp.int32),
                pltpu.VMEM((128, 128), f32),
                pltpu.VMEM((n_cp * tok, 128), f32),
                pltpu.VMEM((max(CHUNKS), q_width), bf16),
                pltpu.VMEM((max(CHUNKS), q_width), bf16),
                *[pltpu.VMEM((o_tiles, r, TILE_N), bf16) for r in CHUNKS * 2],
                *[pltpu.VMEM((r, 128), bf16) for r in rows],
                *[pltpu.VMEM((r, 128), f32) for r in rows],
                dma((tok // LN_ROWS,)), dma, dma((6,)), dma((SLOTS,)),
                dma((n_cp, tok // HALF)), dma((n_cp, tok // HALF)), dma((n_cp,)), dma((n_cp,)),
                dma((len(CHUNKS), o_tiles)), dma((len(CHUNKS), o_tiles)),
            ],
            compiler_params=pltpu.CompilerParams(collective_id=0, has_side_effects=True, vmem_limit_bytes=56 * 1024 * 1024),
            cost_estimate=pl.CostEstimate(flops=flops, bytes_accessed=2 * 4 * d_model * q_width, transcendentals=0),
        )(*args)
        return pl.pallas_call(
            close_kernel,
            out_shape=tuple(jax.ShapeDtypeStruct(a.shape, bf16) for a in (y, k, v)),
            in_specs=[vmem] * 3,
            out_specs=(hbm,) * 3,
            scratch_shapes=[dma((10,))],
            cost_estimate=pl.CostEstimate(flops=1, bytes_accessed=4 * tok * d_model, transcendentals=0),
        )(*(pltpu.with_memory_space_constraint(a, pltpu.VMEM) for a in (y, k, v)))

    row_spec = P(('dp', 'cp'), None)
    tok_spec = P(('dp', 'cp'))
    return jax.shard_map(local_block, mesh=mesh,
                         in_specs=(row_spec, tok_spec, P(None, 'tp'), P('tp'), P(None, None), P(None), P('tp', None), P(None), P(None), P(None)),
                         out_specs=(row_spec, row_spec, row_spec), check_vma=False)
```
